32 devices in a mesh: row: 8 (over y, x, core), col: 4 (over z).
Axes of the slice: x: 2, y: 2, z: 4, core: 2. Of those that a mesh axis runs over, the one named last changes fastest.
Arguments:
- source_points: float32 [3, 32768], P(None, 'col'), may hold values from 0 to 1
- source_areas: float32 [32768], P('col'), may hold values from 0.02 to 0.2
- source_fill: int32 [128], P('col'), may hold values from 128 to 256
- target_points: float32 [3, 32768], P(None, 'row'), may hold values from 0 to 1
- target_fill: int32 [128], P('row'), may hold values from 128 to 256
- charges: bfloat16 [64, 32768], P('row', 'col'), may hold values from -6 to 6
- near_fill: int32 [8, 4], P('row', 'col'), may hold values from 32 to 256, as said below
- near_source: int32 [8, 1024], P('row', 'col'), may hold values from 0 to 31
- near_target: int32 [8, 1024], P('row', 'col'), may hold values from 0 to 15
- far_source: int32 [8, 384], P('row', 'col'), may hold values from 0 to 31
- far_target: int32 [8, 384], P('row', 'col'), may hold values from 0 to 15
- far_rank: int32 [8, 384], P('row', 'col'), may hold values from 8 to 32
- left_basis: bfloat16 [8, 384, 32, 256], P('row', 'col'), may hold values from -0.25 to 0.25
- right_basis: bfloat16 [8, 384, 32, 256], P('row', 'col'), may hold values from -0.375 to 0.375
Outputs:
- potential: float32 [64, 32768], P('col', 'row')
The draws below stay inside these ranges and needn't reach their ends.
Inputs may be any that keep to these rules, and one draw needn't show every extreme that they name: `near_fill`: used slots are the first ones of a device; in every row some device uses all 256. `near_source`: index among the 32 source leaves of the device's column group. `near_target`: index among the 16 target leaves of the device's row group. `far_source`: index among the 32 source leaves of the device's column group. `far_target`: index among the 16 target leaves of the device's row group. `far_rank`: factor rows from the rank on are padding.
All inputs are finite; a program needn't handle non-finite values.
Results may differ from the reference program's by a relative error of at most 0.0029.
Values may be sent and summed in bfloat16 or wider, within the bound.
No kernel may reach another device: no remote copies, remote signals or barrier semaphores. Data moves between devices by JAX's collectives and lax.ppermute only.
A program may use at most 64 MiB of HBM per device.

```python
import math
import jax
import jax.numpy as jnp
from jax import lax

LEAF = 256
RANK = 32
RHS = 64
RL = 16
NEAR_DEV = 256
ADM_DEV = 96
CL = 32
NS = 32768
NT = 32768
N_ROW = 8
N_COL = 4


def draw_near_fill(key, part):
    row_index = jnp.arange(N_ROW)[:, None]
    col_index = jnp.arange(N_COL)[None, :]
    crowded = col_index == row_index * N_COL // N_ROW
    sparse_fill = jax.random.randint(jax.random.fold_in(key, 11), (N_ROW, N_COL), NEAR_DEV // 8, NEAR_DEV // 4 + 1)
    return jnp.where(crowded, NEAR_DEV, sparse_fill).astype(jnp.int32)


def touch_ends(drawn, own_key, smallest, largest):
    longest = drawn.shape.index(max(drawn.shape))
    spots = []
    for shift in (0, 1):
        where = [jax.random.randint(jax.random.fold_in(own_key, axis), (), 0, length) for axis, length in enumerate(drawn.shape)]
        where[longest] = (where[longest] + shift) % drawn.shape[longest]
        spots.append(tuple(where))
    return drawn.at[spots[0]].set(smallest).at[spots[1]].set(largest)


def level_of(own_key, shape, shards, smallest, high):
    level = 1.0
    for dim, blocks in shards:
        draws = jax.random.uniform(jax.random.fold_in(jax.random.fold_in(own_key, 6), dim), (blocks,), jnp.float32, smallest / len(shards), high / len(shards))
        level = level * jnp.repeat(jnp.exp(draws), shape[dim] // blocks).reshape((-1,) + (1,) * (len(shape) - 1 - dim))
    return level


def gaussian(rng, extent, deviation, reach, cuts=(), held_as=jnp.bfloat16):
    result = jax.random.normal(rng, extent, jnp.float32) * deviation
    if len(cuts) > 0:
        result = level_of(rng, extent, cuts, -0.22, 0.18) * result
    return jnp.clip(result, min=-reach, max=reach).astype(held_as)


def setup_inputs(seed: int = 0) -> dict:
    arg_keys = jax.random.split(jax.random.key(seed), 15)
    source_points = jnp.clip(1.0 * jax.random.uniform(arg_keys[0], (3, NS), jnp.float32) ** level_of(arg_keys[0], (3, NS), ((1, 4),), -0.2, 0.2), 0.0, 1.0)
    source_areas = jnp.clip(jnp.exp(math.log(0.2) - 2.3025851 * jax.random.uniform(arg_keys[1], (NS,), jnp.float32) ** level_of(arg_keys[1], (NS,), ((0, 4),), -0.2, 0.2)), 0.02, 0.2)
    source_fill = touch_ends(jax.random.randint(arg_keys[2], (CL * N_COL,), LEAF // 2, LEAF + 1), jax.random.fold_in(arg_keys[2], 1), LEAF // 2, LEAF).astype(jnp.int32)
    target_points = jnp.clip(1.0 * jax.random.uniform(arg_keys[3], (3, NT), jnp.float32) ** level_of(arg_keys[3], (3, NT), ((1, 8),), -0.2, 0.2), 0.0, 1.0)
    target_fill = touch_ends(jax.random.randint(arg_keys[4], (RL * N_ROW,), LEAF // 2, LEAF + 1), jax.random.fold_in(arg_keys[4], 1), LEAF // 2, LEAF).astype(jnp.int32)
    charges = gaussian(arg_keys[5], (RHS, NS), 1.0, 6.0, ((0, 8), (1, 4)))
    near_fill = draw_near_fill(jax.random.fold_in(arg_keys[14], 71), 0)
    near_source = touch_ends(jax.random.randint(arg_keys[7], (N_ROW, N_COL * NEAR_DEV), 0, CL), jax.random.fold_in(arg_keys[7], 1), 0, CL - 1).astype(jnp.int32)
    near_target = touch_ends(jax.random.randint(arg_keys[8], (N_ROW, N_COL * NEAR_DEV), 0, RL), jax.random.fold_in(arg_keys[8], 1), 0, RL - 1).astype(jnp.int32)
    far_source = touch_ends(jax.random.randint(arg_keys[9], (N_ROW, N_COL * ADM_DEV), 0, CL), jax.random.fold_in(arg_keys[9], 1), 0, CL - 1).astype(jnp.int32)
    far_target = touch_ends(jax.random.randint(arg_keys[10], (N_ROW, N_COL * ADM_DEV), 0, RL), jax.random.fold_in(arg_keys[10], 1), 0, RL - 1).astype(jnp.int32)
    far_rank = touch_ends(jax.random.randint(arg_keys[11], (N_ROW, N_COL * ADM_DEV), RANK // 4, RANK + 1), jax.random.fold_in(arg_keys[11], 1), RANK // 4, RANK).astype(jnp.int32)
    left_basis = gaussian(arg_keys[12], (N_ROW, N_COL * ADM_DEV, RANK, LEAF), (16 * RANK) ** -0.5, 0.25, ((0, 8), (1, 4)))
    right_basis = gaussian(arg_keys[13], (N_ROW, N_COL * ADM_DEV, RANK, LEAF), LEAF ** -0.5, 0.375, ((0, 8), (1, 4)))
    return dict(source_points=source_points, source_areas=source_areas, source_fill=source_fill, target_points=target_points, target_fill=target_fill, charges=charges, near_fill=near_fill, near_source=near_source, near_target=near_target, far_source=far_source, far_target=far_target, far_rank=far_rank, left_basis=left_basis, right_basis=right_basis)


INV_FOUR_PI = 0.07957747154594767
SOFTENING_SQ = 0.0025

def kernel_block(target_block, geometry):
    dist_sq = (target_block[0][:, None, :] - geometry[0][:, :, None]) ** 2
    dist_sq = dist_sq + (target_block[1][:, None, :] - geometry[1][:, :, None]) ** 2
    dist_sq = dist_sq + (target_block[2][:, None, :] - geometry[2][:, :, None]) ** 2
    return geometry[3][:, :, None] * INV_FOUR_PI * lax.rsqrt(dist_sq + SOFTENING_SQ)

def reference(source_points, source_areas, source_fill, target_points, target_fill, charges, near_fill, near_source, near_target, far_source, far_target, far_rank, left_basis, right_basis):
    devices_all = N_ROW * N_COL
    source_live = jnp.arange(LEAF, dtype=jnp.int32)[None, :] < source_fill[:, None]
    charge_grid = jnp.where(source_live[None], charges.reshape(RHS, CL * N_COL, LEAF), jnp.zeros((), charges.dtype))
    geometry_grid = jnp.concatenate([source_points, source_areas[None, :]], 0).reshape(4, CL * N_COL, LEAF)
    target_grid = target_points.reshape(3, RL * N_ROW, LEAF)
    row_base = (jnp.arange(N_ROW, dtype=jnp.int32) * RL)[:, None, None]
    col_base = (jnp.arange(N_COL, dtype=jnp.int32) * CL)[None, :, None]
    near_src_all = (near_source.reshape(N_ROW, N_COL, NEAR_DEV) + col_base).reshape(devices_all, NEAR_DEV).astype(jnp.int32)
    near_tgt_all = (near_target.reshape(N_ROW, N_COL, NEAR_DEV) + row_base).reshape(devices_all, NEAR_DEV).astype(jnp.int32)
    near_alive = jnp.arange(NEAR_DEV, dtype=jnp.int32)[None, :] < near_fill.reshape(devices_all, 1)
    far_src_all = (far_source.reshape(N_ROW, N_COL, ADM_DEV) + col_base).reshape(devices_all, ADM_DEV).astype(jnp.int32)
    far_tgt_all = (far_target.reshape(N_ROW, N_COL, ADM_DEV) + row_base).reshape(devices_all, ADM_DEV).astype(jnp.int32)
    rank_all = far_rank.reshape(devices_all, ADM_DEV)
    left_all = left_basis.reshape(devices_all, ADM_DEV, RANK, LEAF)
    right_all = right_basis.reshape(devices_all, ADM_DEV, RANK, LEAF)
    potential = jnp.zeros((RHS, RL * N_ROW, LEAF), jnp.float32)

    def near_step(running, slot_data):
        source_ids, target_ids, alive_mask = slot_data
        charge_block = jnp.take(charge_grid, source_ids, axis=1).astype(jnp.float32)
        geometry_block = jnp.take(geometry_grid, source_ids, axis=1)
        target_block = jnp.take(target_grid, target_ids, axis=1)
        entries = jnp.where(alive_mask[:, None, None], kernel_block(target_block, geometry_block), 0.0).astype(jnp.bfloat16)
        entries = lax.optimization_barrier(entries).astype(jnp.float32)
        blocks = jnp.einsum('ebs,bst->bet', charge_block, entries, precision=lax.Precision.HIGHEST)
        return (running.at[:, target_ids].add(jnp.transpose(blocks, (1, 0, 2))), None)

    def far_step(running, slot_data):
        source_ids, target_ids, ranks, left_slots, right_slots = slot_data
        gathered = jnp.take(charge_grid, source_ids, axis=1).astype(jnp.float32)
        coefficients = jnp.einsum('eas,ars->aer', gathered, right_slots.astype(jnp.float32), precision=lax.Precision.HIGHEST)
        rank_mask = jnp.arange(RANK, dtype=jnp.int32)[None, :] < ranks[:, None]
        coefficients = jnp.where(rank_mask[:, None, :], coefficients, 0.0).astype(jnp.bfloat16)
        coefficients = lax.optimization_barrier(coefficients).astype(jnp.float32)
        blocks = jnp.einsum('aer,art->aet', coefficients, left_slots.astype(jnp.float32), precision=lax.Precision.HIGHEST)
        return (running.at[:, target_ids].add(jnp.transpose(blocks, (1, 0, 2))), None)
    potential, _ = lax.scan(near_step, potential, (near_src_all, near_tgt_all, near_alive))
    potential, _ = lax.scan(far_step, potential, (far_src_all, far_tgt_all, rank_all, left_all, right_all))
    target_live = jnp.arange(LEAF, dtype=jnp.int32)[None, :] < target_fill[:, None]
    potential = jnp.where(target_live[None], potential, 0.0)
    return potential.reshape(RHS, RL * N_ROW * LEAF)
```

```python
import functools

import jax
import jax.numpy as jnp
from jax import lax
from jax.experimental import pallas as pl
from jax.experimental.pallas import tpu as pltpu
from jax.sharding import PartitionSpec as P

INV_FOUR_PI = 0.07957747154594767
SOFTENING_SQ = 0.0025
F32 = jnp.float32
BF16 = jnp.bfloat16
VMEM_LIMIT = 60 << 20


def split3(value):
    first = value.astype(BF16).astype(F32)
    rest = value - first
    second = rest.astype(BF16).astype(F32)
    return first, second, rest - second


def feature_rows(rows):
    count = rows[0].shape[1]
    index = lax.broadcasted_iota(jnp.int32, (8, count), 0)
    out = jnp.zeros((8, count), F32)
    for position, row in enumerate(rows):
        out = jnp.where(index == position, jnp.broadcast_to(row, (8, count)), out)
    return out


def build_list(fill, src_ref, tgt_ref, list_ref, column_leaves, half_id):
    slots = src_ref.shape[1]
    square = (slots, slots)
    id_row = (tgt_ref[...] * column_leaves + src_ref[...]).astype(F32)
    id_r = jnp.broadcast_to(id_row, square)
    id_c = id_r.T
    lane = lax.broadcasted_iota(jnp.int32, square, 1)
    sub = lax.broadcasted_iota(jnp.int32, square, 0)
    same = id_r == id_c
    ones = jnp.ones(square, BF16)

    def lane_sum(mask):
        return jnp.dot(mask.astype(F32).astype(BF16), ones, preferred_element_type=F32)

    count_c = lane_sum(same & (lane < fill))
    earlier_c = lane_sum(same & (lane < sub))
    first_c = (earlier_c == 0.0) & (sub < fill)
    earlier_r = jnp.sum(jnp.where(same & (sub < lane), 1.0, 0.0), axis=0, keepdims=True)
    first_r = (earlier_r == 0.0) & (lane[:1] < fill)
    rank_c = lane_sum(jnp.broadcast_to(jnp.where(first_r, 1.0, 0.0), square) * jnp.where(id_r < id_c, 1.0, 0.0) > 0.5)
    hit = first_c & (rank_c == lane.astype(F32))
    list_r = jnp.sum(jnp.where(hit, id_c, 0.0), axis=0, keepdims=True)
    copies_r = jnp.sum(jnp.where(hit, count_c, 0.0), axis=0, keepdims=True)
    total = jnp.sum(jnp.where(first_r, 1.0, 0.0))
    half = jnp.sum(jnp.where(first_r & (id_row < float(half_id)), 1.0, 0.0))
    index = lax.broadcasted_iota(jnp.int32, (8, slots), 0)
    table = jnp.where(index == 0, jnp.broadcast_to(list_r, (8, slots)), 0.0)
    table = jnp.where(index == 1, jnp.broadcast_to(copies_r, (8, slots)), table)
    table = jnp.where(index == 2, total, table)
    table = jnp.where(index == 3, half, table)
    list_ref[...] = table.astype(jnp.int32)


def entries_kernel(
    fill_ref, src_ref, tgt_ref, spts_ref, area_ref, tpts_ref,
    entries_ref, list_ref,
    s_ref, t_ref, table_ref, sem,
    *, column_leaves, row_leaves, leaf, unroll,
):
    fill = fill_ref[0, 0]
    build_list(fill, src_ref, tgt_ref, list_ref, column_leaves, (row_leaves // 2) * column_leaves)
    copy = pltpu.make_async_copy(list_ref, table_ref, sem)
    copy.start()

    tx, ty, tz = (tpts_ref[i : i + 1, :] - 0.5 for i in range(3))
    norm = tx * tx + ty * ty + tz * tz
    h1, h2, h3 = split3(feature_rows([tx, ty, tz, jnp.ones_like(tx), norm]))
    features = jnp.concatenate([h1, h2, h1, h2, h3, h1, jnp.zeros((16,) + h1.shape[1:], F32)], axis=0).astype(BF16)
    for t in range(row_leaves):
        t_ref[t] = features[:, t * leaf : (t + 1) * leaf]

    sx, sy, sz = (spts_ref[i : i + 1, :] - 0.5 for i in range(3))
    scale = area_ref[...] * INV_FOUR_PI
    weight = 1.0 / (scale * scale)
    norm = sx * sx + sy * sy + sz * sz + SOFTENING_SQ
    g1, g2, g3 = split3(
        feature_rows([-2.0 * weight * sx, -2.0 * weight * sy, -2.0 * weight * sz, weight * norm, weight])
    )
    features = jnp.concatenate([g1, g1, g2, g2, g1, g3, jnp.zeros((16,) + g1.shape[1:], F32)], axis=0)
    for s in range(column_leaves):
        s_ref[s] = features[:, s * leaf : (s + 1) * leaf].T.astype(BF16)

    copy.wait()
    total = table_ref[2, 0]

    @pl.loop(0, (total + unroll - 1) // unroll)
    def _(turn):
        for u in range(unroll):
            k = turn * unroll + u
            pair = table_ref[0, k]
            t = pair // column_leaves
            s = pair % column_leaves
            dist = jnp.dot(s_ref[s], t_ref[t], preferred_element_type=F32)
            entries_ref[k] = lax.rsqrt(dist).astype(BF16)


def make_entries(near_fill, near_source, near_target, source_points, source_areas, target_points, column_leaves, row_leaves):
    slots = near_source.shape[1]
    leaf = source_points.shape[1] // column_leaves
    depth = 64
    vmem = pl.BlockSpec(memory_space=pltpu.VMEM)
    smem = pl.BlockSpec(memory_space=pltpu.SMEM)
    return pl.pallas_call(
        functools.partial(
            entries_kernel, column_leaves=column_leaves, row_leaves=row_leaves, leaf=leaf, unroll=8
        ),
        out_shape=(
            pltpu.VMEM((slots, leaf, leaf), BF16),
            jax.ShapeDtypeStruct((8, slots), jnp.int32),
        ),
        in_specs=[smem, vmem, vmem, vmem, vmem, vmem],
        out_specs=(vmem, vmem),
        scratch_shapes=[
            pltpu.VMEM((column_leaves, leaf, depth), BF16),
            pltpu.VMEM((row_leaves, depth, leaf), BF16),
            pltpu.SMEM((8, slots), jnp.int32),
            pltpu.SemaphoreType.DMA,
        ],
        compiler_params=pltpu.CompilerParams(vmem_limit_bytes=16 << 20),
        cost_estimate=pl.CostEstimate(flops=8_000_000_000, bytes_accessed=1 << 20, transcendentals=0),
        name="entries",
    )(near_fill, near_source, near_target, source_points, source_areas[None, :], target_points)


def apply_kernel(*refs, pieces, plain, leaf, unroll):
    (table_ref, sfill_ref, tfill_ref, fsrc_ref, ftgt_ref, frank_ref, entries_ref, left_ref, right_ref) = refs[:9]
    piece_refs = refs[9 : 9 + pieces]
    x_ref, coef_ref, acc_ref = refs[-3:]
    out_refs = refs[9 + pieces : -3]
    column_leaves, rhs, _ = x_ref.shape
    row_leaves = acc_ref.shape[0]
    far_slots, rank, _ = left_ref.shape

    lane = lax.broadcasted_iota(jnp.int32, (rhs, leaf), 1)
    if not plain:
        parity = lax.rem(lax.axis_index("row"), 2)
    for s in range(column_leaves):
        window = slice(s * leaf, (s + 1) * leaf)
        if plain:
            block = piece_refs[0][:, window].astype(F32)
        else:
            rows = []
            for j in range(pieces // 2):
                mine = piece_refs[j][:, window].astype(F32)
                other = piece_refs[pieces // 2 + j][:, window].astype(F32)
                rows.append(jnp.where(parity == 0, mine, other))
                rows.append(jnp.where(parity == 0, other, mine))
            block = jnp.concatenate(rows, axis=0)
        x_ref[s] = jnp.where(lane < sfill_ref[s], block, 0.0).astype(BF16)

    acc_ref[...] = jnp.zeros_like(acc_ref)

    rank_lane = lax.broadcasted_iota(jnp.int32, (rhs, rank), 1)

    @pl.loop(0, far_slots // unroll)
    def _(turn):
        for u in range(unroll):
            k = turn * unroll + u
            coef = lax.dot_general(
                x_ref[fsrc_ref[0, k]], right_ref[k], (((1,), (1,)), ((), ())), preferred_element_type=F32
            )
            coef_ref[k] = jnp.where(rank_lane < frank_ref[0, k], coef, 0.0).astype(BF16)

    @pl.loop(0, far_slots // unroll)
    def _(turn):
        blocks = []
        for u in range(unroll):
            k = turn * unroll + u
            blocks.append(jnp.dot(coef_ref[k], left_ref[k], preferred_element_type=F32))
        for u in range(unroll):
            t = ftgt_ref[0, turn * unroll + u]
            acc_ref[t] = acc_ref[t] + blocks[u]

    total = table_ref[2, 0]

    @pl.loop(0, (total + unroll - 1) // unroll)
    def _(turn):
        blocks = []
        for u in range(unroll):
            k = turn * unroll + u
            blocks.append(
                jnp.dot(x_ref[table_ref[0, k] % column_leaves], entries_ref[k], preferred_element_type=F32)
            )
        for u in range(unroll):
            k = turn * unroll + u
            t = table_ref[0, k] // column_leaves
            copies = table_ref[1, k].astype(F32)
            acc_ref[t] = acc_ref[t] + jnp.where(copies > 0.0, blocks[u] * copies, 0.0)

    if plain:
        lane_t = lax.broadcasted_iota(jnp.int32, (rhs, leaf), 1)
        for t in range(row_leaves):
            out_refs[0][:, t * leaf : (t + 1) * leaf] = jnp.where(lane_t < tfill_ref[t], acc_ref[t], 0.0)
    else:
        owners = len(out_refs)
        height = rhs // owners
        lane_t = lax.broadcasted_iota(jnp.int32, (height, leaf), 1)
        base = lax.axis_index("col") ^ (lax.axis_index("row") // 2)
        for m in range(owners):
            start = pl.multiple_of((base ^ m) * height, height)
            for t in range(row_leaves):
                value = jnp.where(lane_t < tfill_ref[t], acc_ref[t, pl.ds(start, height), :], 0.0)
                out_refs[m][:, t * leaf : (t + 1) * leaf] = value.astype(out_refs[m].dtype)


def apply_blocks(table, source_fill, target_fill, far_source, far_target, far_rank, entries, left, right, pieces, owners, plain):
    column_leaves, row_leaves = source_fill.shape[0], target_fill.shape[0]
    far_slots, rank, leaf = left.shape
    rhs = sum(p.shape[0] for p in pieces)
    vmem = pl.BlockSpec(memory_space=pltpu.VMEM)
    smem = pl.BlockSpec(memory_space=pltpu.SMEM)
    width = row_leaves * leaf
    if plain:
        out_shape = (jax.ShapeDtypeStruct((rhs, width), F32),)
    else:
        out_shape = tuple(
            jax.ShapeDtypeStruct((rhs // owners, width), F32 if m == 0 else BF16) for m in range(owners)
        )
    return pl.pallas_call(
        functools.partial(apply_kernel, pieces=len(pieces), plain=plain, leaf=leaf, unroll=8),
        out_shape=out_shape,
        in_specs=[smem] * 6 + [vmem] * (3 + len(pieces)),
        out_specs=(vmem,) * len(out_shape),
        scratch_shapes=[
            pltpu.VMEM((column_leaves, rhs, leaf), BF16),
            pltpu.VMEM((far_slots, rhs, rank), BF16),
            pltpu.VMEM((row_leaves, rhs, leaf), F32),
        ],
        compiler_params=pltpu.CompilerParams(vmem_limit_bytes=16 << 20),
        cost_estimate=pl.CostEstimate(flops=8_000_000_000, bytes_accessed=8 << 20, transcendentals=0),
        name="apply",
    )(table, source_fill, target_fill, far_source, far_target, far_rank, entries, left, right, *pieces)


def shards(
    source_points, source_areas, source_fill, target_points, target_fill, charges, near_fill, near_source,
    near_target, far_source, far_target, far_rank, left_basis, right_basis, *, rows, columns,
):
    plain = charges.shape[0] % 8 != 0 or rows != 2 * columns
    if plain:
        pieces = [lax.all_gather(charges, "row", axis=0, tiled=True)]
    else:

        def swap(value, axis, size, mask):
            return lax.ppermute(value, axis, [(i, i ^ mask) for i in range(size)])

        pieces = [charges] + [swap(charges, "row", rows, mask) for mask in range(2, rows, 2)]
    entries, table = make_entries(
        near_fill, near_source, near_target, source_points, source_areas, target_points,
        source_fill.shape[0], target_fill.shape[0],
    )
    if not plain:
        pieces = pieces + [swap(piece, "row", rows, 1) for piece in pieces]
    outs = apply_blocks(
        table, source_fill, target_fill, far_source, far_target, far_rank, entries, left_basis[0], right_basis[0],
        pieces, columns, plain,
    )
    if plain:
        return lax.psum_scatter(outs[0], "col", scatter_dimension=0, tiled=True)
    result = outs[0]
    for mask in range(1, columns):
        result = result + swap(outs[mask], "col", columns, mask).astype(F32)
    return result


def solution(mesh):
    placed = (
        P(None, "col"), P("col"), P("col"), P(None, "row"), P("row"), P("row", "col"), P("row", "col"),
        P("row", "col"), P("row", "col"), P("row", "col"), P("row", "col"), P("row", "col"),
        P("row", "col", None, None), P("row", "col", None, None),
    )
    return jax.shard_map(
        functools.partial(shards, rows=mesh.shape["row"], columns=mesh.shape["col"]),
        mesh=mesh, in_specs=placed, out_specs=P("col", "row"), check_vma=False,
    )
```

```python
import functools

import jax
import jax.numpy as jnp
from jax import lax
from jax.experimental import pallas as pl
from jax.experimental.pallas import tpu as pltpu
from jax.sharding import PartitionSpec as P

INV_FOUR_PI = 0.07957747154594767
SOFTENING_SQ = 0.0025
F32 = jnp.float32
BF16 = jnp.bfloat16
VMEM_LIMIT = 60 << 20


def split3(value):
    first = value.astype(BF16).astype(F32)
    rest = value - first
    second = rest.astype(BF16).astype(F32)
    return first, second, rest - second


def feature_rows(rows):
    count = rows[0].shape[1]
    index = lax.broadcasted_iota(jnp.int32, (8, count), 0)
    out = jnp.zeros((8, count), F32)
    for position, row in enumerate(rows):
        out = jnp.where(index == position, jnp.broadcast_to(row, (8, count)), out)
    return out


def part_count(slots):
    return 4 if slots % 32 == 0 else 1


def build_list(fill, src_ref, tgt_ref, list_ref, column_leaves, half_id):
    slots = src_ref.shape[1]
    square = (slots, slots)
    id_row = (tgt_ref[...] * column_leaves + src_ref[...]).astype(F32)
    id_r = jnp.broadcast_to(id_row, square)
    id_c = id_r.T
    lane = lax.broadcasted_iota(jnp.int32, square, 1)
    sub = lax.broadcasted_iota(jnp.int32, square, 0)
    same = id_r == id_c
    ones = jnp.ones(square, BF16)

    def lane_sum(mask):
        return jnp.dot(mask.astype(F32).astype(BF16), ones, preferred_element_type=F32)

    count_c = lane_sum(same & (lane < fill))
    earlier_c = lane_sum(same & (lane < sub))
    first_c = (earlier_c == 0.0) & (sub < fill)
    earlier_r = jnp.sum(jnp.where(same & (sub < lane), 1.0, 0.0), axis=0, keepdims=True)
    first_r = (earlier_r == 0.0) & (lane[:1] < fill)
    rank_c = lane_sum(jnp.broadcast_to(jnp.where(first_r, 1.0, 0.0), square) * jnp.where(id_r < id_c, 1.0, 0.0) > 0.5)
    hit = first_c & (rank_c == lane.astype(F32))
    list_r = jnp.sum(jnp.where(hit, id_c, 0.0), axis=0, keepdims=True)
    copies_r = jnp.sum(jnp.where(hit, count_c, 0.0), axis=0, keepdims=True)
    total = jnp.sum(jnp.where(first_r, 1.0, 0.0))
    half = jnp.sum(jnp.where(first_r & (id_row < float(half_id)), 1.0, 0.0))
    index = lax.broadcasted_iota(jnp.int32, (8, slots), 0)
    table = jnp.where(index == 0, jnp.broadcast_to(list_r, (8, slots)), 0.0)
    table = jnp.where(index == 1, jnp.broadcast_to(copies_r, (8, slots)), table)
    table = jnp.where(index == 2, total, table)
    table = jnp.where(index == 3, half, table)
    list_ref[...] = table.astype(jnp.int32)


def entries_kernel(*refs, column_leaves, row_leaves, leaf, parts, unroll):
    inputs, outputs, scratch = refs[:6], refs[6 : 7 + parts], refs[7 + parts :]
    entries_refs, list_ref = outputs[:-1], outputs[-1]
    copies, (s_ref, t_ref, table_ref, sem, in_sem) = scratch[:6], scratch[6:]
    loads = [pltpu.make_async_copy(src, dst, in_sem.at[i]) for i, (src, dst) in enumerate(zip(inputs, copies))]
    for load in loads:
        load.start()
    fill_ref, src_ref, tgt_ref, spts_ref, area_ref, tpts_ref = copies
    for load in loads[:3]:
        load.wait()
    fill = fill_ref[0, 0]
    build_list(fill, src_ref, tgt_ref, list_ref, column_leaves, (row_leaves // 2) * column_leaves)
    copy = pltpu.make_async_copy(list_ref, table_ref, sem)
    copy.start()
    for load in loads[3:]:
        load.wait()

    tx, ty, tz = (tpts_ref[i : i + 1, :] - 0.5 for i in range(3))
    norm = tx * tx + ty * ty + tz * tz
    h1, h2, h3 = split3(feature_rows([tx, ty, tz, jnp.ones_like(tx), norm]))
    features = jnp.concatenate([h1, h2, h1, h2, h3, h1, jnp.zeros((16,) + h1.shape[1:], F32)], axis=0).astype(BF16)
    for t in range(row_leaves):
        t_ref[t] = features[:, t * leaf : (t + 1) * leaf]

    sx, sy, sz = (spts_ref[i : i + 1, :] - 0.5 for i in range(3))
    scale = area_ref[...] * INV_FOUR_PI
    weight = 1.0 / (scale * scale)
    norm = sx * sx + sy * sy + sz * sz + SOFTENING_SQ
    g1, g2, g3 = split3(
        feature_rows([-2.0 * weight * sx, -2.0 * weight * sy, -2.0 * weight * sz, weight * norm, weight])
    )
    features = jnp.concatenate([g1, g1, g2, g2, g1, g3, jnp.zeros((16,) + g1.shape[1:], F32)], axis=0)
    for s in range(column_leaves):
        s_ref[s] = features[:, s * leaf : (s + 1) * leaf].T.astype(BF16)

    copy.wait()
    total = table_ref[2, 0]

    for part, entries_ref in enumerate(entries_refs):
        size = entries_ref.shape[0]
        count = jnp.clip(total - part * size, 0, size)

        @pl.loop(0, (count + unroll - 1) // unroll)
        def _(turn):
            for u in range(unroll):
                k = turn * unroll + u
                pair = table_ref[0, part * size + k]
                t = pair // column_leaves
                s = pair % column_leaves
                dist = jnp.dot(s_ref[s], t_ref[t], preferred_element_type=F32)
                entries_ref[k] = lax.rsqrt(dist).astype(BF16)


def make_entries(near_fill, near_source, near_target, source_points, source_areas, target_points, column_leaves, row_leaves):
    slots = near_source.shape[1]
    leaf = source_points.shape[1] // column_leaves
    depth = 64
    vmem = pl.BlockSpec(memory_space=pltpu.VMEM)
    hbm = pl.BlockSpec(memory_space=pltpu.HBM)
    parts = part_count(slots)
    inputs = (near_fill, near_source, near_target, source_points, source_areas[None, :], target_points)
    return pl.pallas_call(
        functools.partial(
            entries_kernel, column_leaves=column_leaves, row_leaves=row_leaves, leaf=leaf, parts=parts, unroll=8
        ),
        out_shape=(pltpu.VMEM((slots // parts, leaf, leaf), BF16),) * parts
        + (jax.ShapeDtypeStruct((8, slots), jnp.int32),),
        in_specs=[hbm] * len(inputs),
        out_specs=(vmem,) * (parts + 1),
        scratch_shapes=[pltpu.SMEM((1, 1), jnp.int32)]
        + [pltpu.VMEM(value.shape, value.dtype) for value in inputs[1:]]
        + [
            pltpu.VMEM((column_leaves, leaf, depth), BF16),
            pltpu.VMEM((row_leaves, depth, leaf), BF16),
            pltpu.SMEM((8, slots), jnp.int32),
            pltpu.SemaphoreType.DMA,
            pltpu.SemaphoreType.DMA((len(inputs),)),
        ],
        compiler_params=pltpu.CompilerParams(vmem_limit_bytes=16 << 20),
        cost_estimate=pl.CostEstimate(flops=8_000_000_000, bytes_accessed=1 << 20, transcendentals=0),
        name="entries",
    )(*inputs)


def apply_kernel(*refs, pieces, parts, plain, leaf, unroll):
    (table_ref, sfill_ref, tfill_ref, fsrc_ref, ftgt_ref, frank_ref, left_ref, right_ref) = refs[:8]
    piece_refs = refs[8 : 8 + pieces]
    entries_refs = refs[8 + pieces : 8 + pieces + parts]
    x_ref, coef_ref, acc_ref = refs[-3:]
    out_refs = refs[8 + pieces + parts : -3]
    column_leaves, rhs, _ = x_ref.shape
    row_leaves = acc_ref.shape[0]
    far_slots, rank, _ = left_ref.shape

    lane = lax.broadcasted_iota(jnp.int32, (rhs, leaf), 1)
    if not plain:
        parity = lax.rem(lax.axis_index("row"), 2)
    for s in range(column_leaves):
        window = slice(s * leaf, (s + 1) * leaf)
        if plain:
            block = piece_refs[0][:, window].astype(F32)
        else:
            rows = []
            for j in range(pieces // 2):
                mine = piece_refs[j][:, window].astype(F32)
                other = piece_refs[pieces // 2 + j][:, window].astype(F32)
                rows.append(jnp.where(parity == 0, mine, other))
                rows.append(jnp.where(parity == 0, other, mine))
            block = jnp.concatenate(rows, axis=0)
        x_ref[s] = jnp.where(lane < sfill_ref[s], block, 0.0).astype(BF16)

    acc_ref[...] = jnp.zeros_like(acc_ref)

    rank_lane = lax.broadcasted_iota(jnp.int32, (rhs, rank), 1)

    @pl.loop(0, far_slots // unroll)
    def _(turn):
        for u in range(unroll):
            k = turn * unroll + u
            coef = lax.dot_general(
                x_ref[fsrc_ref[0, k]], right_ref[k], (((1,), (1,)), ((), ())), preferred_element_type=F32
            )
            coef_ref[k] = jnp.where(rank_lane < frank_ref[0, k], coef, 0.0).astype(BF16)

    @pl.loop(0, far_slots // unroll)
    def _(turn):
        blocks = []
        for u in range(unroll):
            k = turn * unroll + u
            blocks.append(jnp.dot(coef_ref[k], left_ref[k], preferred_element_type=F32))
        for u in range(unroll):
            t = ftgt_ref[0, turn * unroll + u]
            acc_ref[t] = acc_ref[t] + blocks[u]

    total = table_ref[2, 0]

    for part, entries_ref in enumerate(entries_refs):
        size = entries_ref.shape[0]
        count = jnp.clip(total - part * size, 0, size)

        @pl.loop(0, (count + unroll - 1) // unroll)
        def _(turn):
            blocks = []
            for u in range(unroll):
                k = turn * unroll + u
                source = table_ref[0, part * size + k] % column_leaves
                blocks.append(jnp.dot(x_ref[source], entries_ref[k], preferred_element_type=F32))
            for u in range(unroll):
                k = part * size + turn * unroll + u
                t = table_ref[0, k] // column_leaves
                copies = table_ref[1, k].astype(F32)
                acc_ref[t] = acc_ref[t] + jnp.where(copies > 0.0, blocks[u] * copies, 0.0)

    if plain:
        lane_t = lax.broadcasted_iota(jnp.int32, (rhs, leaf), 1)
        for t in range(row_leaves):
            out_refs[0][:, t * leaf : (t + 1) * leaf] = jnp.where(lane_t < tfill_ref[t], acc_ref[t], 0.0)
    else:
        owners = len(out_refs)
        height = rhs // owners
        lane_t = lax.broadcasted_iota(jnp.int32, (height, leaf), 1)
        base = lax.axis_index("col") ^ (lax.axis_index("row") // 2)
        for m in range(owners):
            start = pl.multiple_of((base ^ m) * height, height)
            for t in range(row_leaves):
                value = jnp.where(lane_t < tfill_ref[t], acc_ref[t, pl.ds(start, height), :], 0.0)
                out_refs[m][:, t * leaf : (t + 1) * leaf] = value.astype(out_refs[m].dtype)


def apply_blocks(table, source_fill, target_fill, far_source, far_target, far_rank, entries, left, right, pieces, owners, plain):
    column_leaves, row_leaves = source_fill.shape[0], target_fill.shape[0]
    far_slots, rank, leaf = left.shape
    rhs = sum(p.shape[0] for p in pieces)
    vmem = pl.BlockSpec(memory_space=pltpu.VMEM)
    smem = pl.BlockSpec(memory_space=pltpu.SMEM)
    width = row_leaves * leaf
    if plain:
        out_shape = (jax.ShapeDtypeStruct((rhs, width), F32),)
    else:
        out_shape = tuple(
            jax.ShapeDtypeStruct((rhs // owners, width), F32 if m == 0 else BF16) for m in range(owners)
        )
    return pl.pallas_call(
        functools.partial(apply_kernel, pieces=len(pieces), parts=len(entries), plain=plain, leaf=leaf, unroll=8),
        out_shape=out_shape,
        in_specs=[smem] * 6 + [vmem] * (2 + len(pieces) + len(entries)),
        out_specs=(vmem,) * len(out_shape),
        scratch_shapes=[
            pltpu.VMEM((column_leaves, rhs, leaf), BF16),
            pltpu.VMEM((far_slots, rhs, rank), BF16),
            pltpu.VMEM((row_leaves, rhs, leaf), F32),
        ],
        compiler_params=pltpu.CompilerParams(vmem_limit_bytes=16 << 20),
        cost_estimate=pl.CostEstimate(flops=8_000_000_000, bytes_accessed=8 << 20, transcendentals=0),
        name="apply",
    )(table, source_fill, target_fill, far_source, far_target, far_rank, left, right, *pieces, *entries)


def shards(
    source_points, source_areas, source_fill, target_points, target_fill, charges, near_fill, near_source,
    near_target, far_source, far_target, far_rank, left_basis, right_basis, *, rows, columns,
):
    plain = charges.shape[0] % 8 != 0 or rows != 2 * columns
    if plain:
        pieces = [lax.all_gather(charges, "row", axis=0, tiled=True)]
    else:

        def swap(value, axis, size, mask):
            return lax.ppermute(value, axis, [(i, i ^ mask) for i in range(size)])

        pieces = [charges] + [swap(charges, "row", rows, mask) for mask in range(2, rows, 2)]
    *entries, table = make_entries(
        near_fill, near_source, near_target, source_points, source_areas, target_points,
        source_fill.shape[0], target_fill.shape[0],
    )
    if not plain:
        pieces, table = lax.optimization_barrier((pieces, table))
        pieces = pieces + [swap(piece, "row", rows, 1) for piece in pieces]
    outs = apply_blocks(
        table, source_fill, target_fill, far_source, far_target, far_rank, entries, left_basis[0], right_basis[0],
        pieces, columns, plain,
    )
    if plain:
        return lax.psum_scatter(outs[0], "col", scatter_dimension=0, tiled=True)
    result = outs[0]
    for mask in reversed(range(1, columns)):
        result = result + swap(outs[mask], "col", columns, mask).astype(F32)
    return result


def solution(mesh):
    placed = (
        P(None, "col"), P("col"), P("col"), P(None, "row"), P("row"), P("row", "col"), P("row", "col"),
        P("row", "col"), P("row", "col"), P("row", "col"), P("row", "col"), P("row", "col"),
        P("row", "col", None, None), P("row", "col", None, None),
    )
    return jax.shard_map(
        functools.partial(shards, rows=mesh.shape["row"], columns=mesh.shape["col"]),
        mesh=mesh, in_specs=placed, out_specs=P("col", "row"), check_vma=False,
    )
```

```python
import functools

import jax
import jax.numpy as jnp
from jax import lax
from jax.experimental import pallas as pl
from jax.experimental.pallas import tpu as pltpu
from jax.sharding import PartitionSpec as P

INV_FOUR_PI = 0.07957747154594767
SOFTENING_SQ = 0.0025
F32 = jnp.float32
BF16 = jnp.bfloat16
VMEM_LIMIT = 60 << 20


def split3(value):
    first = value.astype(BF16).astype(F32)
    rest = value - first
    second = rest.astype(BF16).astype(F32)
    return first, second, rest - second


def feature_rows(rows):
    count = rows[0].shape[1]
    index = lax.broadcasted_iota(jnp.int32, (8, count), 0)
    out = jnp.zeros((8, count), F32)
    for position, row in enumerate(rows):
        out = jnp.where(index == position, jnp.broadcast_to(row, (8, count)), out)
    return out


def part_count(slots):
    return 4 if slots % 32 == 0 else 1


def build_list(ids_ref, list_ref, half_id):
    slots = ids_ref.shape[1]
    square = (slots, slots)

    def across(row):
        return jnp.broadcast_to(row, square).T

    id_row = ids_ref[...].astype(F32)
    id_r = jnp.broadcast_to(id_row, square)
    lane = lax.broadcasted_iota(jnp.int32, square, 1)
    sub = lax.broadcasted_iota(jnp.int32, square, 0)
    same = jnp.where(id_r == across(id_row), 1.0, 0.0)
    count_r = jnp.sum(same, axis=0, keepdims=True)
    earlier_r = jnp.sum(jnp.where(sub < lane, same, 0.0), axis=0, keepdims=True)
    first_r = (earlier_r == 0.0) & (id_row >= 0.0)
    key_c = across(jnp.where(first_r, id_row, 1e9))
    rank_r = jnp.sum(jnp.where(key_c < id_r, 1.0, 0.0), axis=0, keepdims=True)
    rank_c = across(jnp.where(first_r, rank_r, -1.0))
    count_c = across(count_r)
    hit = rank_c == lane.astype(F32)
    list_r = jnp.sum(jnp.where(hit, key_c, 0.0), axis=0, keepdims=True)
    copies_r = jnp.sum(jnp.where(hit, count_c, 0.0), axis=0, keepdims=True)
    total = jnp.sum(jnp.where(first_r, 1.0, 0.0))
    half = jnp.sum(jnp.where(first_r & (id_row < float(half_id)), 1.0, 0.0))
    index = lax.broadcasted_iota(jnp.int32, (8, slots), 0)
    table = jnp.where(index == 0, jnp.broadcast_to(list_r, (8, slots)), 0.0)
    table = jnp.where(index == 1, jnp.broadcast_to(copies_r, (8, slots)), table)
    table = jnp.where(index == 2, total, table)
    table = jnp.where(index == 3, half, table)
    list_ref[...] = table.astype(jnp.int32)


def entries_kernel(*refs, column_leaves, row_leaves, leaf, parts):
    ids_ref, inputs, outputs, scratch = refs[0], refs[1:4], refs[4 : 5 + parts], refs[5 + parts :]
    entries_refs, list_ref = outputs[:-1], outputs[-1]
    copies, (s_ref, t_ref, table_ref, sem, in_sem) = scratch[:3], scratch[3:]
    loads = [pltpu.make_async_copy(src, dst, in_sem.at[i]) for i, (src, dst) in enumerate(zip(inputs, copies))]
    for load in loads:
        load.start()
    spts_ref, area_ref, tpts_ref = copies
    build_list(ids_ref, list_ref, (row_leaves // 2) * column_leaves)
    copy = pltpu.make_async_copy(list_ref, table_ref, sem)
    copy.start()
    for load in loads:
        load.wait()

    tx, ty, tz = (tpts_ref[i : i + 1, :] - 0.5 for i in range(3))
    norm = tx * tx + ty * ty + tz * tz
    h1, h2, h3 = split3(feature_rows([tx, ty, tz, jnp.ones_like(tx), norm]))
    features = jnp.concatenate([h1, h2, h1, h2, h3, h1, jnp.zeros((16,) + h1.shape[1:], F32)], axis=0).astype(BF16)
    for t in range(row_leaves):
        t_ref[t] = features[:, t * leaf : (t + 1) * leaf]

    sx, sy, sz = (spts_ref[i : i + 1, :] - 0.5 for i in range(3))
    scale = area_ref[...] * INV_FOUR_PI
    weight = 1.0 / (scale * scale)
    norm = sx * sx + sy * sy + sz * sz + SOFTENING_SQ
    g1, g2, g3 = split3(
        feature_rows([-2.0 * weight * sx, -2.0 * weight * sy, -2.0 * weight * sz, weight * norm, weight])
    )
    features = jnp.concatenate([g1, g1, g2, g2, g1, g3, jnp.zeros((16,) + g1.shape[1:], F32)], axis=0).astype(BF16)
    for s in range(column_leaves):
        column = features[:, s * leaf : (s + 1) * leaf].T
        s_ref[s] = jnp.concatenate([column, jnp.zeros((leaf, 128 - column.shape[1]), BF16)], axis=1)

    copy.wait()
    total = table_ref[2, 0]
    depth = t_ref.shape[1]

    def work(*accs):
        for acc in accs:
            pltpu.matmul_pop(acc)

        def drain(u, row):
            entries_refs[u % parts][row] = lax.rsqrt(pltpu.matmul_pop(accs[u])).astype(BF16)

        @pl.loop(0, (total + 7) // 8)
        def _(turn):
            for u in range(8):
                pair = table_ref[0, turn * 8 + u]
                rhs = jnp.concatenate([t_ref[pair // column_leaves], jnp.zeros((leaf - depth, leaf), BF16)], axis=0)
                lhs = jnp.concatenate([s_ref[pair % column_leaves], jnp.zeros((leaf, leaf - 128), BF16)], axis=1)
                stage = (u // 2) % 2
                pltpu.matmul_push_rhs(rhs, staging_register=stage, mxu_index=u % 2)
                pltpu.matmul_acc_lhs(accs[u], lhs, load_staged_rhs=stage)
                if u < 4:
                    drain(u + 4, jnp.maximum(turn * 2 - 1, 0))
                else:
                    drain(u - 4, turn * 2)

        for u in range(4, 8):
            drain(u, jnp.maximum((total + 7) // 8 * 2 - 1, 0))

    pl.run_scoped(work, *[pltpu.ACC(u % 2)((leaf, leaf), F32) for u in range(8)])


def make_entries(ids, source_points, source_areas, target_points, column_leaves, row_leaves):
    slots = ids.shape[1]
    leaf = source_points.shape[1] // column_leaves
    depth = 64
    vmem = pl.BlockSpec(memory_space=pltpu.VMEM)
    hbm = pl.BlockSpec(memory_space=pltpu.HBM)
    parts = part_count(slots)
    inputs = tuple(
        pltpu.with_memory_space_constraint(value, pltpu.HBM)
        for value in (source_points, source_areas[None, :], target_points)
    )
    return pl.pallas_call(
        functools.partial(
            entries_kernel, column_leaves=column_leaves, row_leaves=row_leaves, leaf=leaf, parts=parts
        ),
        out_shape=(pltpu.VMEM((slots // parts, leaf, leaf), BF16),) * parts
        + (jax.ShapeDtypeStruct((8, slots), jnp.int32),),
        in_specs=[vmem] + [hbm] * len(inputs),
        out_specs=(vmem,) * (parts + 1),
        scratch_shapes=[pltpu.VMEM(value.shape, value.dtype) for value in inputs]
        + [
            pltpu.VMEM((column_leaves, leaf, 128), BF16),
            pltpu.VMEM((row_leaves, depth, leaf), BF16),
            pltpu.SMEM((8, slots), jnp.int32),
            pltpu.SemaphoreType.DMA,
            pltpu.SemaphoreType.DMA((len(inputs),)),
        ],
        compiler_params=pltpu.CompilerParams(vmem_limit_bytes=16 << 20),
        cost_estimate=pl.CostEstimate(flops=8_000_000_000, bytes_accessed=1 << 20, transcendentals=0),
        name="entries",
    )(ids, *inputs)


def far_kernel(*refs, pieces, plain, leaf, unroll):
    (sfill_ref, fsrc_ref, ftgt_ref, frank_ref, left_ref, right_ref) = refs[:6]
    piece_refs = refs[6 : 6 + pieces]
    x_ref, acc_ref, coef_ref = refs[6 + pieces :]
    column_leaves, rhs, _ = x_ref.shape
    far_slots, rank, _ = left_ref.shape

    lane = lax.broadcasted_iota(jnp.int32, (rhs, leaf), 1)
    if not plain:
        parity = lax.rem(lax.axis_index("row"), 2)
    for s in range(column_leaves):
        window = slice(s * leaf, (s + 1) * leaf)
        if plain:
            block = piece_refs[0][:, window].astype(F32)
        else:
            rows = []
            for j in range(pieces // 2):
                mine = piece_refs[j][:, window].astype(F32)
                other = piece_refs[pieces // 2 + j][:, window].astype(F32)
                rows.append(jnp.where(parity == 0, mine, other))
                rows.append(jnp.where(parity == 0, other, mine))
            block = jnp.concatenate(rows, axis=0)
        x_ref[s] = jnp.where(lane < sfill_ref[s], block, 0.0).astype(BF16)

    acc_ref[...] = jnp.zeros_like(acc_ref)

    rank_lane = lax.broadcasted_iota(jnp.int32, (rhs, rank), 1)

    @pl.loop(0, far_slots // unroll)
    def _(turn):
        for u in range(unroll):
            k = turn * unroll + u
            coef = lax.dot_general(
                x_ref[fsrc_ref[0, k]], right_ref[k], (((1,), (1,)), ((), ())), preferred_element_type=F32
            )
            coef_ref[k] = jnp.where(rank_lane < frank_ref[0, k], coef, 0.0).astype(BF16)

    @pl.loop(0, far_slots // unroll)
    def _(turn):
        blocks = []
        for u in range(unroll):
            k = turn * unroll + u
            blocks.append(jnp.dot(coef_ref[k], left_ref[k], preferred_element_type=F32))
        for u in range(unroll):
            t = ftgt_ref[0, turn * unroll + u]
            acc_ref[t] = acc_ref[t] + blocks[u]


def near_kernel(*refs, parts, plain, leaf):
    (table_ref, tfill_ref, far_ref, x_ref) = refs[:4]
    entries_refs = refs[4 : 4 + parts]
    out_refs, acc_ref = refs[4 + parts : -1], refs[-1]
    row_leaves, rhs, _ = acc_ref.shape
    column_leaves = x_ref.shape[0]
    acc_ref[...] = jnp.zeros_like(acc_ref)
    total = table_ref[2, 0]
    trips = (total + 15) // 16

    def work(*accs):
        for acc in accs:
            pltpu.matmul_pop(acc)

        def drain(u, k):
            t = table_ref[0, k] // column_leaves
            copies = table_ref[1, k].astype(F32)
            block = pltpu.matmul_pop(accs[u])
            acc_ref[t] = acc_ref[t] + jnp.where(copies > 0.0, block * copies, 0.0)

        @pl.loop(0, trips)
        def _(turn):
            for u in range(16):
                source = table_ref[0, turn * 16 + u] % column_leaves
                stage = (u // 2) % 2
                entries = entries_refs[u % parts][turn * (16 // parts) + u // parts]
                pltpu.matmul_push_rhs(entries, staging_register=stage, mxu_index=u % 2)
                pltpu.matmul_acc_lhs(accs[u], x_ref[source], load_staged_rhs=stage)
                if u >= 8:
                    drain(u - 8, turn * 16 + u - 8)
                else:
                    drain(u + 8, jnp.maximum(turn * 16 + u - 8, u))

        @pl.when(trips > 0)
        def _():
            for u in range(8, 16):
                drain(u, trips * 16 - 16 + u)

    pl.run_scoped(work, *[pltpu.ACC(u % 2)((rhs, leaf), F32) for u in range(16)])

    if plain:
        lane_t = lax.broadcasted_iota(jnp.int32, (rhs, leaf), 1)
        for t in range(row_leaves):
            out_refs[0][:, t * leaf : (t + 1) * leaf] = jnp.where(lane_t < tfill_ref[t], acc_ref[t] + far_ref[t], 0.0)
    else:
        owners = len(out_refs)
        height = rhs // owners
        lane_t = lax.broadcasted_iota(jnp.int32, (height, leaf), 1)
        base = lax.axis_index("col") ^ (lax.axis_index("row") // 2)
        for m in range(owners):
            start = pl.multiple_of((base ^ m) * height, height)
            for t in range(row_leaves):
                value = acc_ref[t, pl.ds(start, height), :] + far_ref[t, pl.ds(start, height), :]
                value = jnp.where(lane_t < tfill_ref[t], value, 0.0)
                out_refs[m][:, t * leaf : (t + 1) * leaf] = value.astype(out_refs[m].dtype)


def far_field(source_fill, row_leaves, far_source, far_target, far_rank, left, right, pieces, plain):
    column_leaves = source_fill.shape[0]
    far_slots, rank, leaf = left.shape
    rhs = sum(p.shape[0] for p in pieces)
    vmem = pl.BlockSpec(memory_space=pltpu.VMEM)
    smem = pl.BlockSpec(memory_space=pltpu.SMEM)
    unroll = next(u for u in (32, 16, 8, 4, 2, 1) if far_slots % u == 0)
    return pl.pallas_call(
        functools.partial(far_kernel, pieces=len(pieces), plain=plain, leaf=leaf, unroll=unroll),
        out_shape=(pltpu.VMEM((column_leaves, rhs, leaf), BF16), pltpu.VMEM((row_leaves, rhs, leaf), F32)),
        in_specs=[smem] * 4 + [vmem] * (2 + len(pieces)),
        out_specs=(vmem, vmem),
        scratch_shapes=[pltpu.VMEM((far_slots, rhs, rank), BF16)],
        compiler_params=pltpu.CompilerParams(vmem_limit_bytes=12 << 20),
        cost_estimate=pl.CostEstimate(flops=2_000_000_000, bytes_accessed=8 << 20, transcendentals=0),
        name="far",
    )(source_fill, far_source, far_target, far_rank, left, right, *pieces)


def near_field(table, target_fill, far, x, entries, owners, plain):
    row_leaves, rhs, leaf = far.shape
    vmem = pl.BlockSpec(memory_space=pltpu.VMEM)
    smem = pl.BlockSpec(memory_space=pltpu.SMEM)
    width = row_leaves * leaf
    if plain:
        out_shape = (jax.ShapeDtypeStruct((rhs, width), F32),)
    else:
        out_shape = tuple(
            jax.ShapeDtypeStruct((rhs // owners, width), F32 if m == 0 else BF16) for m in range(owners)
        )
    return pl.pallas_call(
        functools.partial(near_kernel, parts=len(entries), plain=plain, leaf=leaf),
        out_shape=out_shape,
        in_specs=[smem] * 2 + [vmem] * (2 + len(entries)),
        out_specs=(vmem,) * len(out_shape),
        scratch_shapes=[pltpu.VMEM((row_leaves, rhs, leaf), F32)],
        compiler_params=pltpu.CompilerParams(vmem_limit_bytes=12 << 20),
        cost_estimate=pl.CostEstimate(flops=4_000_000_000, bytes_accessed=8 << 20, transcendentals=0),
        name="near",
    )(table, target_fill, far, x, *entries)


def shards(
    source_points, source_areas, source_fill, target_points, target_fill, charges, near_fill, near_source,
    near_target, far_source, far_target, far_rank, left_basis, right_basis, *, rows, columns,
):
    plain = charges.shape[0] % 8 != 0 or rows != 2 * columns
    if plain:
        pieces = [lax.all_gather(charges, "row", axis=0, tiled=True)]
    else:

        def swap(value, axis, size, mask):
            return lax.ppermute(value, axis, [(i, i ^ mask) for i in range(size)])

        pieces = [charges] + [swap(charges, "row", rows, mask) for mask in range(2, rows, 2)]
    used = jnp.arange(near_source.shape[1])[None, :] < near_fill
    ids = jnp.where(used, near_target * source_fill.shape[0] + near_source, -1)
    *entries, table = make_entries(
        ids, source_points, source_areas, target_points, source_fill.shape[0], target_fill.shape[0]
    )
    if not plain:
        pieces, table = lax.optimization_barrier((pieces, table))
        pieces = pieces + [swap(piece, "row", rows, 1) for piece in pieces]
    x, far = far_field(
        source_fill, target_fill.shape[0], far_source, far_target, far_rank, left_basis[0], right_basis[0],
        pieces, plain,
    )
    outs = near_field(table, target_fill, far, x, entries, columns, plain)
    if plain:
        return lax.psum_scatter(outs[0], "col", scatter_dimension=0, tiled=True)
    result = outs[0]
    for mask in reversed(range(1, columns)):
        result = result + swap(outs[mask], "col", columns, mask).astype(F32)
    return result


def solution(mesh):
    placed = (
        P(None, "col"), P("col"), P("col"), P(None, "row"), P("row"), P("row", "col"), P("row", "col"),
        P("row", "col"), P("row", "col"), P("row", "col"), P("row", "col"), P("row", "col"),
        P("row", "col", None, None), P("row", "col", None, None),
    )
    return jax.shard_map(
        functools.partial(shards, rows=mesh.shape["row"], columns=mesh.shape["col"]),
        mesh=mesh, in_specs=placed, out_specs=P("col", "row"), check_vma=False,
    )
```

```python
import functools

import jax
import jax.numpy as jnp
from jax import lax
from jax.experimental import pallas as pl
from jax.experimental.pallas import tpu as pltpu
from jax.sharding import PartitionSpec as P


INV_FOUR_PI = 0.07957747154594767
SOFTENING_SQ = 0.0025
F32 = jnp.float32
BF16 = jnp.bfloat16


def split3(value):
    first = value.astype(BF16).astype(F32)
    rest = value - first
    second = rest.astype(BF16).astype(F32)
    return first, second, rest - second


def feature_rows(rows):
    count = rows[0].shape[1]
    index = lax.broadcasted_iota(jnp.int32, (8, count), 0)
    out = jnp.zeros((8, count), F32)
    for position, row in enumerate(rows):
        out = jnp.where(index == position, jnp.broadcast_to(row, (8, count)), out)
    return out


def build_list(ids_ref, list_ref, half_id):
    slots = ids_ref.shape[1]
    square = (slots, slots)

    def across(row):
        return jnp.broadcast_to(row, square).T

    id_row = ids_ref[...].astype(F32)
    id_r = jnp.broadcast_to(id_row, square)
    lane = lax.broadcasted_iota(jnp.int32, square, 1)
    sub = lax.broadcasted_iota(jnp.int32, square, 0)
    same = jnp.where(id_r == across(id_row), 1.0, 0.0)
    count_r = jnp.sum(same, axis=0, keepdims=True)
    earlier_r = jnp.sum(jnp.where(sub < lane, same, 0.0), axis=0, keepdims=True)
    first_r = (earlier_r == 0.0) & (id_row >= 0.0)
    key_c = across(jnp.where(first_r, id_row, 1e9))
    rank_r = jnp.sum(jnp.where(key_c < id_r, 1.0, 0.0), axis=0, keepdims=True)
    rank_c = across(jnp.where(first_r, rank_r, -1.0))
    count_c = across(count_r)
    hit = rank_c == lane.astype(F32)
    list_r = jnp.sum(jnp.where(hit, key_c, 0.0), axis=0, keepdims=True)
    copies_r = jnp.sum(jnp.where(hit, count_c, 0.0), axis=0, keepdims=True)
    total = jnp.sum(jnp.where(first_r, 1.0, 0.0))
    half = jnp.sum(jnp.where(first_r & (id_row < float(half_id)), 1.0, 0.0))
    index = lax.broadcasted_iota(jnp.int32, (8, slots), 0)
    table = jnp.where(index == 0, jnp.broadcast_to(list_r, (8, slots)), 0.0)
    table = jnp.where(index == 1, jnp.broadcast_to(copies_r, (8, slots)), table)
    table = jnp.where(index == 2, total, table)
    table = jnp.where(index == 3, half, table)
    list_ref[...] = table.astype(jnp.int32)


def entry_loop(table_ref, s_ref, t_ref, entries_refs, first, last):
    parts = len(entries_refs)
    column_leaves, leaf, width = s_ref.shape
    depth = t_ref.shape[1]
    rows = 8 // parts
    trips = (last - first + 7) // 8

    def work(*accs):
        for acc in accs:
            pltpu.matmul_pop(acc)

        def drain(u, turn):
            row = jnp.maximum(turn * rows + u // parts, 0)
            entries_refs[u % parts][row] = lax.rsqrt(pltpu.matmul_pop(accs[u])).astype(BF16)

        @pl.loop(0, trips)
        def _(turn):
            for u in range(8):
                pair = table_ref[0, first + turn * 8 + u]
                rhs = jnp.concatenate([t_ref[pair // column_leaves], jnp.zeros((leaf - depth, leaf), BF16)], axis=0)
                lhs = jnp.concatenate([s_ref[pair % column_leaves], jnp.zeros((leaf, leaf - width), BF16)], axis=1)
                stage = (u // 2) % 2
                pltpu.matmul_push_rhs(rhs, staging_register=stage, mxu_index=u % 2)
                pltpu.matmul_acc_lhs(accs[u], lhs, load_staged_rhs=stage)
                if u < 4:
                    drain(u + 4, turn - 1)
                else:
                    drain(u - 4, turn)

        for u in range(4, 8):
            drain(u, trips - 1)

    pl.run_scoped(work, *[pltpu.ACC(u % 2)((leaf, leaf), F32) for u in range(8)])


def first_entries_kernel(*refs, column_leaves, row_leaves, leaf, parts):
    ids_ref, inputs, outputs, scratch = refs[0], refs[1:4], refs[4 : 7 + parts], refs[7 + parts :]
    entries_refs, (table_ref, s_ref, t_ref) = outputs[:parts], outputs[parts:]
    copies, (list_ref, sem, in_sem) = scratch[:3], scratch[3:]
    loads = [pltpu.make_async_copy(src, dst, in_sem.at[i]) for i, (src, dst) in enumerate(zip(inputs, copies))]
    for load in loads:
        load.start()
    spts_ref, area_ref, tpts_ref = copies
    build_list(ids_ref, list_ref, (row_leaves // 2) * column_leaves)
    copy = pltpu.make_async_copy(list_ref, table_ref, sem)
    copy.start()
    for load in loads:
        load.wait()

    tx, ty, tz = (tpts_ref[i : i + 1, :] - 0.5 for i in range(3))
    norm = tx * tx + ty * ty + tz * tz
    h1, h2, h3 = split3(feature_rows([tx, ty, tz, jnp.ones_like(tx), norm]))
    features = jnp.concatenate([h1, h2, h1, h2, h3, h1, jnp.zeros((16,) + h1.shape[1:], F32)], axis=0).astype(BF16)
    for t in range(row_leaves):
        t_ref[t] = features[:, t * leaf : (t + 1) * leaf]

    sx, sy, sz = (spts_ref[i : i + 1, :] - 0.5 for i in range(3))
    scale = area_ref[...] * INV_FOUR_PI
    weight = 1.0 / (scale * scale)
    norm = sx * sx + sy * sy + sz * sz + SOFTENING_SQ
    g1, g2, g3 = split3(
        feature_rows([-2.0 * weight * sx, -2.0 * weight * sy, -2.0 * weight * sz, weight * norm, weight])
    )
    features = jnp.concatenate([g1, g1, g2, g2, g1, g3, jnp.zeros((16,) + g1.shape[1:], F32)], axis=0).astype(BF16)
    for s in range(column_leaves):
        column = features[:, s * leaf : (s + 1) * leaf].T
        s_ref[s] = jnp.concatenate([column, jnp.zeros((leaf, 128 - column.shape[1]), BF16)], axis=1)

    copy.wait()
    group = parts * entries_refs[0].shape[0]
    entry_loop(table_ref, s_ref, t_ref, entries_refs, 0, jnp.minimum(table_ref[2, 0], group))


def second_entries_kernel(table_ref, s_ref, t_ref, *entries_refs):
    first = table_ref.shape[1] - len(entries_refs) * entries_refs[0].shape[0]
    entry_loop(table_ref, s_ref, t_ref, entries_refs, first, jnp.maximum(table_ref[2, 0], first))


VMEM = pl.BlockSpec(memory_space=pltpu.VMEM)
SMEM = pl.BlockSpec(memory_space=pltpu.SMEM)
HBM = pl.BlockSpec(memory_space=pltpu.HBM)


def first_entries(ids, source_points, source_areas, target_points, column_leaves, row_leaves):
    slots = ids.shape[1]
    leaf = source_points.shape[1] // column_leaves
    depth = 64
    inputs = tuple(
        pltpu.with_memory_space_constraint(value, pltpu.HBM)
        for value in (source_points, source_areas[None, :], target_points)
    )
    return pl.pallas_call(
        functools.partial(
            first_entries_kernel, column_leaves=column_leaves, row_leaves=row_leaves, leaf=leaf, parts=2
        ),
        out_shape=(pltpu.VMEM((slots // 4, leaf, leaf), BF16),) * 2
        + (
            pltpu.SMEM((8, slots), jnp.int32),
            pltpu.VMEM((column_leaves, leaf, 128), BF16),
            pltpu.VMEM((row_leaves, depth, leaf), BF16),
        ),
        in_specs=[VMEM] + [HBM] * len(inputs),
        out_specs=(VMEM, VMEM, SMEM, VMEM, VMEM),
        scratch_shapes=[pltpu.VMEM(value.shape, value.dtype) for value in inputs]
        + [pltpu.VMEM((8, slots), jnp.int32), pltpu.SemaphoreType.DMA, pltpu.SemaphoreType.DMA((len(inputs),))],
        compiler_params=pltpu.CompilerParams(vmem_limit_bytes=10 << 20),
        cost_estimate=pl.CostEstimate(flops=8_000_000_000, bytes_accessed=1 << 20, transcendentals=0),
        name="entries",
    )(ids, *inputs)


def second_entries(table, s_features, t_features):
    slots = table.shape[1]
    leaf = s_features.shape[1]
    return pl.pallas_call(
        second_entries_kernel,
        out_shape=(pltpu.VMEM((slots // 4, leaf, leaf), BF16),) * 2,
        in_specs=[SMEM, VMEM, VMEM],
        out_specs=(VMEM, VMEM),
        compiler_params=pltpu.CompilerParams(vmem_limit_bytes=4 << 20),
        cost_estimate=pl.CostEstimate(flops=8_000_000_000, bytes_accessed=1 << 20, transcendentals=0),
        name="entries_rest",
    )(table, s_features, t_features)


def far_kernel(*refs, pieces, plain, leaf, unroll):
    (sfill_ref, fsrc_ref, ftgt_ref, frank_ref, left_ref, right_ref) = refs[:6]
    piece_refs = refs[6 : 6 + pieces]
    x_ref, acc_ref, coef_ref = refs[6 + pieces :]
    column_leaves, rhs, _ = x_ref.shape
    far_slots, rank, _ = left_ref.shape

    lane = lax.broadcasted_iota(jnp.int32, (rhs, leaf), 1)
    if not plain:
        parity = lax.rem(lax.axis_index("row"), 2)
    for s in range(column_leaves):
        window = slice(s * leaf, (s + 1) * leaf)
        if plain:
            block = piece_refs[0][:, window].astype(F32)
        else:
            rows = []
            for j in range(pieces // 2):
                mine = piece_refs[j][:, window].astype(F32)
                other = piece_refs[pieces // 2 + j][:, window].astype(F32)
                rows.append(jnp.where(parity == 0, mine, other))
                rows.append(jnp.where(parity == 0, other, mine))
            block = jnp.concatenate(rows, axis=0)
        x_ref[s] = jnp.where(lane < sfill_ref[s], block, 0.0).astype(BF16)

    acc_ref[...] = jnp.zeros_like(acc_ref)

    rank_lane = lax.broadcasted_iota(jnp.int32, (rhs, rank), 1)

    @pl.loop(0, far_slots // unroll)
    def _(turn):
        for u in range(unroll):
            k = turn * unroll + u
            coef = lax.dot_general(
                x_ref[fsrc_ref[0, k]], right_ref[k], (((1,), (1,)), ((), ())), preferred_element_type=F32
            )
            coef_ref[k] = jnp.where(rank_lane < frank_ref[0, k], coef, 0.0).astype(BF16)

    @pl.loop(0, far_slots // unroll)
    def _(turn):
        blocks = []
        for u in range(unroll):
            k = turn * unroll + u
            blocks.append(jnp.dot(coef_ref[k], left_ref[k], preferred_element_type=F32))
        for u in range(unroll):
            t = ftgt_ref[0, turn * unroll + u]
            acc_ref[t] = acc_ref[t] + blocks[u]


def near_kernel(*refs, groups, chunk, chunks, plain):
    (table_ref, tfill_ref, far_ref, x_ref) = refs[:4]
    entries_refs = refs[4 : 4 + 2 * groups]
    carried = 1 if chunk > 0 and not plain else 0
    carried_refs = refs[4 + 2 * groups : 4 + 2 * groups + carried]
    out_refs, acc_ref = refs[4 + 2 * groups + carried : -1], refs[-1]
    chunk_leaves, rhs, leaf = acc_ref.shape
    column_leaves = x_ref.shape[0]
    base_leaf = chunk * chunk_leaves
    group = table_ref.shape[1] // groups
    total, half = table_ref[2, 0], table_ref[3, 0]
    low = half if chunk > 0 else 0
    high = total if chunk == chunks - 1 else half
    acc_ref[...] = jnp.zeros_like(acc_ref)

    def work(*accs):
        for acc in accs:
            pltpu.matmul_pop(acc)

        def drain(u, k):
            inside = (k >= low) & (k < high)
            slot = jnp.maximum(k, 0)
            t = jnp.clip(table_ref[0, slot] // column_leaves - base_leaf, 0, chunk_leaves - 1)
            copies = jnp.where(inside, table_ref[1, slot], 0).astype(F32)
            block = pltpu.matmul_pop(accs[u])
            acc_ref[t] = acc_ref[t] + jnp.where(inside, block * copies, 0.0)

        for g in range(groups):
            pair_refs = entries_refs[2 * g : 2 * g + 2]
            start = jnp.clip(low, g * group, (g + 1) * group) // 16
            stop = (jnp.clip(high, g * group, (g + 1) * group) + 15) // 16

            @pl.loop(start, stop)
            def _(turn):
                for u in range(16):
                    k = turn * 16 + u
                    source = table_ref[0, k] % column_leaves
                    stage = (u // 2) % 2
                    entries = pair_refs[u % 2][turn * 8 - g * (group // 2) + u // 2]
                    pltpu.matmul_push_rhs(entries, staging_register=stage, mxu_index=u % 2)
                    pltpu.matmul_acc_lhs(accs[u], x_ref[source], load_staged_rhs=stage)
                    if u >= 8:
                        drain(u - 8, k - 8)
                    else:
                        drain(u + 8, k - 8)

        end = (high + 15) // 16 * 16
        for u in range(8, 16):
            drain(u, end - 16 + u)

    pl.run_scoped(work, *[pltpu.ACC(u % 2)((rhs, leaf), F32) for u in range(16)])

    if plain:
        lane_t = lax.broadcasted_iota(jnp.int32, (rhs, leaf), 1)
        for t in range(chunk_leaves):
            value = acc_ref[t] + far_ref[base_leaf + t]
            out_refs[0][:, t * leaf : (t + 1) * leaf] = jnp.where(lane_t < tfill_ref[base_leaf + t], value, 0.0)
    else:
        owners = len(out_refs)
        height = rhs // owners
        lane_t = lax.broadcasted_iota(jnp.int32, (height, leaf), 1)
        base = lax.axis_index("col") ^ (lax.axis_index("row") // 2)
        for m in range(owners):
            start = pl.multiple_of((base ^ m) * height, height)
            shift = out_refs[m].shape[1] - chunk_leaves * leaf
            if shift:
                out_refs[m][:, :shift] = carried_refs[0][...]
            for t in range(chunk_leaves):
                value = acc_ref[t, pl.ds(start, height), :] + far_ref[base_leaf + t, pl.ds(start, height), :]
                value = jnp.where(lane_t < tfill_ref[base_leaf + t], value, 0.0)
                window = slice(shift + t * leaf, shift + (t + 1) * leaf)
                out_refs[m][:, window] = value.astype(out_refs[m].dtype)


def far_field(source_fill, row_leaves, far_source, far_target, far_rank, left, right, pieces, plain):
    column_leaves = source_fill.shape[0]
    far_slots, rank, leaf = left.shape
    rhs = sum(p.shape[0] for p in pieces)
    vmem = pl.BlockSpec(memory_space=pltpu.VMEM)
    smem = pl.BlockSpec(memory_space=pltpu.SMEM)
    unroll = next(u for u in (32, 16, 8, 4, 2, 1) if far_slots % u == 0)
    return pl.pallas_call(
        functools.partial(far_kernel, pieces=len(pieces), plain=plain, leaf=leaf, unroll=unroll),
        out_shape=(pltpu.VMEM((column_leaves, rhs, leaf), BF16), pltpu.VMEM((row_leaves, rhs, leaf), F32)),
        in_specs=[smem] * 4 + [vmem] * (2 + len(pieces)),
        out_specs=(vmem, vmem),
        scratch_shapes=[pltpu.VMEM((far_slots, rhs, rank), BF16)],
        compiler_params=pltpu.CompilerParams(vmem_limit_bytes=12 << 20),
        cost_estimate=pl.CostEstimate(flops=2_000_000_000, bytes_accessed=8 << 20, transcendentals=0),
        name="far",
    )(source_fill, far_source, far_target, far_rank, left, right, *pieces)


def near_field(table, target_fill, far, x, entries, owners, plain, chunk, chunks, carried=()):
    row_leaves, rhs, leaf = far.shape
    width = row_leaves // chunks * leaf
    if plain:
        out_shape = (jax.ShapeDtypeStruct((rhs, width), F32),)
    else:
        out_shape = tuple(
            jax.ShapeDtypeStruct(
                (rhs // owners, width + (carried[0].shape[1] if m == 1 and carried else 0)), F32 if m == 0 else BF16
            )
            for m in range(owners)
        )
    return pl.pallas_call(
        functools.partial(near_kernel, groups=len(entries) // 2, chunk=chunk, chunks=chunks, plain=plain),
        out_shape=out_shape,
        in_specs=[SMEM] * 2 + [VMEM] * (2 + len(entries) + len(carried)),
        out_specs=(VMEM,) * len(out_shape),
        scratch_shapes=[pltpu.VMEM((row_leaves // chunks, rhs, leaf), F32)],
        compiler_params=pltpu.CompilerParams(vmem_limit_bytes=4 << 20),
        cost_estimate=pl.CostEstimate(flops=4_000_000_000, bytes_accessed=8 << 20, transcendentals=0),
        name="near",
    )(table, target_fill, far, x, *entries, *carried)


def shards(
    source_points, source_areas, source_fill, target_points, target_fill, charges, near_fill, near_source,
    near_target, far_source, far_target, far_rank, left_basis, right_basis, *, rows, columns,
):
    plain = charges.shape[0] % 8 != 0 or rows != 2 * columns
    if plain:
        pieces = [lax.all_gather(charges, "row", axis=0, tiled=True)]
    else:

        def swap(value, axis, size, mask):
            return lax.ppermute(value, axis, [(i, i ^ mask) for i in range(size)])

        pieces = [charges] + [swap(charges, "row", rows, mask) for mask in range(2, rows, 2)]
    used = jnp.arange(near_source.shape[1])[None, :] < near_fill
    ids = jnp.where(used, near_target * source_fill.shape[0] + near_source, -1)
    row_leaves = target_fill.shape[0]
    *entries, table, s_features, t_features = first_entries(
        ids, source_points, source_areas, target_points, source_fill.shape[0], row_leaves
    )
    if not plain:
        pieces, table = lax.optimization_barrier((pieces, table))
        pieces = pieces + [swap(piece, "row", rows, 1) for piece in pieces]
    entries = entries + list(second_entries(table, s_features, t_features))
    if not plain:
        pieces, entries[-1] = lax.optimization_barrier((pieces, entries[-1]))
    x, far = far_field(
        source_fill, row_leaves, far_source, far_target, far_rank, left_basis[0], right_basis[0], pieces, plain
    )
    if plain or row_leaves % 2 or columns < 3:
        outs = near_field(table, target_fill, far, x, entries, columns, plain, 0, 1)
        if plain:
            return lax.psum_scatter(outs[0], "col", scatter_dimension=0, tiled=True)
        result = outs[0]
        for mask in reversed(range(1, columns)):
            result = result + swap(outs[mask], "col", columns, mask).astype(F32)
        return result

    def exchange(value, mask):
        return swap(value, "col", columns, mask)

    first = near_field(table, target_fill, far, x, entries, columns, plain, 0, 2)
    early = [exchange(first[mask], mask) for mask in reversed(range(2, columns))]
    second = near_field(table, target_fill, far, x, entries, columns, plain, 1, 2, (first[1],))
    neighbour = exchange(second[1], 1)
    late = [exchange(second[mask], mask) for mask in reversed(range(2, columns))]
    result = jnp.concatenate([first[0], second[0]], axis=1) + neighbour.astype(F32)
    for a, b in zip(early, late):
        result = result + jnp.concatenate([a, b], axis=1).astype(F32)
    return result


def solution(mesh):
    placed = (
        P(None, "col"), P("col"), P("col"), P(None, "row"), P("row"), P("row", "col"), P("row", "col"),
        P("row", "col"), P("row", "col"), P("row", "col"), P("row", "col"), P("row", "col"),
        P("row", "col", None, None), P("row", "col", None, None),
    )
    return jax.shard_map(
        functools.partial(shards, rows=mesh.shape["row"], columns=mesh.shape["col"]),
        mesh=mesh, in_specs=placed, out_specs=P("col", "row"), check_vma=False,
    )
```

```python
import functools

import jax
import jax.numpy as jnp
from jax import lax
from jax.experimental import pallas as pl
from jax.experimental.pallas import tpu as pltpu
from jax.sharding import PartitionSpec as P


INV_FOUR_PI = 0.07957747154594767
SOFTENING_SQ = 0.0025
F32 = jnp.float32
BF16 = jnp.bfloat16


def split3(value):
    first = value.astype(BF16).astype(F32)
    rest = value - first
    second = rest.astype(BF16).astype(F32)
    return first, second, rest - second


def feature_rows(rows):
    count = rows[0].shape[1]
    index = lax.broadcasted_iota(jnp.int32, (8, count), 0)
    out = jnp.zeros((8, count), F32)
    for position, row in enumerate(rows):
        out = jnp.where(index == position, jnp.broadcast_to(row, (8, count)), out)
    return out


def build_list(id_row, list_ref, half_id):
    slots = id_row.shape[1]
    square = (slots, slots)

    def across(row):
        return jnp.broadcast_to(row, square).T

    id_row = id_row.astype(F32)
    id_r = jnp.broadcast_to(id_row, square)
    lane = lax.broadcasted_iota(jnp.int32, square, 1)
    sub = lax.broadcasted_iota(jnp.int32, square, 0)
    same = jnp.where(id_r == across(id_row), 1.0, 0.0)
    count_r = jnp.sum(same, axis=0, keepdims=True)
    earlier_r = jnp.sum(jnp.where(sub < lane, same, 0.0), axis=0, keepdims=True)
    first_r = (earlier_r == 0.0) & (id_row >= 0.0)
    key_c = across(jnp.where(first_r, id_row, 1e9))
    rank_r = jnp.sum(jnp.where(key_c < id_r, 1.0, 0.0), axis=0, keepdims=True)
    rank_c = across(jnp.where(first_r, rank_r, -1.0))
    count_c = across(count_r)
    hit = rank_c == lane.astype(F32)
    list_r = jnp.sum(jnp.where(hit, key_c, 0.0), axis=0, keepdims=True)
    copies_r = jnp.sum(jnp.where(hit, count_c, 0.0), axis=0, keepdims=True)
    total = jnp.sum(jnp.where(first_r, 1.0, 0.0))
    half = jnp.sum(jnp.where(first_r & (id_row < float(half_id)), 1.0, 0.0))
    index = lax.broadcasted_iota(jnp.int32, (8, slots), 0)
    table = jnp.where(index == 0, jnp.broadcast_to(list_r, (8, slots)), 0.0)
    table = jnp.where(index == 1, jnp.broadcast_to(copies_r, (8, slots)), table)
    table = jnp.where(index == 2, total, table)
    table = jnp.where(index == 3, half, table)
    list_ref[...] = table.astype(jnp.int32)


def entry_loop(table_ref, s_ref, t_ref, entries_refs, first, last):
    parts = len(entries_refs)
    column_leaves, leaf, width = s_ref.shape
    depth = t_ref.shape[1]
    rows = 8 // parts
    trips = (last - first + 7) // 8

    def work(*accs):
        for acc in accs:
            pltpu.matmul_pop(acc)

        def drain(u, turn):
            row = jnp.maximum(turn * rows + u // parts, 0)
            entries_refs[u % parts][row] = lax.rsqrt(pltpu.matmul_pop(accs[u])).astype(BF16)

        @pl.loop(0, trips)
        def _(turn):
            for u in range(8):
                pair = table_ref[0, first + turn * 8 + u]
                rhs = jnp.concatenate([t_ref[pair // column_leaves], jnp.zeros((leaf - depth, leaf), BF16)], axis=0)
                lhs = jnp.concatenate([s_ref[pair % column_leaves], jnp.zeros((leaf, leaf - width), BF16)], axis=1)
                stage = (u // 2) % 2
                pltpu.matmul_push_rhs(rhs, staging_register=stage, mxu_index=u % 2)
                pltpu.matmul_acc_lhs(accs[u], lhs, load_staged_rhs=stage)
                if u < 4:
                    drain(u + 4, turn - 1)
                else:
                    drain(u - 4, turn)

        for u in range(4, 8):
            drain(u, trips - 1)

    pl.run_scoped(work, *[pltpu.ACC(u % 2)((leaf, leaf), F32) for u in range(8)])


def first_entries_kernel(*refs, column_leaves, row_leaves, leaf, parts, indices):
    fill_ref, inputs, index_inputs = refs[0], refs[1:6], refs[6 : 6 + indices]
    outputs, scratch = refs[6 + indices : 9 + parts + 2 * indices], refs[9 + parts + 2 * indices :]
    entries_refs, (table_ref, s_ref, t_ref), index_outputs = outputs[:parts], outputs[parts : parts + 3], outputs[parts + 3 :]
    copies, (list_ref, sem, in_sem) = scratch[:5], scratch[5:]
    moves = list(zip(inputs, copies)) + list(zip(index_inputs, index_outputs))
    loads = [pltpu.make_async_copy(src, dst, in_sem.at[i]) for i, (src, dst) in enumerate(moves)]
    for load in loads:
        load.start()
    nsrc_ref, ntgt_ref, spts_ref, area_ref, tpts_ref = copies
    for load in loads[:2]:
        load.wait()
    used = lax.broadcasted_iota(jnp.int32, nsrc_ref.shape, 1) < fill_ref[0, 0]
    ids = jnp.where(used, ntgt_ref[...] * column_leaves + nsrc_ref[...], -1)
    build_list(ids, list_ref, (row_leaves // 2) * column_leaves)
    copy = pltpu.make_async_copy(list_ref, table_ref, sem)
    copy.start()
    for load in loads[2:]:
        load.wait()

    tx, ty, tz = (tpts_ref[i : i + 1, :] - 0.5 for i in range(3))
    norm = tx * tx + ty * ty + tz * tz
    h1, h2, h3 = split3(feature_rows([tx, ty, tz, jnp.ones_like(tx), norm]))
    features = jnp.concatenate([h1, h2, h1, h2, h3, h1, jnp.zeros((16,) + h1.shape[1:], F32)], axis=0).astype(BF16)
    for t in range(row_leaves):
        t_ref[t] = features[:, t * leaf : (t + 1) * leaf]

    sx, sy, sz = (spts_ref[i : i + 1, :] - 0.5 for i in range(3))
    scale = area_ref[...] * INV_FOUR_PI
    weight = 1.0 / (scale * scale)
    norm = sx * sx + sy * sy + sz * sz + SOFTENING_SQ
    g1, g2, g3 = split3(
        feature_rows([-2.0 * weight * sx, -2.0 * weight * sy, -2.0 * weight * sz, weight * norm, weight])
    )
    features = jnp.concatenate([g1, g1, g2, g2, g1, g3, jnp.zeros((16,) + g1.shape[1:], F32)], axis=0).astype(BF16)
    for s in range(column_leaves):
        column = features[:, s * leaf : (s + 1) * leaf].T
        s_ref[s] = jnp.concatenate([column, jnp.zeros((leaf, 128 - column.shape[1]), BF16)], axis=1)

    copy.wait()
    group = parts * entries_refs[0].shape[0]
    entry_loop(table_ref, s_ref, t_ref, entries_refs, 0, jnp.minimum(table_ref[2, 0], group))


def second_entries_kernel(table_ref, s_ref, t_ref, *entries_refs):
    first = table_ref.shape[1] - len(entries_refs) * entries_refs[0].shape[0]
    entry_loop(table_ref, s_ref, t_ref, entries_refs, first, jnp.maximum(table_ref[2, 0], first))


VMEM = pl.BlockSpec(memory_space=pltpu.VMEM)
SMEM = pl.BlockSpec(memory_space=pltpu.SMEM)
HBM = pl.BlockSpec(memory_space=pltpu.HBM)


def first_entries(near_fill, near_source, near_target, source_points, source_areas, target_points, indices, leaves):
    column_leaves, row_leaves = leaves
    slots = near_source.shape[1]
    leaf = source_points.shape[1] // column_leaves
    depth = 64
    inputs = (near_source, near_target, source_points, source_areas[None, :], target_points)
    hbm_inputs = tuple(pltpu.with_memory_space_constraint(value, pltpu.HBM) for value in inputs + tuple(indices))
    return pl.pallas_call(
        functools.partial(
            first_entries_kernel, column_leaves=column_leaves, row_leaves=row_leaves, leaf=leaf, parts=2,
            indices=len(indices),
        ),
        out_shape=(pltpu.VMEM((slots // 4, leaf, leaf), BF16),) * 2
        + (
            pltpu.SMEM((8, slots), jnp.int32),
            pltpu.VMEM((column_leaves, leaf, 128), BF16),
            pltpu.VMEM((row_leaves, depth, leaf), BF16),
        )
        + tuple(pltpu.SMEM(value.shape, jnp.int32) for value in indices),
        in_specs=[SMEM] + [HBM] * len(hbm_inputs),
        out_specs=(VMEM, VMEM, SMEM, VMEM, VMEM) + (SMEM,) * len(indices),
        scratch_shapes=[pltpu.VMEM(value.shape, value.dtype) for value in inputs]
        + [pltpu.VMEM((8, slots), jnp.int32), pltpu.SemaphoreType.DMA, pltpu.SemaphoreType.DMA((len(hbm_inputs),))],
        compiler_params=pltpu.CompilerParams(vmem_limit_bytes=10 << 20),
        cost_estimate=pl.CostEstimate(flops=8_000_000_000, bytes_accessed=1 << 20, transcendentals=0),
        name="entries",
    )(near_fill, *hbm_inputs)


def second_entries(table, s_features, t_features):
    slots = table.shape[1]
    leaf = s_features.shape[1]
    return pl.pallas_call(
        second_entries_kernel,
        out_shape=(pltpu.VMEM((slots // 4, leaf, leaf), BF16),) * 2,
        in_specs=[SMEM, VMEM, VMEM],
        out_specs=(VMEM, VMEM),
        compiler_params=pltpu.CompilerParams(vmem_limit_bytes=4 << 20),
        cost_estimate=pl.CostEstimate(flops=8_000_000_000, bytes_accessed=1 << 20, transcendentals=0),
        name="entries_rest",
    )(table, s_features, t_features)


def far_kernel(*refs, pieces, plain, leaf, unroll):
    (sfill_ref, fsrc_ref, ftgt_ref, frank_ref, left_ref, right_ref) = refs[:6]
    piece_refs = refs[6 : 6 + pieces]
    x_ref, acc_ref, coef_ref = refs[6 + pieces :]
    column_leaves, rhs, _ = x_ref.shape
    far_slots, rank, _ = left_ref.shape

    lane = lax.broadcasted_iota(jnp.int32, (rhs, leaf), 1)
    if not plain:
        parity = lax.rem(lax.axis_index("row"), 2)
    for s in range(column_leaves):
        window = slice(s * leaf, (s + 1) * leaf)
        if plain:
            block = piece_refs[0][:, window].astype(F32)
        else:
            rows = []
            for j in range(pieces // 2):
                mine = piece_refs[j][:, window].astype(F32)
                other = piece_refs[pieces // 2 + j][:, window].astype(F32)
                rows.append(jnp.where(parity == 0, mine, other))
                rows.append(jnp.where(parity == 0, other, mine))
            block = jnp.concatenate(rows, axis=0)
        x_ref[s] = jnp.where(lane < sfill_ref[s], block, 0.0).astype(BF16)

    acc_ref[...] = jnp.zeros_like(acc_ref)

    rank_lane = lax.broadcasted_iota(jnp.int32, (rhs, rank), 1)

    @pl.loop(0, far_slots // unroll)
    def _(turn):
        for u in range(unroll):
            k = turn * unroll + u
            coef = lax.dot_general(
                x_ref[fsrc_ref[0, k]], right_ref[k], (((1,), (1,)), ((), ())), preferred_element_type=F32
            )
            coef_ref[k] = jnp.where(rank_lane < frank_ref[0, k], coef, 0.0).astype(BF16)

    @pl.loop(0, far_slots // unroll)
    def _(turn):
        blocks = []
        for u in range(unroll):
            k = turn * unroll + u
            blocks.append(jnp.dot(coef_ref[k], left_ref[k], preferred_element_type=F32))
        for u in range(unroll):
            t = ftgt_ref[0, turn * unroll + u]
            acc_ref[t] = acc_ref[t] + blocks[u]


def near_kernel(*refs, groups, chunk, chunks, plain, out_carried):
    (table_ref, tfill_ref, far_ref, x_ref) = refs[:4]
    entries_refs = refs[4 : 4 + 2 * groups]
    carried = len(out_carried)
    carried_refs = refs[4 + 2 * groups : 4 + 2 * groups + carried]
    out_refs, acc_ref = refs[4 + 2 * groups + carried : -1], refs[-1]
    chunk_leaves, rhs, leaf = acc_ref.shape
    column_leaves = x_ref.shape[0]
    base_leaf = chunk * chunk_leaves
    group = table_ref.shape[1] // groups
    total, half = table_ref[2, 0], table_ref[3, 0]
    low = half if chunk > 0 else 0
    high = total if chunk == chunks - 1 else half
    acc_ref[...] = jnp.zeros_like(acc_ref)

    def work(*accs):
        for acc in accs:
            pltpu.matmul_pop(acc)

        def drain(u, k):
            inside = (k >= low) & (k < high)
            slot = jnp.maximum(k, 0)
            t = jnp.clip(table_ref[0, slot] // column_leaves - base_leaf, 0, chunk_leaves - 1)
            copies = jnp.where(inside, table_ref[1, slot], 0).astype(F32)
            block = pltpu.matmul_pop(accs[u])
            acc_ref[t] = acc_ref[t] + jnp.where(inside, block * copies, 0.0)

        for g in range(groups):
            pair_refs = entries_refs[2 * g : 2 * g + 2]
            start = jnp.clip(low, g * group, (g + 1) * group) // 16
            stop = (jnp.clip(high, g * group, (g + 1) * group) + 15) // 16

            @pl.loop(start, stop)
            def _(turn):
                for u in range(16):
                    k = turn * 16 + u
                    source = table_ref[0, k] % column_leaves
                    stage = (u // 2) % 2
                    entries = pair_refs[u % 2][turn * 8 - g * (group // 2) + u // 2]
                    pltpu.matmul_push_rhs(entries, staging_register=stage, mxu_index=u % 2)
                    pltpu.matmul_acc_lhs(accs[u], x_ref[source], load_staged_rhs=stage)
                    if u >= 8:
                        drain(u - 8, k - 8)
                    else:
                        drain(u + 8, k - 8)

        end = (high + 15) // 16 * 16
        for u in range(8, 16):
            drain(u, end - 16 + u)

    pl.run_scoped(work, *[pltpu.ACC(u % 2)((rhs, leaf), F32) for u in range(16)])

    if plain:
        lane_t = lax.broadcasted_iota(jnp.int32, (rhs, leaf), 1)
        for t in range(chunk_leaves):
            value = acc_ref[t] + far_ref[base_leaf + t]
            out_refs[0][:, t * leaf : (t + 1) * leaf] = jnp.where(lane_t < tfill_ref[base_leaf + t], value, 0.0)
    else:
        owners = len(out_refs)
        height = rhs // owners
        lane_t = lax.broadcasted_iota(jnp.int32, (height, leaf), 1)
        base = lax.axis_index("col") ^ (lax.axis_index("row") // 2)
        for m in range(owners):
            start = pl.multiple_of((base ^ m) * height, height)
            shift = out_refs[m].shape[1] - chunk_leaves * leaf
            if shift:
                out_refs[m][:, :shift] = carried_refs[out_carried.index(m)][...]
            for t in range(chunk_leaves):
                value = acc_ref[t, pl.ds(start, height), :] + far_ref[base_leaf + t, pl.ds(start, height), :]
                value = jnp.where(lane_t < tfill_ref[base_leaf + t], value, 0.0)
                window = slice(shift + t * leaf, shift + (t + 1) * leaf)
                out_refs[m][:, window] = value.astype(out_refs[m].dtype)


def far_field(source_fill, row_leaves, far_source, far_target, far_rank, left, right, pieces, plain):
    column_leaves = source_fill.shape[0]
    far_slots, rank, leaf = left.shape
    rhs = sum(p.shape[0] for p in pieces)
    vmem = pl.BlockSpec(memory_space=pltpu.VMEM)
    smem = pl.BlockSpec(memory_space=pltpu.SMEM)
    unroll = next(u for u in (32, 16, 8, 4, 2, 1) if far_slots % u == 0)
    return pl.pallas_call(
        functools.partial(far_kernel, pieces=len(pieces), plain=plain, leaf=leaf, unroll=unroll),
        out_shape=(pltpu.VMEM((column_leaves, rhs, leaf), BF16), pltpu.VMEM((row_leaves, rhs, leaf), F32)),
        in_specs=[smem] * 4 + [vmem] * (2 + len(pieces)),
        out_specs=(vmem, vmem),
        scratch_shapes=[pltpu.VMEM((far_slots, rhs, rank), BF16)],
        compiler_params=pltpu.CompilerParams(vmem_limit_bytes=12 << 20),
        cost_estimate=pl.CostEstimate(flops=2_000_000_000, bytes_accessed=8 << 20, transcendentals=0),
        name="far",
    )(source_fill, far_source, far_target, far_rank, left, right, *pieces)


def near_field(table, target_fill, far, x, entries, owners, plain, chunk, chunks, carried=(), out_carried=()):
    row_leaves, rhs, leaf = far.shape
    width = row_leaves // chunks * leaf
    if plain:
        out_shape = (jax.ShapeDtypeStruct((rhs, width), F32),)
    else:
        out_shape = tuple(
            jax.ShapeDtypeStruct(
                (rhs // owners, width + (carried[0].shape[1] if m in out_carried else 0)), F32 if m == 0 else BF16
            )
            for m in range(owners)
        )
    return pl.pallas_call(
        functools.partial(near_kernel, groups=len(entries) // 2, chunk=chunk, chunks=chunks, plain=plain, out_carried=tuple(out_carried)),
        out_shape=out_shape,
        in_specs=[SMEM] * 2 + [VMEM] * (2 + len(entries) + len(carried)),
        out_specs=(VMEM,) * len(out_shape),
        scratch_shapes=[pltpu.VMEM((row_leaves // chunks, rhs, leaf), F32)],
        compiler_params=pltpu.CompilerParams(vmem_limit_bytes=4 << 20),
        cost_estimate=pl.CostEstimate(flops=4_000_000_000, bytes_accessed=8 << 20, transcendentals=0),
        name="near",
    )(table, target_fill, far, x, *entries, *carried)


def shards(
    source_points, source_areas, source_fill, target_points, target_fill, charges, near_fill, near_source,
    near_target, far_source, far_target, far_rank, left_basis, right_basis, *, rows, columns,
):
    plain = charges.shape[0] % 8 != 0 or rows != 2 * columns
    if plain:
        pieces = [lax.all_gather(charges, "row", axis=0, tiled=True)]
    else:

        def swap(value, axis, size, mask):
            return lax.ppermute(value, axis, [(i, i ^ mask) for i in range(size)])

        pieces = [charges] + [swap(charges, "row", rows, mask) for mask in range(2, rows, 2)]
    row_leaves, column_leaves = target_fill.shape[0], source_fill.shape[0]
    first_outs = first_entries(
        near_fill, near_source, near_target, source_points, source_areas, target_points,
        (source_fill, target_fill, far_source, far_target, far_rank), (column_leaves, row_leaves),
    )
    entries, (table, s_features, t_features) = list(first_outs[:2]), first_outs[2:5]
    source_fill, target_fill, far_source, far_target, far_rank = first_outs[5:]
    if not plain:
        pieces, table = lax.optimization_barrier((pieces, table))
        pieces = pieces + [swap(piece, "row", rows, 1) for piece in pieces]
    entries = entries + list(second_entries(table, s_features, t_features))
    if not plain:
        pieces, entries[-1] = lax.optimization_barrier((pieces, entries[-1]))
    x, far = far_field(
        source_fill, row_leaves, far_source, far_target, far_rank, left_basis[0], right_basis[0], pieces, plain
    )
    if plain or row_leaves % 2 or columns < 3:
        outs = near_field(table, target_fill, far, x, entries, columns, plain, 0, 1)
        if plain:
            return lax.psum_scatter(outs[0], "col", scatter_dimension=0, tiled=True)
        result = outs[0]
        for mask in reversed(range(1, columns)):
            result = result + swap(outs[mask], "col", columns, mask).astype(F32)
        return result

    def exchange(value, mask):
        return swap(value, "col", columns, mask)

    far_masks = tuple(range(2, columns))
    first = near_field(table, target_fill, far, x, entries, columns, plain, 0, 2)
    early = exchange(first[1], 1)
    second = near_field(
        table, target_fill, far, x, entries, columns, plain, 1, 2, [first[m] for m in far_masks], far_masks
    )
    late = [exchange(second[mask], mask) for mask in reversed(far_masks)]
    late_neighbour = exchange(second[1], 1)
    result = jnp.concatenate([first[0], second[0]], axis=1)
    result = result + jnp.concatenate([early, late_neighbour], axis=1).astype(F32)
    for value in late:
        result = result + value.astype(F32)
    return result


def solution(mesh):
    placed = (
        P(None, "col"), P("col"), P("col"), P(None, "row"), P("row"), P("row", "col"), P("row", "col"),
        P("row", "col"), P("row", "col"), P("row", "col"), P("row", "col"), P("row", "col"),
        P("row", "col", None, None), P("row", "col", None, None),
    )
    return jax.shard_map(
        functools.partial(shards, rows=mesh.shape["row"], columns=mesh.shape["col"]),
        mesh=mesh, in_specs=placed, out_specs=P("col", "row"), check_vma=False,
    )
```

```python
import functools

import jax
import jax.numpy as jnp
from jax import lax
from jax.experimental import pallas as pl
from jax.experimental.pallas import tpu as pltpu
from jax.sharding import PartitionSpec as P


INV_FOUR_PI = 0.07957747154594767
SOFTENING_SQ = 0.0025
F32 = jnp.float32
BF16 = jnp.bfloat16


def split3(value):
    first = value.astype(BF16).astype(F32)
    rest = value - first
    second = rest.astype(BF16).astype(F32)
    return first, second, rest - second


def feature_rows(rows):
    count = rows[0].shape[1]
    index = lax.broadcasted_iota(jnp.int32, (8, count), 0)
    out = jnp.zeros((8, count), F32)
    for position, row in enumerate(rows):
        out = jnp.where(index == position, jnp.broadcast_to(row, (8, count)), out)
    return out


def build_list(id_row, list_ref, half_id):
    slots = id_row.shape[1]
    square = (slots, slots)

    def across(row):
        return jnp.broadcast_to(row, square).T

    id_row = id_row.astype(F32)
    id_r = jnp.broadcast_to(id_row, square)
    lane = lax.broadcasted_iota(jnp.int32, square, 1)
    sub = lax.broadcasted_iota(jnp.int32, square, 0)
    same = jnp.where(id_r == across(id_row), 1.0, 0.0)
    count_r = jnp.sum(same, axis=0, keepdims=True)
    earlier_r = jnp.sum(jnp.where(sub < lane, same, 0.0), axis=0, keepdims=True)
    first_r = (earlier_r == 0.0) & (id_row >= 0.0)
    key_c = across(jnp.where(first_r, id_row, 1e9))
    rank_r = jnp.sum(jnp.where(key_c < id_r, 1.0, 0.0), axis=0, keepdims=True)
    rank_c = across(jnp.where(first_r, rank_r, -1.0))
    count_c = across(count_r)
    hit = rank_c == lane.astype(F32)
    list_r = jnp.sum(jnp.where(hit, key_c, 0.0), axis=0, keepdims=True)
    copies_r = jnp.sum(jnp.where(hit, count_c, 0.0), axis=0, keepdims=True)
    total = jnp.sum(jnp.where(first_r, 1.0, 0.0))
    half = jnp.sum(jnp.where(first_r & (id_row < float(half_id)), 1.0, 0.0))
    index = lax.broadcasted_iota(jnp.int32, (8, slots), 0)
    table = jnp.where(index == 0, jnp.broadcast_to(list_r, (8, slots)), 0.0)
    table = jnp.where(index == 1, jnp.broadcast_to(copies_r, (8, slots)), table)
    table = jnp.where(index == 2, total, table)
    table = jnp.where(index == 3, half, table)
    list_ref[...] = table.astype(jnp.int32)


def entry_loop(table_ref, s_ref, t_ref, entries_ref, base, low, high):
    column_leaves, leaf, width = s_ref.shape
    depth = t_ref.shape[1]
    start, stop = (low - base) // 8, (high - base + 7) // 8

    def work(*accs):
        def drain(u, turn):
            row = jnp.maximum(turn * 8 + u, 0)
            entries_ref[row] = lax.rsqrt(pltpu.matmul_pop(accs[u])).astype(BF16)

        @pl.when(stop > start)
        def _():
            for acc in accs:
                pltpu.matmul_pop(acc)

            @pl.loop(start, stop)
            def _(turn):
                for u in range(8):
                    pair = table_ref[0, base + turn * 8 + u]
                    rhs = jnp.concatenate([t_ref[pair // column_leaves], jnp.zeros((leaf - depth, leaf), BF16)], axis=0)
                    lhs = jnp.concatenate([s_ref[pair % column_leaves], jnp.zeros((leaf, leaf - width), BF16)], axis=1)
                    stage = (u // 2) % 2
                    pltpu.matmul_push_rhs(rhs, staging_register=stage, mxu_index=u % 2)
                    pltpu.matmul_acc_lhs(accs[u], lhs, load_staged_rhs=stage)
                    if u < 4:
                        drain(u + 4, turn - 1)
                    else:
                        drain(u - 4, turn)

            for u in range(4, 8):
                drain(u, stop - 1)

    pl.run_scoped(work, *[pltpu.ACC(u % 2)((leaf, leaf), F32) for u in range(8)])


def near_loop(table_ref, x_ref, entries, acc_ref, base_leaf, low, high):
    chunk_leaves, rhs, leaf = acc_ref.shape
    column_leaves = x_ref.shape[0]

    def work(*accs):
        def drain(u, k):
            inside = (k >= low) & (k < high)
            slot = jnp.maximum(k, 0)
            t = jnp.clip(table_ref[0, slot] // column_leaves - base_leaf, 0, chunk_leaves - 1)
            copies = jnp.where(inside, table_ref[1, slot], 0).astype(F32)
            block = pltpu.matmul_pop(accs[u])
            acc_ref[t] = acc_ref[t] + jnp.where(inside, block * copies, 0.0)

        @pl.when(high > low)
        def _():
            for acc in accs:
                pltpu.matmul_pop(acc)

            for entries_ref, base in entries:
                end = base + entries_ref.shape[0]
                start, stop = jnp.clip(low, base, end) // 16, (jnp.clip(high, base, end) + 15) // 16

                @pl.loop(start, stop)
                def _(turn):
                    for u in range(16):
                        k = turn * 16 + u
                        source = table_ref[0, k] % column_leaves
                        stage = (u // 2) % 2
                        pltpu.matmul_push_rhs(entries_ref[k - base], staging_register=stage, mxu_index=u % 2)
                        pltpu.matmul_acc_lhs(accs[u], x_ref[source], load_staged_rhs=stage)
                        if u >= 8:
                            drain(u - 8, k - 8)
                        else:
                            drain(u + 8, k - 8)

            end = (high + 15) // 16 * 16
            for u in range(8, 16):
                drain(u, end - 16 + u)

    pl.run_scoped(work, *[pltpu.ACC(u % 2)((rhs, leaf), F32) for u in range(16)])


def first_entries_kernel(*refs, column_leaves, row_leaves, leaf, indices):
    fill_ref, inputs, index_inputs = refs[0], refs[1:6], refs[6 : 6 + indices]
    outputs, scratch = refs[6 + indices : 10 + 2 * indices], refs[10 + 2 * indices :]
    (entries_ref, table_ref, s_ref, t_ref), index_outputs = outputs[:4], outputs[4:]
    copies, (list_ref, sem, in_sem) = scratch[:5], scratch[5:]
    moves = list(zip(inputs, copies)) + list(zip(index_inputs, index_outputs))
    loads = [pltpu.make_async_copy(src, dst, in_sem.at[i]) for i, (src, dst) in enumerate(moves)]
    for load in loads:
        load.start()
    nsrc_ref, ntgt_ref, spts_ref, area_ref, tpts_ref = copies
    for load in loads[:2]:
        load.wait()
    used = lax.broadcasted_iota(jnp.int32, nsrc_ref.shape, 1) < fill_ref[0, 0]
    ids = jnp.where(used, ntgt_ref[...] * column_leaves + nsrc_ref[...], -1)
    build_list(ids, list_ref, (row_leaves // 2) * column_leaves)
    copy = pltpu.make_async_copy(list_ref, table_ref, sem)
    copy.start()
    for load in loads[2:5]:
        load.wait()

    tx, ty, tz = (tpts_ref[i : i + 1, :] - 0.5 for i in range(3))
    norm = tx * tx + ty * ty + tz * tz
    h1, h2, h3 = split3(feature_rows([tx, ty, tz, jnp.ones_like(tx), norm]))
    features = jnp.concatenate([h1, h2, h1, h2, h3, h1, jnp.zeros((16,) + h1.shape[1:], F32)], axis=0).astype(BF16)
    for t in range(row_leaves):
        t_ref[t] = features[:, t * leaf : (t + 1) * leaf]

    sx, sy, sz = (spts_ref[i : i + 1, :] - 0.5 for i in range(3))
    scale = area_ref[...] * INV_FOUR_PI
    weight = 1.0 / (scale * scale)
    norm = sx * sx + sy * sy + sz * sz + SOFTENING_SQ
    g1, g2, g3 = split3(
        feature_rows([-2.0 * weight * sx, -2.0 * weight * sy, -2.0 * weight * sz, weight * norm, weight])
    )
    features = jnp.concatenate([g1, g1, g2, g2, g1, g3, jnp.zeros((16,) + g1.shape[1:], F32)], axis=0).astype(BF16)
    for s in range(column_leaves):
        column = features[:, s * leaf : (s + 1) * leaf].T
        s_ref[s] = jnp.concatenate([column, jnp.zeros((leaf, 128 - column.shape[1]), BF16)], axis=1)

    copy.wait()
    entry_loop(table_ref, s_ref, t_ref, entries_ref, 0, 0, jnp.minimum(table_ref[2, 0], entries_ref.shape[0]))
    for load in loads[5:]:
        load.wait()


def second_entries_kernel(table_ref, s_ref, t_ref, entries_ref, *, first):
    total = table_ref[2, 0]
    entry_loop(
        table_ref, s_ref, t_ref, entries_ref, first, first, jnp.clip(total, first, first + entries_ref.shape[0])
    )


VMEM = pl.BlockSpec(memory_space=pltpu.VMEM)
SMEM = pl.BlockSpec(memory_space=pltpu.SMEM)
HBM = pl.BlockSpec(memory_space=pltpu.HBM)


def first_count(slots):
    return max(slots * 3 // 8 // 16 * 16, 16)


def second_count(slots):
    return max(slots // 8 // 16 * 16, 16)


def first_entries(near_fill, near_source, near_target, source_points, source_areas, target_points, indices, leaves):
    column_leaves, row_leaves = leaves
    slots = near_source.shape[1]
    leaf = source_points.shape[1] // column_leaves
    depth = 64
    inputs = (near_source, near_target, source_points, source_areas[None, :], target_points)
    hbm_inputs = tuple(pltpu.with_memory_space_constraint(value, pltpu.HBM) for value in inputs + tuple(indices))
    return pl.pallas_call(
        functools.partial(
            first_entries_kernel, column_leaves=column_leaves, row_leaves=row_leaves, leaf=leaf,
            indices=len(indices),
        ),
        out_shape=(
            pltpu.VMEM((first_count(slots), leaf, leaf), BF16),
            pltpu.SMEM((8, slots), jnp.int32),
            pltpu.VMEM((column_leaves, leaf, 128), BF16),
            pltpu.VMEM((row_leaves, depth, leaf), BF16),
        )
        + tuple(pltpu.SMEM(value.shape, jnp.int32) for value in indices),
        in_specs=[SMEM] + [HBM] * len(hbm_inputs),
        out_specs=(VMEM, SMEM, VMEM, VMEM) + (SMEM,) * len(indices),
        scratch_shapes=[pltpu.VMEM(value.shape, value.dtype) for value in inputs]
        + [pltpu.VMEM((8, slots), jnp.int32), pltpu.SemaphoreType.DMA, pltpu.SemaphoreType.DMA((len(hbm_inputs),))],
        compiler_params=pltpu.CompilerParams(vmem_limit_bytes=10 << 20),
        cost_estimate=pl.CostEstimate(flops=8_000_000_000, bytes_accessed=1 << 20, transcendentals=0),
        name="entries",
    )(near_fill, *hbm_inputs)


def second_entries(table, s_features, t_features):
    slots = table.shape[1]
    leaf = s_features.shape[1]
    return pl.pallas_call(
        functools.partial(second_entries_kernel, first=first_count(slots)),
        out_shape=pltpu.VMEM((second_count(slots), leaf, leaf), BF16),
        in_specs=[SMEM, VMEM, VMEM],
        out_specs=VMEM,
        compiler_params=pltpu.CompilerParams(vmem_limit_bytes=4 << 20),
        cost_estimate=pl.CostEstimate(flops=8_000_000_000, bytes_accessed=1 << 20, transcendentals=0),
        name="entries_rest",
    )(table, s_features, t_features)


def far_kernel(*refs, pieces, plain, leaf, unroll):
    (sfill_ref, fsrc_ref, ftgt_ref, frank_ref, left_ref, right_ref) = refs[:6]
    piece_refs = refs[6 : 6 + pieces]
    x_ref, acc_ref, coef_ref = refs[6 + pieces :]
    column_leaves, rhs, _ = x_ref.shape
    far_slots, rank, _ = left_ref.shape

    lane = lax.broadcasted_iota(jnp.int32, (rhs, leaf), 1)
    if not plain:
        parity = lax.rem(lax.axis_index("row"), 2)
    for s in range(column_leaves):
        window = slice(s * leaf, (s + 1) * leaf)
        if plain:
            block = piece_refs[0][:, window].astype(F32)
        else:
            rows = []
            for j in range(pieces // 2):
                mine = piece_refs[j][:, window].astype(F32)
                other = piece_refs[pieces // 2 + j][:, window].astype(F32)
                rows.append(jnp.where(parity == 0, mine, other))
                rows.append(jnp.where(parity == 0, other, mine))
            block = jnp.concatenate(rows, axis=0)
        x_ref[s] = jnp.where(lane < sfill_ref[s], block, 0.0).astype(BF16)

    acc_ref[...] = jnp.zeros_like(acc_ref)

    rank_lane = lax.broadcasted_iota(jnp.int32, (rhs, rank), 1)

    @pl.loop(0, far_slots // unroll)
    def _(turn):
        for u in range(unroll):
            k = turn * unroll + u
            coef = lax.dot_general(
                x_ref[fsrc_ref[0, k]], right_ref[k], (((1,), (1,)), ((), ())), preferred_element_type=F32
            )
            coef_ref[k] = jnp.where(rank_lane < frank_ref[0, k], coef, 0.0).astype(BF16)

    @pl.loop(0, far_slots // unroll)
    def _(turn):
        blocks = []
        for u in range(unroll):
            k = turn * unroll + u
            blocks.append(jnp.dot(coef_ref[k], left_ref[k], preferred_element_type=F32))
        for u in range(unroll):
            t = ftgt_ref[0, turn * unroll + u]
            acc_ref[t] = acc_ref[t] + blocks[u]


def near_kernel(*refs, chunk, chunks, plain, out_carried):
    (table_ref, tfill_ref, far_ref, x_ref, first_ref, second_ref, s_ref, t_ref) = refs[:8]
    carried = len(out_carried)
    carried_refs = refs[8 : 8 + carried]
    out_refs, (rest_ref, acc_ref) = refs[8 + carried : -2], refs[-2:]
    chunk_leaves, rhs, leaf = acc_ref.shape
    base_leaf = chunk * chunk_leaves
    total, half = table_ref[2, 0], table_ref[3, 0]
    low = half if chunk > 0 else 0
    high = total if chunk == chunks - 1 else half
    made = first_ref.shape[0] + second_ref.shape[0]
    acc_ref[...] = jnp.zeros_like(acc_ref)
    near_loop(
        table_ref, x_ref, [(first_ref, 0), (second_ref, first_ref.shape[0])], acc_ref, base_leaf,
        jnp.minimum(low, made), jnp.minimum(high, made),
    )
    rest = (jnp.maximum(low, made), jnp.maximum(high, made))
    entry_loop(table_ref, s_ref, t_ref, rest_ref, made, *rest)
    near_loop(table_ref, x_ref, [(rest_ref, made)], acc_ref, base_leaf, *rest)

    if plain:
        lane_t = lax.broadcasted_iota(jnp.int32, (rhs, leaf), 1)
        for t in range(chunk_leaves):
            value = acc_ref[t] + far_ref[base_leaf + t]
            out_refs[0][:, t * leaf : (t + 1) * leaf] = jnp.where(lane_t < tfill_ref[base_leaf + t], value, 0.0)
    else:
        owners = len(out_refs)
        height = rhs // owners
        lane_t = lax.broadcasted_iota(jnp.int32, (height, leaf), 1)
        base = lax.axis_index("col") ^ (lax.axis_index("row") // 2)
        for m in range(owners):
            start = pl.multiple_of((base ^ m) * height, height)
            shift = out_refs[m].shape[1] - chunk_leaves * leaf
            if shift:
                out_refs[m][:, :shift] = carried_refs[out_carried.index(m)][...]
            for t in range(chunk_leaves):
                value = acc_ref[t, pl.ds(start, height), :] + far_ref[base_leaf + t, pl.ds(start, height), :]
                value = jnp.where(lane_t < tfill_ref[base_leaf + t], value, 0.0)
                window = slice(shift + t * leaf, shift + (t + 1) * leaf)
                out_refs[m][:, window] = value.astype(out_refs[m].dtype)


def far_field(source_fill, row_leaves, far_source, far_target, far_rank, left, right, pieces, plain):
    column_leaves = source_fill.shape[0]
    far_slots, rank, leaf = left.shape
    rhs = sum(p.shape[0] for p in pieces)
    vmem = pl.BlockSpec(memory_space=pltpu.VMEM)
    smem = pl.BlockSpec(memory_space=pltpu.SMEM)
    unroll = next(u for u in (32, 16, 8, 4, 2, 1) if far_slots % u == 0)
    return pl.pallas_call(
        functools.partial(far_kernel, pieces=len(pieces), plain=plain, leaf=leaf, unroll=unroll),
        out_shape=(pltpu.VMEM((column_leaves, rhs, leaf), BF16), pltpu.VMEM((row_leaves, rhs, leaf), F32)),
        in_specs=[smem] * 4 + [vmem] * (2 + len(pieces)),
        out_specs=(vmem, vmem),
        scratch_shapes=[pltpu.VMEM((far_slots, rhs, rank), BF16)],
        compiler_params=pltpu.CompilerParams(vmem_limit_bytes=12 << 20),
        cost_estimate=pl.CostEstimate(flops=2_000_000_000, bytes_accessed=8 << 20, transcendentals=0),
        name="far",
    )(source_fill, far_source, far_target, far_rank, left, right, *pieces)


def near_field(table, target_fill, far, x, made, features, owners, plain, chunk, chunks, carried=(), out_carried=()):
    row_leaves, rhs, leaf = far.shape
    width = row_leaves // chunks * leaf
    if plain:
        out_shape = (jax.ShapeDtypeStruct((rhs, width), F32),)
    else:
        out_shape = tuple(
            jax.ShapeDtypeStruct(
                (rhs // owners, width + (carried[0].shape[1] if m in out_carried else 0)), F32 if m == 0 else BF16
            )
            for m in range(owners)
        )
    rest = table.shape[1] - sum(value.shape[0] for value in made)
    return pl.pallas_call(
        functools.partial(near_kernel, chunk=chunk, chunks=chunks, plain=plain, out_carried=tuple(out_carried)),
        out_shape=out_shape,
        in_specs=[SMEM] * 2 + [VMEM] * (6 + len(carried)),
        out_specs=(VMEM,) * len(out_shape),
        scratch_shapes=[pltpu.VMEM((rest, leaf, leaf), BF16), pltpu.VMEM((row_leaves // chunks, rhs, leaf), F32)],
        compiler_params=pltpu.CompilerParams(vmem_limit_bytes=20 << 20),
        cost_estimate=pl.CostEstimate(flops=4_000_000_000, bytes_accessed=8 << 20, transcendentals=0),
        name="near",
    )(table, target_fill, far, x, *made, *features, *carried)


def shards(
    source_points, source_areas, source_fill, target_points, target_fill, charges, near_fill, near_source,
    near_target, far_source, far_target, far_rank, left_basis, right_basis, *, rows, columns,
):
    plain = charges.shape[0] % 8 != 0 or rows != 2 * columns
    if plain:
        pieces = [lax.all_gather(charges, "row", axis=0, tiled=True)]
    else:

        def swap(value, axis, size, mask):
            return lax.ppermute(value, axis, [(i, i ^ mask) for i in range(size)])

        pieces = [charges] + [swap(charges, "row", rows, mask) for mask in range(2, rows, 2)]
    row_leaves, column_leaves = target_fill.shape[0], source_fill.shape[0]
    first_outs = first_entries(
        near_fill, near_source, near_target, source_points, source_areas, target_points,
        (source_fill, target_fill, far_source, far_target, far_rank), (column_leaves, row_leaves),
    )
    entries, table, *features = first_outs[:4]
    source_fill, target_fill, far_source, far_target, far_rank = first_outs[4:]
    if not plain:
        pieces, table = lax.optimization_barrier((pieces, table))
        pieces = pieces + [swap(piece, "row", rows, 1) for piece in pieces]
    more_entries = second_entries(table, *features)
    if not plain:
        pieces, more_entries = lax.optimization_barrier((pieces, more_entries))
    made = (entries, more_entries)
    x, far = far_field(
        source_fill, row_leaves, far_source, far_target, far_rank, left_basis[0], right_basis[0], pieces, plain
    )
    if plain or row_leaves % 2 or columns < 3:
        outs = near_field(table, target_fill, far, x, made, features, columns, plain, 0, 1)
        if plain:
            return lax.psum_scatter(outs[0], "col", scatter_dimension=0, tiled=True)
        result = outs[0]
        for mask in reversed(range(1, columns)):
            result = result + swap(outs[mask], "col", columns, mask).astype(F32)
        return result

    def exchange(value, mask):
        return swap(value, "col", columns, mask)

    last = columns - 1
    first = near_field(table, target_fill, far, x, made, features, columns, plain, 0, 2)
    early = {mask: exchange(first[mask], mask) for mask in range(1, last)}
    second = near_field(table, target_fill, far, x, made, features, columns, plain, 1, 2, (first[last],), (last,))
    late = {mask: exchange(second[mask], mask) for mask in reversed(range(1, columns))}
    result = jnp.concatenate([first[0], second[0]], axis=1) + late[last].astype(F32)
    for mask in early:
        result = result + jnp.concatenate([early[mask], late[mask]], axis=1).astype(F32)
    return result


def solution(mesh):
    placed = (
        P(None, "col"), P("col"), P("col"), P(None, "row"), P("row"), P("row", "col"), P("row", "col"),
        P("row", "col"), P("row", "col"), P("row", "col"), P("row", "col"), P("row", "col"),
        P("row", "col", None, None), P("row", "col", None, None),
    )
    return jax.shard_map(
        functools.partial(shards, rows=mesh.shape["row"], columns=mesh.shape["col"]),
        mesh=mesh, in_specs=placed, out_specs=P("col", "row"), check_vma=False,
    )
```

```python
import functools

import jax
import jax.numpy as jnp
from jax import lax
from jax.experimental import pallas as pl
from jax.experimental.pallas import tpu as pltpu
from jax.sharding import PartitionSpec as P


INV_FOUR_PI = 0.07957747154594767
SOFTENING_SQ = 0.0025
F32 = jnp.float32
BF16 = jnp.bfloat16
ENTRY_TRIP = 16
NEAR_TRIP = 16


def split3(value):
    first = value.astype(BF16).astype(F32)
    rest = value - first
    second = rest.astype(BF16).astype(F32)
    return first, second, rest - second


def feature_rows(rows):
    count = rows[0].shape[1]
    index = lax.broadcasted_iota(jnp.int32, (8, count), 0)
    out = jnp.zeros((8, count), F32)
    for position, row in enumerate(rows):
        out = jnp.where(index == position, jnp.broadcast_to(row, (8, count)), out)
    return out


def build_list(id_row, list_ref, half_id):
    slots = id_row.shape[1]
    square = (slots, slots)

    def across(row):
        return jnp.broadcast_to(row, square).T

    id_row = id_row.astype(F32)
    id_r = jnp.broadcast_to(id_row, square)
    lane = lax.broadcasted_iota(jnp.int32, square, 1)
    sub = lax.broadcasted_iota(jnp.int32, square, 0)
    same = jnp.where(id_r == across(id_row), 1.0, 0.0)
    count_r = jnp.sum(same, axis=0, keepdims=True)
    earlier_r = jnp.sum(jnp.where(sub < lane, same, 0.0), axis=0, keepdims=True)
    first_r = (earlier_r == 0.0) & (id_row >= 0.0)
    key_c = across(jnp.where(first_r, id_row, 1e9))
    rank_r = jnp.sum(jnp.where(key_c < id_r, 1.0, 0.0), axis=0, keepdims=True)
    rank_c = across(jnp.where(first_r, rank_r, -1.0))
    count_c = across(count_r)
    hit = rank_c == lane.astype(F32)
    list_r = jnp.sum(jnp.where(hit, key_c, 0.0), axis=0, keepdims=True)
    copies_r = jnp.sum(jnp.where(hit, count_c, 0.0), axis=0, keepdims=True)
    total = jnp.sum(jnp.where(first_r, 1.0, 0.0))
    half = jnp.sum(jnp.where(first_r & (id_row < float(half_id)), 1.0, 0.0))
    index = lax.broadcasted_iota(jnp.int32, (8, slots), 0)
    table = jnp.where(index == 0, jnp.broadcast_to(list_r, (8, slots)), 0.0)
    table = jnp.where(index == 1, jnp.broadcast_to(copies_r, (8, slots)), table)
    table = jnp.where(index == 2, total, table)
    table = jnp.where(index == 3, half, table)
    list_ref[...] = table.astype(jnp.int32)


def entry_loop(table_ref, s_ref, t_ref, entries_refs, base, low, high):
    column_leaves, leaf, width = s_ref.shape
    depth = t_ref.shape[1]
    start, stop = (low - base) // ENTRY_TRIP, (high - base + ENTRY_TRIP - 1) // ENTRY_TRIP

    def work(*accs):
        def drain(u, turn):
            row = jnp.maximum(turn * (ENTRY_TRIP // 2) + u // 2, 0)
            entries_refs[u % 2][row] = lax.rsqrt(pltpu.matmul_pop(accs[u % 8])).astype(BF16)

        @pl.when(stop > start)
        def _():
            for acc in accs:
                pltpu.matmul_pop(acc)

            @pl.loop(start, stop)
            def _(turn):
                for u in range(ENTRY_TRIP):
                    pair = table_ref[0, base + turn * ENTRY_TRIP + u]
                    rhs = jnp.concatenate([t_ref[pair // column_leaves], jnp.zeros((leaf - depth, leaf), BF16)], axis=0)
                    lhs = jnp.concatenate([s_ref[pair % column_leaves], jnp.zeros((leaf, leaf - width), BF16)], axis=1)
                    stage = (u // 2) % 2
                    pltpu.matmul_push_rhs(rhs, staging_register=stage, mxu_index=u % 2)
                    pltpu.matmul_acc_lhs(accs[u % 8], lhs, load_staged_rhs=stage)
                    if u < 4:
                        drain(ENTRY_TRIP - 4 + u, turn - 1)
                    else:
                        drain(u - 4, turn)

            for u in range(ENTRY_TRIP - 4, ENTRY_TRIP):
                drain(u, stop - 1)

    pl.run_scoped(work, *[pltpu.ACC(u % 2)((leaf, leaf), F32) for u in range(8)])


def near_loop(table_ref, x_ref, entries, acc_refs, base_leaf, low, high):
    chunk_leaves, rhs, leaf = acc_refs[0].shape
    column_leaves = x_ref.shape[0]

    def work(*accs):
        def drain(u, k):
            inside = (k >= low) & (k < high)
            slot = jnp.maximum(k, 0)
            t = jnp.clip(table_ref[0, slot] // column_leaves - base_leaf, 0, chunk_leaves - 1)
            copies = jnp.where(inside, table_ref[1, slot], 0).astype(F32)
            block = pltpu.matmul_pop(accs[u])
            acc_refs[u % 2][t] = acc_refs[u % 2][t] + jnp.where(inside, block * copies, 0.0)

        @pl.when(high > low)
        def _():
            for acc in accs:
                pltpu.matmul_pop(acc)

            for *entries_refs, base in entries:
                end = base + 2 * entries_refs[0].shape[0]
                start = jnp.clip(low, base, end) // NEAR_TRIP
                stop = (jnp.clip(high, base, end) + NEAR_TRIP - 1) // NEAR_TRIP

                @pl.loop(start, stop)
                def _(turn):
                    for u in range(NEAR_TRIP):
                        k = turn * NEAR_TRIP + u
                        source = table_ref[0, k] % column_leaves
                        row = turn * (NEAR_TRIP // 2) - base // 2 + u // 2
                        stage = (u // 2) % 2
                        pltpu.matmul_push_rhs(entries_refs[u % 2][row], staging_register=stage, mxu_index=u % 2)
                        pltpu.matmul_acc_lhs(accs[u % 16], x_ref[source], load_staged_rhs=stage)
                        drain((u + 8) % 16, k - 8)

            end = (high + NEAR_TRIP - 1) // NEAR_TRIP * NEAR_TRIP
            for u in range(8):
                drain(u + 8, end - 8 + u)

    pl.run_scoped(work, *[pltpu.ACC(u % 2)((rhs, leaf), F32) for u in range(16)])


def first_entries_kernel(*refs, column_leaves, row_leaves, leaf, indices):
    fill_ref, inputs, index_inputs = refs[0], refs[1:6], refs[6 : 6 + indices]
    outputs, scratch = refs[6 + indices : 11 + 2 * indices], refs[11 + 2 * indices :]
    (*entries_refs, table_ref, s_ref, t_ref), index_outputs = outputs[:5], outputs[5:]
    copies, (list_ref, sem, in_sem) = scratch[:5], scratch[5:]
    moves = list(zip(inputs, copies)) + list(zip(index_inputs, index_outputs))
    loads = [pltpu.make_async_copy(src, dst, in_sem.at[i]) for i, (src, dst) in enumerate(moves)]
    for load in loads:
        load.start()
    nsrc_ref, ntgt_ref, spts_ref, area_ref, tpts_ref = copies
    for load in loads[:2]:
        load.wait()
    used = lax.broadcasted_iota(jnp.int32, nsrc_ref.shape, 1) < fill_ref[0, 0]
    ids = jnp.where(used, ntgt_ref[...] * column_leaves + nsrc_ref[...], -1)
    build_list(ids, list_ref, first_leaves(row_leaves) * column_leaves)
    copy = pltpu.make_async_copy(list_ref, table_ref, sem)
    copy.start()
    for load in loads[2:5]:
        load.wait()

    tx, ty, tz = (tpts_ref[i : i + 1, :] - 0.5 for i in range(3))
    norm = tx * tx + ty * ty + tz * tz
    h1, h2, h3 = split3(feature_rows([tx, ty, tz, jnp.ones_like(tx), norm]))
    features = jnp.concatenate([h1, h2, h1, h2, h3, h1, jnp.zeros((16,) + h1.shape[1:], F32)], axis=0).astype(BF16)
    for t in range(row_leaves):
        t_ref[t] = features[:, t * leaf : (t + 1) * leaf]

    sx, sy, sz = (spts_ref[i : i + 1, :] - 0.5 for i in range(3))
    scale = area_ref[...] * INV_FOUR_PI
    weight = 1.0 / (scale * scale)
    norm = sx * sx + sy * sy + sz * sz + SOFTENING_SQ
    g1, g2, g3 = split3(
        feature_rows([-2.0 * weight * sx, -2.0 * weight * sy, -2.0 * weight * sz, weight * norm, weight])
    )
    features = jnp.concatenate([g1, g1, g2, g2, g1, g3, jnp.zeros((16,) + g1.shape[1:], F32)], axis=0).astype(BF16)
    for s in range(column_leaves):
        column = features[:, s * leaf : (s + 1) * leaf].T
        s_ref[s] = jnp.concatenate([column, jnp.zeros((leaf, 128 - column.shape[1]), BF16)], axis=1)

    copy.wait()
    entry_loop(table_ref, s_ref, t_ref, entries_refs, 0, 0, jnp.minimum(table_ref[2, 0], 2 * entries_refs[0].shape[0]))
    for load in loads[5:]:
        load.wait()


def second_entries_kernel(table_ref, s_ref, t_ref, *entries_refs, first):
    last = first + 2 * entries_refs[0].shape[0]
    entry_loop(table_ref, s_ref, t_ref, entries_refs, first, first, jnp.clip(table_ref[2, 0], first, last))


VMEM = pl.BlockSpec(memory_space=pltpu.VMEM)
SMEM = pl.BlockSpec(memory_space=pltpu.SMEM)
HBM = pl.BlockSpec(memory_space=pltpu.HBM)


def first_leaves(row_leaves):
    return row_leaves * 5 // 8


def first_count(slots):
    return max(slots * 3 // 8 // NEAR_TRIP, 1) * NEAR_TRIP


def second_count(slots):
    return max(slots // 8 // NEAR_TRIP, 1) * NEAR_TRIP


def first_entries(near_fill, near_source, near_target, source_points, source_areas, target_points, indices, leaves):
    column_leaves, row_leaves = leaves
    slots = near_source.shape[1]
    leaf = source_points.shape[1] // column_leaves
    depth = 64
    inputs = (near_source, near_target, source_points, source_areas[None, :], target_points)
    hbm_inputs = tuple(pltpu.with_memory_space_constraint(value, pltpu.HBM) for value in inputs + tuple(indices))
    return pl.pallas_call(
        functools.partial(
            first_entries_kernel, column_leaves=column_leaves, row_leaves=row_leaves, leaf=leaf,
            indices=len(indices),
        ),
        out_shape=(
            *[pltpu.VMEM((first_count(slots) // 2, leaf, leaf), BF16)] * 2,
            pltpu.SMEM((8, slots), jnp.int32),
            pltpu.VMEM((column_leaves, leaf, 128), BF16),
            pltpu.VMEM((row_leaves, depth, leaf), BF16),
        )
        + tuple(pltpu.SMEM(value.shape, jnp.int32) for value in indices),
        in_specs=[SMEM] + [HBM] * len(hbm_inputs),
        out_specs=(VMEM, VMEM, SMEM, VMEM, VMEM) + (SMEM,) * len(indices),
        scratch_shapes=[pltpu.VMEM(value.shape, value.dtype) for value in inputs]
        + [pltpu.VMEM((8, slots), jnp.int32), pltpu.SemaphoreType.DMA, pltpu.SemaphoreType.DMA((len(hbm_inputs),))],
        compiler_params=pltpu.CompilerParams(vmem_limit_bytes=10 << 20),
        cost_estimate=pl.CostEstimate(flops=8_000_000_000, bytes_accessed=1 << 20, transcendentals=0),
        name="entries",
    )(near_fill, *hbm_inputs)


def second_entries(table, s_features, t_features):
    slots = table.shape[1]
    leaf = s_features.shape[1]
    return pl.pallas_call(
        functools.partial(second_entries_kernel, first=first_count(slots)),
        out_shape=(pltpu.VMEM((second_count(slots) // 2, leaf, leaf), BF16),) * 2,
        in_specs=[SMEM, VMEM, VMEM],
        out_specs=(VMEM, VMEM),
        compiler_params=pltpu.CompilerParams(vmem_limit_bytes=4 << 20),
        cost_estimate=pl.CostEstimate(flops=8_000_000_000, bytes_accessed=1 << 20, transcendentals=0),
        name="entries_rest",
    )(table, s_features, t_features)


def far_kernel(*refs, pieces, plain, leaf, unroll):
    (sfill_ref, fsrc_ref, ftgt_ref, frank_ref, left_ref, right_ref) = refs[:6]
    piece_refs = refs[6 : 6 + pieces]
    x_ref, acc_ref, coef_ref = refs[6 + pieces :]
    column_leaves, rhs, _ = x_ref.shape
    far_slots, rank, _ = left_ref.shape

    lane = lax.broadcasted_iota(jnp.int32, (rhs, leaf), 1)
    if not plain:
        parity = lax.rem(lax.axis_index("row"), 2)
    for s in range(column_leaves):
        window = slice(s * leaf, (s + 1) * leaf)
        if plain:
            block = piece_refs[0][:, window].astype(F32)
        else:
            rows = []
            for j in range(pieces // 2):
                mine = piece_refs[j][:, window].astype(F32)
                other = piece_refs[pieces // 2 + j][:, window].astype(F32)
                rows.append(jnp.where(parity == 0, mine, other))
                rows.append(jnp.where(parity == 0, other, mine))
            block = jnp.concatenate(rows, axis=0)
        x_ref[s] = jnp.where(lane < sfill_ref[s], block, 0.0).astype(BF16)

    acc_ref[...] = jnp.zeros_like(acc_ref)

    rank_lane = lax.broadcasted_iota(jnp.int32, (rhs, rank), 1)

    @pl.loop(0, far_slots // unroll)
    def _(turn):
        for u in range(unroll):
            k = turn * unroll + u
            coef = lax.dot_general(
                x_ref[fsrc_ref[0, k]], right_ref[k], (((1,), (1,)), ((), ())), preferred_element_type=F32
            )
            coef_ref[k] = jnp.where(rank_lane < frank_ref[0, k], coef, 0.0).astype(BF16)

    @pl.loop(0, far_slots // unroll)
    def _(turn):
        blocks = []
        for u in range(unroll):
            k = turn * unroll + u
            blocks.append(jnp.dot(coef_ref[k], left_ref[k], preferred_element_type=F32))
        for u in range(unroll):
            t = ftgt_ref[0, turn * unroll + u]
            acc_ref[t] = acc_ref[t] + blocks[u]


def near_kernel(*refs, base_leaf, plain, out_carried):
    (table_ref, tfill_ref, far_ref, x_ref), first_refs, second_refs, (s_ref, t_ref) = refs[:4], refs[4:6], refs[6:8], refs[8:10]
    carried = len(out_carried)
    carried_refs = refs[10 : 10 + carried]
    out_refs, rest_refs, acc_refs = refs[10 + carried : -4], refs[-4:-2], refs[-2:]
    chunk_leaves, rhs, leaf = acc_refs[0].shape
    total, half = table_ref[2, 0], table_ref[3, 0]
    low = half if base_leaf > 0 else 0
    high = total if base_leaf + chunk_leaves == far_ref.shape[0] else half
    first, second = 2 * first_refs[0].shape[0], 2 * second_refs[0].shape[0]
    made = first + second
    for acc_ref in acc_refs:
        acc_ref[...] = jnp.zeros_like(acc_ref)
    near_loop(
        table_ref, x_ref, [(*first_refs, 0), (*second_refs, first)], acc_refs, base_leaf,
        jnp.minimum(low, made), jnp.minimum(high, made),
    )
    rest = (jnp.maximum(low, made), jnp.maximum(high, made))
    entry_loop(table_ref, s_ref, t_ref, rest_refs, made, *rest)
    near_loop(table_ref, x_ref, [(*rest_refs, made)], acc_refs, base_leaf, *rest)

    if plain:
        lane_t = lax.broadcasted_iota(jnp.int32, (rhs, leaf), 1)
        for t in range(chunk_leaves):
            value = acc_refs[0][t] + acc_refs[1][t] + far_ref[base_leaf + t]
            out_refs[0][:, t * leaf : (t + 1) * leaf] = jnp.where(lane_t < tfill_ref[base_leaf + t], value, 0.0)
    else:
        owners = len(out_refs)
        height = rhs // owners
        lane_t = lax.broadcasted_iota(jnp.int32, (height, leaf), 1)
        base = lax.axis_index("col") ^ (lax.axis_index("row") // 2)
        for m in range(owners):
            start = pl.multiple_of((base ^ m) * height, height)
            shift = out_refs[m].shape[1] - chunk_leaves * leaf
            if shift:
                out_refs[m][:, :shift] = carried_refs[out_carried.index(m)][...]
            for t in range(chunk_leaves):
                rows = pl.ds(start, height)
                value = acc_refs[0][t, rows, :] + acc_refs[1][t, rows, :] + far_ref[base_leaf + t, rows, :]
                value = jnp.where(lane_t < tfill_ref[base_leaf + t], value, 0.0)
                window = slice(shift + t * leaf, shift + (t + 1) * leaf)
                out_refs[m][:, window] = value.astype(out_refs[m].dtype)


def far_field(source_fill, row_leaves, far_source, far_target, far_rank, left, right, pieces, plain):
    column_leaves = source_fill.shape[0]
    far_slots, rank, leaf = left.shape
    rhs = sum(p.shape[0] for p in pieces)
    vmem = pl.BlockSpec(memory_space=pltpu.VMEM)
    smem = pl.BlockSpec(memory_space=pltpu.SMEM)
    unroll = next(u for u in (32, 16, 8, 4, 2, 1) if far_slots % u == 0)
    return pl.pallas_call(
        functools.partial(far_kernel, pieces=len(pieces), plain=plain, leaf=leaf, unroll=unroll),
        out_shape=(pltpu.VMEM((column_leaves, rhs, leaf), BF16), pltpu.VMEM((row_leaves, rhs, leaf), F32)),
        in_specs=[smem] * 4 + [vmem] * (2 + len(pieces)),
        out_specs=(vmem, vmem),
        scratch_shapes=[pltpu.VMEM((far_slots, rhs, rank), BF16)],
        compiler_params=pltpu.CompilerParams(vmem_limit_bytes=12 << 20),
        cost_estimate=pl.CostEstimate(flops=2_000_000_000, bytes_accessed=8 << 20, transcendentals=0),
        name="far",
    )(source_fill, far_source, far_target, far_rank, left, right, *pieces)


def near_field(table, target_fill, far, x, made, features, owners, plain, leaves, carried=(), out_carried=()):
    _, rhs, leaf = far.shape
    width = len(leaves) * leaf
    if plain:
        out_shape = (jax.ShapeDtypeStruct((rhs, width), F32),)
    else:
        out_shape = tuple(
            jax.ShapeDtypeStruct(
                (rhs // owners, width + (carried[0].shape[1] if m in out_carried else 0)), F32 if m == 0 else BF16
            )
            for m in range(owners)
        )
    rest = (table.shape[1] - sum(value.shape[0] for value in made)) // 2
    return pl.pallas_call(
        functools.partial(near_kernel, base_leaf=leaves[0], plain=plain, out_carried=tuple(out_carried)),
        out_shape=out_shape,
        in_specs=[SMEM] * 2 + [VMEM] * (8 + len(carried)),
        out_specs=(VMEM,) * len(out_shape),
        scratch_shapes=[pltpu.VMEM((rest, leaf, leaf), BF16)] * 2 + [pltpu.VMEM((len(leaves), rhs, leaf), F32)] * 2,
        compiler_params=pltpu.CompilerParams(vmem_limit_bytes=20 << 20),
        cost_estimate=pl.CostEstimate(flops=4_000_000_000, bytes_accessed=8 << 20, transcendentals=0),
        name="near",
    )(table, target_fill, far, x, *made, *features, *carried)


def shards(
    source_points, source_areas, source_fill, target_points, target_fill, charges, near_fill, near_source,
    near_target, far_source, far_target, far_rank, left_basis, right_basis, *, rows, columns,
):
    plain = charges.shape[0] % 8 != 0 or rows != 2 * columns
    if plain:
        pieces = [lax.all_gather(charges, "row", axis=0, tiled=True)]
    else:

        def swap(value, axis, size, mask):
            return lax.ppermute(value, axis, [(i, i ^ mask) for i in range(size)])

        pieces = [charges] + [swap(charges, "row", rows, mask) for mask in range(2, rows, 2)]
    row_leaves, column_leaves = target_fill.shape[0], source_fill.shape[0]
    first_outs = first_entries(
        near_fill, near_source, near_target, source_points, source_areas, target_points,
        (source_fill, target_fill, far_source, far_target, far_rank), (column_leaves, row_leaves),
    )
    *entries, table, s_features, t_features = first_outs[:5]
    features = (s_features, t_features)
    source_fill, target_fill, far_source, far_target, far_rank = first_outs[5:]
    if not plain:
        pieces, table = lax.optimization_barrier((pieces, table))
        pieces = pieces + [swap(piece, "row", rows, 1) for piece in pieces]
    more_entries = list(second_entries(table, *features))
    if not plain:
        pieces, more_entries[0] = lax.optimization_barrier((pieces, more_entries[0]))
    made = (*entries, *more_entries)
    x, far = far_field(
        source_fill, row_leaves, far_source, far_target, far_rank, left_basis[0], right_basis[0], pieces, plain
    )
    if plain or row_leaves < 2 or columns < 3:
        outs = near_field(table, target_fill, far, x, made, features, columns, plain, range(row_leaves))
        if plain:
            return lax.psum_scatter(outs[0], "col", scatter_dimension=0, tiled=True)
        result = outs[0]
        for mask in reversed(range(1, columns)):
            result = result + swap(outs[mask], "col", columns, mask).astype(F32)
        return result

    def exchange(value, mask):
        return swap(value, "col", columns, mask)

    split = first_leaves(row_leaves)
    inputs = (table, target_fill, far, x, made, features, columns, plain)
    first = near_field(*inputs, range(split))
    early = {mask: exchange(first[mask], mask) for mask in range(2, columns)}
    second = near_field(*inputs, range(split, row_leaves), (first[1],), (1,))
    late = {mask: exchange(second[mask], mask) for mask in late_order(columns)}
    result = jnp.concatenate([first[0], second[0]], axis=1) + late[1].astype(F32)
    for mask in early:
        result = result + jnp.concatenate([early[mask], late[mask]], axis=1).astype(F32)
    return result


def late_order(columns):
    return list(range(2, columns)) + [1]


def solution(mesh):
    placed = (
        P(None, "col"), P("col"), P("col"), P(None, "row"), P("row"), P("row", "col"), P("row", "col"),
        P("row", "col"), P("row", "col"), P("row", "col"), P("row", "col"), P("row", "col"),
        P("row", "col", None, None), P("row", "col", None, None),
    )
    return jax.shard_map(
        functools.partial(shards, rows=mesh.shape["row"], columns=mesh.shape["col"]),
        mesh=mesh, in_specs=placed, out_specs=P("col", "row"), check_vma=False,
    )
```

```python
import functools

import jax
import jax.numpy as jnp
from jax import lax
from jax.experimental import pallas as pl
from jax.experimental.pallas import tpu as pltpu
from jax.sharding import PartitionSpec as P


INV_FOUR_PI = 0.07957747154594767
SOFTENING_SQ = 0.0025
F32 = jnp.float32
BF16 = jnp.bfloat16
ENTRY_TRIP = 16
SUMS = 2
NEAR_TRIP = 16


def split3(value):
    first = value.astype(BF16).astype(F32)
    rest = value - first
    second = rest.astype(BF16).astype(F32)
    return first, second, rest - second


def feature_rows(rows):
    count = rows[0].shape[1]
    index = lax.broadcasted_iota(jnp.int32, (8, count), 0)
    out = jnp.zeros((8, count), F32)
    for position, row in enumerate(rows):
        out = jnp.where(index == position, jnp.broadcast_to(row, (8, count)), out)
    return out


def build_list(id_row, list_ref, half_id):
    slots = id_row.shape[1]
    square = (slots, slots)

    def across(row):
        return jnp.broadcast_to(row, square).T

    id_row = id_row.astype(F32)
    id_r = jnp.broadcast_to(id_row, square)
    lane = lax.broadcasted_iota(jnp.int32, square, 1)
    sub = lax.broadcasted_iota(jnp.int32, square, 0)
    same = jnp.where(id_r == across(id_row), 1.0, 0.0)
    count_r = jnp.sum(same, axis=0, keepdims=True)
    earlier_r = jnp.sum(jnp.where(sub < lane, same, 0.0), axis=0, keepdims=True)
    first_r = (earlier_r == 0.0) & (id_row >= 0.0)
    key_c = across(jnp.where(first_r, id_row, 1e9))
    rank_r = jnp.sum(jnp.where(key_c < id_r, 1.0, 0.0), axis=0, keepdims=True)
    rank_c = across(jnp.where(first_r, rank_r, -1.0))
    count_c = across(count_r)
    hit = rank_c == lane.astype(F32)
    list_r = jnp.sum(jnp.where(hit, key_c, 0.0), axis=0, keepdims=True)
    copies_r = jnp.sum(jnp.where(hit, count_c, 0.0), axis=0, keepdims=True)
    total = jnp.sum(jnp.where(first_r, 1.0, 0.0))
    half = jnp.sum(jnp.where(first_r & (id_row < float(half_id)), 1.0, 0.0))
    index = lax.broadcasted_iota(jnp.int32, (8, slots), 0)
    table = jnp.where(index == 0, jnp.broadcast_to(list_r, (8, slots)), 0.0)
    table = jnp.where(index == 1, jnp.broadcast_to(copies_r, (8, slots)), table)
    table = jnp.where(index == 2, total, table)
    table = jnp.where(index == 3, half, table)
    list_ref[...] = table.astype(jnp.int32)


def entry_loop(table_ref, s_ref, t_ref, entries_refs, base, low, high, fresh):
    column_leaves, leaf, width = s_ref.shape
    depth = t_ref.shape[1]
    slots = table_ref.shape[1]
    start, stop = (low - base) // ENTRY_TRIP, (high - base + ENTRY_TRIP - 1) // ENTRY_TRIP

    def push(k, u):
        pair = table_ref[0, jnp.minimum(k, slots - 1)]
        rhs = jnp.concatenate([t_ref[pair // column_leaves], jnp.zeros((leaf - depth, leaf), BF16)], axis=0)
        pltpu.matmul_push_rhs(rhs, staging_register=(u // 2) % 2, mxu_index=u % 2)

    def work(*accs):
        def drain(u, turn):
            row = jnp.maximum(turn * (ENTRY_TRIP // 2) + u // 2, 0)
            entries_refs[u % 2][row] = lax.rsqrt(pltpu.matmul_pop(accs[u % 8])).astype(BF16)

        if fresh:
            for acc in accs:
                pltpu.matmul_pop(acc)

        @pl.when(stop > start)
        def _():
            for u in range(2):
                push(base + start * ENTRY_TRIP + u, u)

            @pl.loop(start, stop)
            def _(turn):
                for u in range(ENTRY_TRIP):
                    k = base + turn * ENTRY_TRIP + u
                    lhs = jnp.concatenate(
                        [s_ref[table_ref[0, k] % column_leaves], jnp.zeros((leaf, leaf - width), BF16)], axis=1
                    )
                    pltpu.matmul_acc_lhs(accs[u % 8], lhs, load_staged_rhs=(u // 2) % 2)
                    push(k + 2, u + 2)
                    if u < 4:
                        drain(ENTRY_TRIP - 4 + u, turn - 1)
                    else:
                        drain(u - 4, turn)

            for u in range(2):
                pltpu.matmul_acc_lhs(accs[u], jnp.zeros((leaf, leaf), BF16), load_staged_rhs=0)
            for u in range(ENTRY_TRIP - 4, ENTRY_TRIP):
                drain(u, stop - 1)

    pl.run_scoped(work, *[pltpu.ACC(u % 2)((leaf, leaf), F32) for u in range(8)])


def near_loop(table_ref, x_ref, entries, acc_refs, base_leaf, low, high, fresh):
    chunk_leaves, rhs, leaf = acc_refs[0].shape
    column_leaves = x_ref.shape[0]

    def work(*accs):
        def drain(u, k):
            inside = (k >= low) & (k < high)
            slot = jnp.maximum(k, 0)
            t = jnp.clip(table_ref[0, slot] // column_leaves - base_leaf, 0, chunk_leaves - 1)
            copies = jnp.where(inside, table_ref[1, slot], 0).astype(F32)
            block = pltpu.matmul_pop(accs[u])
            acc_ref = acc_refs[u % len(acc_refs)]
            acc_ref[t] = acc_ref[t] + jnp.where(inside, block * copies, 0.0)

        if fresh:
            for acc in accs:
                pltpu.matmul_pop(acc)

        @pl.when(high > low)
        def _():
            for *entries_refs, base in entries:
                rows = entries_refs[0].shape[0]
                end = base + 2 * rows
                start = jnp.clip(low, base, end) // NEAR_TRIP
                stop = (jnp.clip(high, base, end) + NEAR_TRIP - 1) // NEAR_TRIP

                def push(row, u):
                    pltpu.matmul_push_rhs(
                        entries_refs[u % 2][jnp.minimum(row, rows - 1)], staging_register=(u // 2) % 2, mxu_index=u % 2
                    )

                @pl.when(stop > start)
                def _():
                    for u in range(2):
                        push(start * (NEAR_TRIP // 2) - base // 2, u)

                    @pl.loop(start, stop)
                    def _(turn):
                        for u in range(NEAR_TRIP):
                            k = turn * NEAR_TRIP + u
                            row = turn * (NEAR_TRIP // 2) - base // 2 + u // 2
                            source = table_ref[0, k] % column_leaves
                            pltpu.matmul_acc_lhs(accs[u % 16], x_ref[source], load_staged_rhs=(u // 2) % 2)
                            push(row + 1, u + 2)
                            drain((u + 8) % 16, k - 8)

                    for u in range(2):
                        pltpu.matmul_acc_lhs(accs[16 + u], jnp.zeros((16, leaf), BF16), load_staged_rhs=0)
                        pltpu.matmul_pop(accs[16 + u])

            end = (high + NEAR_TRIP - 1) // NEAR_TRIP * NEAR_TRIP
            for u in range(8):
                drain(u + 8, end - 8 + u)

    spare = pltpu.ACC(0)((rhs, leaf), F32), pltpu.ACC(1)((rhs, leaf), F32)
    flush = pltpu.ACC(0)((16, leaf), F32), pltpu.ACC(1)((16, leaf), F32)
    pl.run_scoped(work, *(spare * 8), *flush, *(spare * 7 if fresh else ()))


def first_entries_kernel(*refs, column_leaves, row_leaves, leaf, indices):
    fill_ref, inputs, index_inputs = refs[0], refs[1:6], refs[6 : 6 + indices]
    outputs, scratch = refs[6 + indices : 11 + 2 * indices], refs[11 + 2 * indices :]
    (*entries_refs, table_ref, s_ref, t_ref), index_outputs = outputs[:5], outputs[5:]
    copies, (list_ref, sem, in_sem) = scratch[:5], scratch[5:]
    moves = list(zip(inputs, copies)) + list(zip(index_inputs, index_outputs))
    loads = [pltpu.make_async_copy(src, dst, in_sem.at[i]) for i, (src, dst) in enumerate(moves)]
    for load in loads:
        load.start()
    nsrc_ref, ntgt_ref, spts_ref, area_ref, tpts_ref = copies
    for load in loads[:5]:
        load.wait()
    used = lax.broadcasted_iota(jnp.int32, nsrc_ref.shape, 1) < fill_ref[0, 0]
    ids = jnp.where(used, ntgt_ref[...] * column_leaves + nsrc_ref[...], -1)
    build_list(ids, list_ref, first_leaves(row_leaves) * column_leaves)
    copy = pltpu.make_async_copy(list_ref, table_ref, sem)
    copy.start()

    tx, ty, tz = (tpts_ref[i : i + 1, :] - 0.5 for i in range(3))
    norm = tx * tx + ty * ty + tz * tz
    h1, h2, h3 = split3(feature_rows([tx, ty, tz, jnp.ones_like(tx), norm]))
    features = jnp.concatenate([h1, h2, h1, h2, h3, h1, jnp.zeros((16,) + h1.shape[1:], F32)], axis=0).astype(BF16)
    for t in range(row_leaves):
        t_ref[t] = features[:, t * leaf : (t + 1) * leaf]

    sx, sy, sz = (spts_ref[i : i + 1, :] - 0.5 for i in range(3))
    scale = area_ref[...] * INV_FOUR_PI
    weight = 1.0 / (scale * scale)
    norm = sx * sx + sy * sy + sz * sz + SOFTENING_SQ
    g1, g2, g3 = split3(
        feature_rows([-2.0 * weight * sx, -2.0 * weight * sy, -2.0 * weight * sz, weight * norm, weight])
    )
    features = jnp.concatenate([g1, g1, g2, g2, g1, g3, jnp.zeros((16,) + g1.shape[1:], F32)], axis=0).astype(BF16)
    for s in range(column_leaves):
        column = features[:, s * leaf : (s + 1) * leaf].T
        s_ref[s] = jnp.concatenate([column, jnp.zeros((leaf, 128 - column.shape[1]), BF16)], axis=1)

    copy.wait()
    entry_loop(table_ref, s_ref, t_ref, entries_refs, 0, 0, jnp.minimum(table_ref[2, 0], 2 * entries_refs[0].shape[0]), True)
    for load in loads[5:]:
        load.wait()


def more_entries_kernel(table_ref, s_ref, t_ref, *entries_refs, first):
    slots = table_ref.shape[1]
    last = first + 2 * entries_refs[0].shape[0]
    low = jnp.clip(table_ref[3, 0], first, last) if last == slots else first
    entry_loop(table_ref, s_ref, t_ref, entries_refs, first, low, jnp.clip(table_ref[2, 0], first, last), False)


VMEM = pl.BlockSpec(memory_space=pltpu.VMEM)
SMEM = pl.BlockSpec(memory_space=pltpu.SMEM)
HBM = pl.BlockSpec(memory_space=pltpu.HBM)


def first_leaves(row_leaves):
    return row_leaves * 5 // 8


def first_count(slots):
    return max(slots * 3 // 8 // NEAR_TRIP, 1) * NEAR_TRIP


def second_count(slots):
    return max(slots // 8 // NEAR_TRIP, 1) * NEAR_TRIP


def first_entries(near_fill, near_source, near_target, source_points, source_areas, target_points, indices, leaves):
    column_leaves, row_leaves = leaves
    slots = near_source.shape[1]
    leaf = source_points.shape[1] // column_leaves
    depth = 64
    inputs = (near_source, near_target, source_points, source_areas[None, :], target_points)
    hbm_inputs = tuple(pltpu.with_memory_space_constraint(value, pltpu.HBM) for value in inputs + tuple(indices))
    return pl.pallas_call(
        functools.partial(
            first_entries_kernel, column_leaves=column_leaves, row_leaves=row_leaves, leaf=leaf,
            indices=len(indices),
        ),
        out_shape=(
            *[pltpu.VMEM((first_count(slots) // 2, leaf, leaf), BF16)] * 2,
            pltpu.SMEM((8, slots), jnp.int32),
            pltpu.VMEM((column_leaves, leaf, 128), BF16),
            pltpu.VMEM((row_leaves, depth, leaf), BF16),
        )
        + tuple(pltpu.SMEM(value.shape, jnp.int32) for value in indices),
        in_specs=[SMEM] + [HBM] * len(hbm_inputs),
        out_specs=(VMEM, VMEM, SMEM, VMEM, VMEM) + (SMEM,) * len(indices),
        scratch_shapes=[pltpu.VMEM(value.shape, value.dtype) for value in inputs]
        + [pltpu.VMEM((8, slots), jnp.int32), pltpu.SemaphoreType.DMA, pltpu.SemaphoreType.DMA((len(hbm_inputs),))],
        compiler_params=pltpu.CompilerParams(vmem_limit_bytes=10 << 20),
        cost_estimate=pl.CostEstimate(flops=8_000_000_000, bytes_accessed=1 << 20, transcendentals=0),
        name="entries",
    )(near_fill, *hbm_inputs)


def more_entries(table, s_features, t_features, first, count):
    leaf = s_features.shape[1]
    return pl.pallas_call(
        functools.partial(more_entries_kernel, first=first),
        out_shape=(pltpu.VMEM((count // 2, leaf, leaf), BF16),) * 2,
        in_specs=[SMEM, VMEM, VMEM],
        out_specs=(VMEM, VMEM),
        compiler_params=pltpu.CompilerParams(vmem_limit_bytes=4 << 20),
        cost_estimate=pl.CostEstimate(flops=8_000_000_000, bytes_accessed=1 << 20, transcendentals=0),
        name="entries_rest",
    )(table, s_features, t_features)


def far_kernel(*refs, pieces, plain, leaf, unroll):
    (sfill_ref, fsrc_ref, ftgt_ref, frank_ref, left_ref, right_ref) = refs[:6]
    piece_refs = refs[6 : 6 + pieces]
    x_ref, acc_ref, coef_ref = refs[6 + pieces :]
    column_leaves, rhs, _ = x_ref.shape
    far_slots, rank, _ = left_ref.shape

    lane = lax.broadcasted_iota(jnp.int32, (rhs, leaf), 1)
    if not plain:
        parity = lax.rem(lax.axis_index("row"), 2)
    for s in range(column_leaves):
        window = slice(s * leaf, (s + 1) * leaf)
        if plain:
            block = piece_refs[0][:, window].astype(F32)
        else:
            rows = []
            for j in range(pieces // 2):
                mine = piece_refs[j][:, window].astype(F32)
                other = piece_refs[pieces // 2 + j][:, window].astype(F32)
                rows.append(jnp.where(parity == 0, mine, other))
                rows.append(jnp.where(parity == 0, other, mine))
            block = jnp.concatenate(rows, axis=0)
        x_ref[s] = jnp.where(lane < sfill_ref[s], block, 0.0).astype(BF16)

    acc_ref[...] = jnp.zeros_like(acc_ref)

    rank_lane = lax.broadcasted_iota(jnp.int32, (rhs, rank), 1)

    @pl.loop(0, far_slots // unroll)
    def _(turn):
        for u in range(unroll):
            k = turn * unroll + u
            coef = lax.dot_general(
                x_ref[fsrc_ref[0, k]], right_ref[k], (((1,), (1,)), ((), ())), preferred_element_type=F32
            )
            coef_ref[k] = jnp.where(rank_lane < frank_ref[0, k], coef, 0.0).astype(BF16)

    @pl.loop(0, far_slots // unroll)
    def _(turn):
        blocks = []
        for u in range(unroll):
            k = turn * unroll + u
            blocks.append(jnp.dot(coef_ref[k], left_ref[k], preferred_element_type=F32))
        for u in range(unroll):
            t = ftgt_ref[0, turn * unroll + u]
            acc_ref[t] = acc_ref[t] + blocks[u]


def near_kernel(*refs, base_leaf, plain, out_carried, firsts, complete):
    carried, arrays = len(out_carried), 2 * len(firsts)
    (table_ref, tfill_ref, far_ref, x_ref, s_ref, t_ref), made_refs = refs[:6], refs[6 : 6 + arrays]
    carried_refs = refs[6 + arrays : 6 + arrays + carried]
    tail = len(refs) - SUMS
    out_refs, rest_refs, acc_refs = refs[6 + arrays + carried : tail - 2], refs[tail - 2 : tail], refs[tail:]
    chunk_leaves, rhs, leaf = acc_refs[0].shape
    total, half = table_ref[2, 0], table_ref[3, 0]
    low = half if base_leaf > 0 else 0
    high = total if base_leaf + chunk_leaves == far_ref.shape[0] else half
    made = firsts[-1] + 2 * made_refs[-1].shape[0]
    for acc_ref in acc_refs:
        acc_ref[...] = jnp.zeros_like(acc_ref)
    near_loop(
        table_ref, x_ref, [(made_refs[2 * i], made_refs[2 * i + 1], first) for i, first in enumerate(firsts)], acc_refs,
        base_leaf, jnp.minimum(low, made), jnp.minimum(high, made), base_leaf == 0,
    )
    if not complete:
        rest = (jnp.maximum(low, made), jnp.maximum(high, made))
        entry_loop(table_ref, s_ref, t_ref, rest_refs, made, *rest, False)
        near_loop(table_ref, x_ref, [(*rest_refs, made)], acc_refs, base_leaf, *rest, False)

    if plain:
        lane_t = lax.broadcasted_iota(jnp.int32, (rhs, leaf), 1)
        for t in range(chunk_leaves):
            value = sum((acc_ref[t] for acc_ref in acc_refs), far_ref[base_leaf + t])
            out_refs[0][:, t * leaf : (t + 1) * leaf] = jnp.where(lane_t < tfill_ref[base_leaf + t], value, 0.0)
    else:
        owners = len(out_refs)
        height = rhs // owners
        lane_t = lax.broadcasted_iota(jnp.int32, (height, leaf), 1)
        base = lax.axis_index("col") ^ (lax.axis_index("row") // 2)
        for m in range(owners):
            start = pl.multiple_of((base ^ m) * height, height)
            shift = out_refs[m].shape[1] - chunk_leaves * leaf
            if shift:
                out_refs[m][:, :shift] = carried_refs[out_carried.index(m)][...]
            for t in range(chunk_leaves):
                rows = pl.ds(start, height)
                value = sum((acc_ref[t, rows, :] for acc_ref in acc_refs), far_ref[base_leaf + t, rows, :])
                value = jnp.where(lane_t < tfill_ref[base_leaf + t], value, 0.0)
                window = slice(shift + t * leaf, shift + (t + 1) * leaf)
                out_refs[m][:, window] = value.astype(out_refs[m].dtype)


def far_field(source_fill, row_leaves, far_source, far_target, far_rank, left, right, pieces, plain):
    column_leaves = source_fill.shape[0]
    far_slots, rank, leaf = left.shape
    rhs = sum(p.shape[0] for p in pieces)
    vmem = pl.BlockSpec(memory_space=pltpu.VMEM)
    smem = pl.BlockSpec(memory_space=pltpu.SMEM)
    unroll = next(u for u in (32, 16, 8, 4, 2, 1) if far_slots % u == 0)
    return pl.pallas_call(
        functools.partial(far_kernel, pieces=len(pieces), plain=plain, leaf=leaf, unroll=unroll),
        out_shape=(pltpu.VMEM((column_leaves, rhs, leaf), BF16), pltpu.VMEM((row_leaves, rhs, leaf), F32)),
        in_specs=[smem] * 4 + [vmem] * (2 + len(pieces)),
        out_specs=(vmem, vmem),
        scratch_shapes=[pltpu.VMEM((far_slots, rhs, rank), BF16)],
        compiler_params=pltpu.CompilerParams(vmem_limit_bytes=12 << 20),
        cost_estimate=pl.CostEstimate(flops=2_000_000_000, bytes_accessed=8 << 20, transcendentals=0),
        name="far",
    )(source_fill, far_source, far_target, far_rank, left, right, *pieces)


def near_field(table, target_fill, far, x, made, features, owners, plain, leaves, carried=(), out_carried=()):
    firsts, arrays = zip(*made)
    made = [value for pair in arrays for value in pair]
    _, rhs, leaf = far.shape
    width = len(leaves) * leaf
    if plain:
        out_shape = (jax.ShapeDtypeStruct((rhs, width), F32),)
    else:
        out_shape = tuple(
            jax.ShapeDtypeStruct(
                (rhs // owners, width + (carried[0].shape[1] if m in out_carried else 0)), F32 if m == 0 else BF16
            )
            for m in range(owners)
        )
    rest = table.shape[1] // 2 - sum(value.shape[0] for value in made) // 2
    complete = rest == 0
    rest = max(rest, 1)
    return pl.pallas_call(
        functools.partial(
            near_kernel, base_leaf=leaves[0], firsts=firsts, complete=complete, plain=plain,
            out_carried=tuple(out_carried),
        ),
        out_shape=out_shape,
        in_specs=[SMEM] * 2 + [VMEM] * (4 + len(made) + len(carried)),
        out_specs=(VMEM,) * len(out_shape),
        scratch_shapes=[pltpu.VMEM((rest, leaf, leaf), BF16)] * 2 + [pltpu.VMEM((len(leaves), rhs, leaf), F32)] * SUMS,
        compiler_params=pltpu.CompilerParams(vmem_limit_bytes=(8 if complete else 24) << 20),
        cost_estimate=pl.CostEstimate(flops=4_000_000_000, bytes_accessed=8 << 20, transcendentals=0),
        name="near",
    )(table, target_fill, far, x, *features, *made, *carried)


def shards(
    source_points, source_areas, source_fill, target_points, target_fill, charges, near_fill, near_source,
    near_target, far_source, far_target, far_rank, left_basis, right_basis, *, rows, columns,
):
    plain = charges.shape[0] % 8 != 0 or rows != 2 * columns
    if plain:
        pieces = [lax.all_gather(charges, "row", axis=0, tiled=True)]
    else:

        def swap(value, axis, size, mask):
            return lax.ppermute(value, axis, [(i, i ^ mask) for i in range(size)])

        pieces = [charges] + [swap(charges, "row", rows, mask) for mask in range(2, rows, 2)]
    row_leaves, column_leaves = target_fill.shape[0], source_fill.shape[0]
    first_outs = first_entries(
        near_fill, near_source, near_target, source_points, source_areas, target_points,
        (source_fill, target_fill, far_source, far_target, far_rank), (column_leaves, row_leaves),
    )
    *entries, table, s_features, t_features = first_outs[:5]
    features = (s_features, t_features)
    source_fill, target_fill, far_source, far_target, far_rank = first_outs[5:]
    if not plain:
        pieces, table = lax.optimization_barrier((pieces, table))
        pieces = pieces + [swap(piece, "row", rows, 1) for piece in pieces]
    slots = near_source.shape[1]
    first, second = first_count(slots), second_count(slots)
    more = list(more_entries(table, *features, first, second))
    if not plain:
        pieces, more[0] = lax.optimization_barrier((pieces, more[0]))
    made = [(0, entries), (first, more)]
    x, far = far_field(
        source_fill, row_leaves, far_source, far_target, far_rank, left_basis[0], right_basis[0], pieces, plain
    )
    if plain or row_leaves < 2 or columns < 3:
        outs = near_field(table, target_fill, far, x, made, features, columns, plain, range(row_leaves))
        if plain:
            return lax.psum_scatter(outs[0], "col", scatter_dimension=0, tiled=True)
        result = outs[0]
        for mask in reversed(range(1, columns)):
            result = result + swap(outs[mask], "col", columns, mask).astype(F32)
        return result

    def exchange(value, mask):
        return swap(value, "col", columns, mask)

    split = first_leaves(row_leaves)
    one = near_field(table, target_fill, far, x, made, features, columns, plain, range(split))
    early = {mask: exchange(one[mask], mask) for mask in exchange_order(columns)}
    table, one_last = lax.optimization_barrier((table, one[0]))
    made = made + [(first + second, more_entries(table, *features, first + second, slots - first - second))]
    two = near_field(table, target_fill, far, x, made, features, columns, plain, range(split, row_leaves))
    late = {mask: exchange(two[mask], mask) for mask in exchange_order(columns)}
    result = jnp.concatenate([one_last, two[0]], axis=1)
    for mask in early:
        result = result + jnp.concatenate([early[mask], late[mask]], axis=1).astype(F32)
    return result


def exchange_order(columns):
    return list(range(2, columns)) + [1]


def solution(mesh):
    placed = (
        P(None, "col"), P("col"), P("col"), P(None, "row"), P("row"), P("row", "col"), P("row", "col"),
        P("row", "col"), P("row", "col"), P("row", "col"), P("row", "col"), P("row", "col"),
        P("row", "col", None, None), P("row", "col", None, None),
    )
    return jax.shard_map(
        functools.partial(shards, rows=mesh.shape["row"], columns=mesh.shape["col"]),
        mesh=mesh, in_specs=placed, out_specs=P("col", "row"), check_vma=False,
    )
```

```python
import functools

import jax
import jax.numpy as jnp
from jax import lax
from jax.experimental import pallas as pl
from jax.experimental.pallas import tpu as pltpu
from jax.sharding import PartitionSpec as P


INV_FOUR_PI = 0.07957747154594767
SOFTENING_SQ = 0.0025
F32 = jnp.float32
BF16 = jnp.bfloat16
ENTRY_TRIP = 16
SUMS = 2
NEAR_TRIP = 16


def split3(value):
    first = value.astype(BF16).astype(F32)
    rest = value - first
    second = rest.astype(BF16).astype(F32)
    return first, second, rest - second


def feature_rows(rows):
    count = rows[0].shape[1]
    index = lax.broadcasted_iota(jnp.int32, (8, count), 0)
    out = jnp.zeros((8, count), F32)
    for position, row in enumerate(rows):
        out = jnp.where(index == position, jnp.broadcast_to(row, (8, count)), out)
    return out


def build_list(id_row, list_ref, half_id):
    slots = id_row.shape[1]
    square = (slots, slots)

    def across(row):
        return jnp.broadcast_to(row, square).T

    id_row = id_row.astype(F32)
    id_r = jnp.broadcast_to(id_row, square)
    lane = lax.broadcasted_iota(jnp.int32, square, 1)
    sub = lax.broadcasted_iota(jnp.int32, square, 0)
    same = jnp.where(id_r == across(id_row), 1.0, 0.0)
    count_r = jnp.sum(same, axis=0, keepdims=True)
    earlier_r = jnp.sum(jnp.where(sub < lane, same, 0.0), axis=0, keepdims=True)
    first_r = (earlier_r == 0.0) & (id_row >= 0.0)
    key_c = across(jnp.where(first_r, id_row, 1e9))
    rank_r = jnp.sum(jnp.where(key_c < id_r, 1.0, 0.0), axis=0, keepdims=True)
    rank_c = across(jnp.where(first_r, rank_r, -1.0))
    count_c = across(count_r)
    hit = rank_c == lane.astype(F32)
    list_r = jnp.sum(jnp.where(hit, key_c, 0.0), axis=0, keepdims=True)
    copies_r = jnp.sum(jnp.where(hit, count_c, 0.0), axis=0, keepdims=True)
    total = jnp.sum(jnp.where(first_r, 1.0, 0.0))
    half = jnp.sum(jnp.where(first_r & (id_row < float(half_id)), 1.0, 0.0))
    index = lax.broadcasted_iota(jnp.int32, (8, slots), 0)
    table = jnp.where(index == 0, jnp.broadcast_to(list_r, (8, slots)), 0.0)
    table = jnp.where(index == 1, jnp.broadcast_to(copies_r, (8, slots)), table)
    table = jnp.where(index == 2, total, table)
    table = jnp.where(index == 3, half, table)
    list_ref[...] = table.astype(jnp.int32)


def entry_loop(table_ref, s_ref, t_ref, entries_refs, base, low, high, fresh):
    column_leaves, leaf, width = s_ref.shape
    depth = t_ref.shape[1]
    slots = table_ref.shape[1]
    start, stop = (low - base) // ENTRY_TRIP, (high - base + ENTRY_TRIP - 1) // ENTRY_TRIP

    def push(k, u):
        pair = table_ref[0, jnp.minimum(k, slots - 1)]
        rhs = jnp.concatenate([t_ref[pair // column_leaves], jnp.zeros((leaf - depth, leaf), BF16)], axis=0)
        pltpu.matmul_push_rhs(rhs, staging_register=(u // 2) % 2, mxu_index=u % 2)

    def work(*accs):
        def drain(u, turn):
            row = jnp.maximum(turn * (ENTRY_TRIP // 2) + u // 2, 0)
            entries_refs[u % 2][row] = lax.rsqrt(pltpu.matmul_pop(accs[u % 8])).astype(BF16)

        if fresh:
            for acc in accs:
                pltpu.matmul_pop(acc)

        @pl.when(stop > start)
        def _():
            for u in range(2):
                push(base + start * ENTRY_TRIP + u, u)

            @pl.loop(start, stop)
            def _(turn):
                for u in range(ENTRY_TRIP):
                    k = base + turn * ENTRY_TRIP + u
                    lhs = jnp.concatenate(
                        [s_ref[table_ref[0, k] % column_leaves], jnp.zeros((leaf, leaf - width), BF16)], axis=1
                    )
                    pltpu.matmul_acc_lhs(accs[u % 8], lhs, load_staged_rhs=(u // 2) % 2)
                    push(k + 2, u + 2)
                    if u < 4:
                        drain(ENTRY_TRIP - 4 + u, turn - 1)
                    else:
                        drain(u - 4, turn)

            for u in range(2):
                pltpu.matmul_acc_lhs(accs[u], jnp.zeros((leaf, leaf), BF16), load_staged_rhs=0)
            for u in range(ENTRY_TRIP - 4, ENTRY_TRIP):
                drain(u, stop - 1)

    pl.run_scoped(work, *[pltpu.ACC(u % 2)((leaf, leaf), F32) for u in range(8)])


def near_loop(table_ref, x_ref, entries, acc_refs, base_leaf, low, high, fresh):
    chunk_leaves, rhs, leaf = acc_refs[0].shape
    column_leaves = x_ref.shape[0]

    def work(*accs):
        def drain(u, k):
            inside = (k >= low) & (k < high)
            slot = jnp.maximum(k, 0)
            t = jnp.clip(table_ref[0, slot] // column_leaves - base_leaf, 0, chunk_leaves - 1)
            copies = jnp.where(inside, table_ref[1, slot], 0).astype(F32)
            block = pltpu.matmul_pop(accs[u])
            acc_ref = acc_refs[u % len(acc_refs)]
            acc_ref[t] = acc_ref[t] + jnp.where(inside, block * copies, 0.0)

        if fresh:
            for acc in accs:
                pltpu.matmul_pop(acc)

        @pl.when(high > low)
        def _():
            for *entries_refs, base in entries:
                rows = entries_refs[0].shape[0]
                end = base + 2 * rows
                start = jnp.clip(low, base, end) // NEAR_TRIP
                stop = (jnp.clip(high, base, end) + NEAR_TRIP - 1) // NEAR_TRIP

                def push(row, u):
                    pltpu.matmul_push_rhs(
                        entries_refs[u % 2][jnp.minimum(row, rows - 1)], staging_register=(u // 2) % 2, mxu_index=u % 2
                    )

                @pl.when(stop > start)
                def _():
                    for u in range(2):
                        push(start * (NEAR_TRIP // 2) - base // 2, u)

                    @pl.loop(start, stop)
                    def _(turn):
                        for u in range(NEAR_TRIP):
                            k = turn * NEAR_TRIP + u
                            row = turn * (NEAR_TRIP // 2) - base // 2 + u // 2
                            source = table_ref[0, k] % column_leaves
                            pltpu.matmul_acc_lhs(accs[u % 16], x_ref[source], load_staged_rhs=(u // 2) % 2)
                            push(row + 1, u + 2)
                            drain((u + 8) % 16, k - 8)

                    for u in range(2):
                        pltpu.matmul_acc_lhs(accs[16 + u], jnp.zeros((16, leaf), BF16), load_staged_rhs=0)
                        pltpu.matmul_pop(accs[16 + u])

            end = (high + NEAR_TRIP - 1) // NEAR_TRIP * NEAR_TRIP
            for u in range(8):
                drain(u + 8, end - 8 + u)

    spare = pltpu.ACC(0)((rhs, leaf), F32), pltpu.ACC(1)((rhs, leaf), F32)
    flush = pltpu.ACC(0)((16, leaf), F32), pltpu.ACC(1)((16, leaf), F32)
    pl.run_scoped(work, *(spare * 8), *flush, *(spare * 7 if fresh else ()))


def first_entries_kernel(*refs, column_leaves, row_leaves, leaf, indices, bases):
    fill_ref, inputs, index_inputs = refs[0], refs[1:6], refs[6 : 6 + indices + bases]
    moved = indices + bases
    outputs, scratch = refs[6 + moved : 11 + 2 * moved], refs[11 + 2 * moved :]
    (*entries_refs, table_ref, s_ref, t_ref), index_outputs = outputs[:5], outputs[5:]
    copies, (list_ref, sem, in_sem) = scratch[:5], scratch[5:]
    moves = list(zip(inputs, copies)) + list(zip(index_inputs, index_outputs))
    loads = [pltpu.make_async_copy(src, dst, in_sem.at[i]) for i, (src, dst) in enumerate(moves)]
    for load in loads:
        load.start()
    nsrc_ref, ntgt_ref, spts_ref, area_ref, tpts_ref = copies
    for load in loads[:2]:
        load.wait()
    used = lax.broadcasted_iota(jnp.int32, nsrc_ref.shape, 1) < fill_ref[0, 0]
    ids = jnp.where(used, ntgt_ref[...] * column_leaves + nsrc_ref[...], -1)
    build_list(ids, list_ref, first_leaves(row_leaves) * column_leaves)
    copy = pltpu.make_async_copy(list_ref, table_ref, sem)
    copy.start()
    for load in loads[2:5]:
        load.wait()

    tx, ty, tz = (tpts_ref[i : i + 1, :] - 0.5 for i in range(3))
    norm = tx * tx + ty * ty + tz * tz
    h1, h2, h3 = split3(feature_rows([tx, ty, tz, jnp.ones_like(tx), norm]))
    features = jnp.concatenate([h1, h2, h1, h2, h3, h1, jnp.zeros((16,) + h1.shape[1:], F32)], axis=0).astype(BF16)
    for t in range(row_leaves):
        t_ref[t] = features[:, t * leaf : (t + 1) * leaf]

    sx, sy, sz = (spts_ref[i : i + 1, :] - 0.5 for i in range(3))
    scale = area_ref[...] * INV_FOUR_PI
    weight = 1.0 / (scale * scale)
    norm = sx * sx + sy * sy + sz * sz + SOFTENING_SQ
    g1, g2, g3 = split3(
        feature_rows([-2.0 * weight * sx, -2.0 * weight * sy, -2.0 * weight * sz, weight * norm, weight])
    )
    features = jnp.concatenate([g1, g1, g2, g2, g1, g3, jnp.zeros((16,) + g1.shape[1:], F32)], axis=0).astype(BF16)
    for s in range(column_leaves):
        column = features[:, s * leaf : (s + 1) * leaf].T
        s_ref[s] = jnp.concatenate([column, jnp.zeros((leaf, 128 - column.shape[1]), BF16)], axis=1)

    copy.wait()
    entry_loop(table_ref, s_ref, t_ref, entries_refs, 0, 0, jnp.minimum(table_ref[2, 0], 2 * entries_refs[0].shape[0]), True)
    for load in loads[5:]:
        load.wait()


def more_entries_kernel(table_ref, s_ref, t_ref, *entries_refs, first):
    last = first + 2 * entries_refs[0].shape[0]
    entry_loop(table_ref, s_ref, t_ref, entries_refs, first, first, jnp.clip(table_ref[2, 0], first, last), False)


VMEM = pl.BlockSpec(memory_space=pltpu.VMEM)
SMEM = pl.BlockSpec(memory_space=pltpu.SMEM)
HBM = pl.BlockSpec(memory_space=pltpu.HBM)


def first_leaves(row_leaves):
    return row_leaves * 9 // 16


def first_count(slots):
    return max(slots * 3 // 8 // NEAR_TRIP, 1) * NEAR_TRIP


def second_count(slots):
    return max(slots // 8 // NEAR_TRIP, 1) * NEAR_TRIP


def first_entries(near_fill, near_source, near_target, source_points, source_areas, target_points, indices, bases, leaves):
    column_leaves, row_leaves = leaves
    slots = near_source.shape[1]
    leaf = source_points.shape[1] // column_leaves
    depth = 64
    inputs = (near_source, near_target, source_points, source_areas[None, :], target_points)
    hbm_inputs = tuple(pltpu.with_memory_space_constraint(value, pltpu.HBM) for value in inputs + tuple(indices) + tuple(bases))
    return pl.pallas_call(
        functools.partial(
            first_entries_kernel, column_leaves=column_leaves, row_leaves=row_leaves, leaf=leaf,
            indices=len(indices), bases=len(bases),
        ),
        out_shape=(
            *[pltpu.VMEM((first_count(slots) // 2, leaf, leaf), BF16)] * 2,
            pltpu.SMEM((8, slots), jnp.int32),
            pltpu.VMEM((column_leaves, leaf, 128), BF16),
            pltpu.VMEM((row_leaves, depth, leaf), BF16),
        )
        + tuple(pltpu.SMEM(value.shape, jnp.int32) for value in indices)
        + tuple(pltpu.VMEM(value.shape, value.dtype) for value in bases),
        in_specs=[SMEM] + [HBM] * len(hbm_inputs),
        out_specs=(VMEM, VMEM, SMEM, VMEM, VMEM) + (SMEM,) * len(indices) + (VMEM,) * len(bases),
        scratch_shapes=[pltpu.VMEM(value.shape, value.dtype) for value in inputs]
        + [pltpu.VMEM((8, slots), jnp.int32), pltpu.SemaphoreType.DMA, pltpu.SemaphoreType.DMA((len(hbm_inputs),))],
        compiler_params=pltpu.CompilerParams(vmem_limit_bytes=10 << 20),
        cost_estimate=pl.CostEstimate(flops=8_000_000_000, bytes_accessed=1 << 20, transcendentals=0),
        name="entries",
    )(near_fill, *hbm_inputs)


def more_entries(table, s_features, t_features, first, count):
    leaf = s_features.shape[1]
    return pl.pallas_call(
        functools.partial(more_entries_kernel, first=first),
        out_shape=(pltpu.VMEM((count // 2, leaf, leaf), BF16),) * 2,
        in_specs=[SMEM, VMEM, VMEM],
        out_specs=(VMEM, VMEM),
        compiler_params=pltpu.CompilerParams(vmem_limit_bytes=4 << 20),
        cost_estimate=pl.CostEstimate(flops=8_000_000_000, bytes_accessed=1 << 20, transcendentals=0),
        name="entries_rest",
    )(table, s_features, t_features)


def far_kernel(*refs, pieces, plain, leaf, unroll):
    (sfill_ref, fsrc_ref, ftgt_ref, frank_ref, left_ref, right_ref) = refs[:6]
    piece_refs = refs[6 : 6 + pieces]
    x_ref, acc_ref, coef_ref = refs[6 + pieces :]
    column_leaves, rhs, _ = x_ref.shape
    far_slots, rank, _ = left_ref.shape

    lane = lax.broadcasted_iota(jnp.int32, (rhs, leaf), 1)
    if not plain:
        parity = lax.rem(lax.axis_index("row"), 2)
    for s in range(column_leaves):
        window = slice(s * leaf, (s + 1) * leaf)
        if plain:
            block = piece_refs[0][:, window].astype(F32)
        else:
            rows = []
            for j in range(pieces // 2):
                mine = piece_refs[j][:, window].astype(F32)
                other = piece_refs[pieces // 2 + j][:, window].astype(F32)
                rows.append(jnp.where(parity == 0, mine, other))
                rows.append(jnp.where(parity == 0, other, mine))
            block = jnp.concatenate(rows, axis=0)
        x_ref[s] = jnp.where(lane < sfill_ref[s], block, 0.0).astype(BF16)

    acc_ref[...] = jnp.zeros_like(acc_ref)

    rank_lane = lax.broadcasted_iota(jnp.int32, (rhs, rank), 1)

    @pl.loop(0, far_slots // unroll)
    def _(turn):
        for u in range(unroll):
            k = turn * unroll + u
            coef = lax.dot_general(
                x_ref[fsrc_ref[0, k]], right_ref[k], (((1,), (1,)), ((), ())), preferred_element_type=F32
            )
            coef_ref[k] = jnp.where(rank_lane < frank_ref[0, k], coef, 0.0).astype(BF16)

    @pl.loop(0, far_slots // unroll)
    def _(turn):
        blocks = []
        for u in range(unroll):
            k = turn * unroll + u
            blocks.append(jnp.dot(coef_ref[k], left_ref[k], preferred_element_type=F32))
        for u in range(unroll):
            t = ftgt_ref[0, turn * unroll + u]
            acc_ref[t] = acc_ref[t] + blocks[u]


def near_kernel(*refs, base_leaf, plain, out_carried, firsts, complete):
    carried, arrays = len(out_carried), 2 * len(firsts)
    (table_ref, tfill_ref, far_ref, x_ref, s_ref, t_ref), made_refs = refs[:6], refs[6 : 6 + arrays]
    carried_refs = refs[6 + arrays : 6 + arrays + carried]
    tail = len(refs) - SUMS
    out_refs, rest_refs, acc_refs = refs[6 + arrays + carried : tail - 2], refs[tail - 2 : tail], refs[tail:]
    chunk_leaves, rhs, leaf = acc_refs[0].shape
    total, half = table_ref[2, 0], table_ref[3, 0]
    low = half if base_leaf > 0 else 0
    high = total if base_leaf + chunk_leaves == far_ref.shape[0] else half
    made = firsts[-1] + 2 * made_refs[-1].shape[0]
    for acc_ref in acc_refs:
        acc_ref[...] = jnp.zeros_like(acc_ref)
    near_loop(
        table_ref, x_ref, [(made_refs[2 * i], made_refs[2 * i + 1], first) for i, first in enumerate(firsts)], acc_refs,
        base_leaf, jnp.minimum(low, made), jnp.minimum(high, made), base_leaf == 0,
    )
    if not complete:
        rest = (jnp.maximum(low, made), jnp.maximum(high, made))
        entry_loop(table_ref, s_ref, t_ref, rest_refs, made, *rest, False)
        near_loop(table_ref, x_ref, [(*rest_refs, made)], acc_refs, base_leaf, *rest, False)

    if plain:
        lane_t = lax.broadcasted_iota(jnp.int32, (rhs, leaf), 1)
        for t in range(chunk_leaves):
            value = sum((acc_ref[t] for acc_ref in acc_refs), far_ref[base_leaf + t])
            out_refs[0][:, t * leaf : (t + 1) * leaf] = jnp.where(lane_t < tfill_ref[base_leaf + t], value, 0.0)
    else:
        owners = len(out_refs)
        height = rhs // owners
        lane_t = lax.broadcasted_iota(jnp.int32, (height, leaf), 1)
        base = lax.axis_index("col") ^ (lax.axis_index("row") // 2)
        for m in range(owners):
            start = pl.multiple_of((base ^ m) * height, height)
            shift = out_refs[m].shape[1] - chunk_leaves * leaf
            if shift:
                out_refs[m][:, :shift] = carried_refs[out_carried.index(m)][...]
            for t in range(chunk_leaves):
                rows = pl.ds(start, height)
                value = sum((acc_ref[t, rows, :] for acc_ref in acc_refs), far_ref[base_leaf + t, rows, :])
                value = jnp.where(lane_t < tfill_ref[base_leaf + t], value, 0.0)
                window = slice(shift + t * leaf, shift + (t + 1) * leaf)
                out_refs[m][:, window] = value.astype(out_refs[m].dtype)


def far_field(source_fill, row_leaves, far_source, far_target, far_rank, left, right, pieces, plain):
    column_leaves = source_fill.shape[0]
    far_slots, rank, leaf = left.shape
    rhs = sum(p.shape[0] for p in pieces)
    vmem = pl.BlockSpec(memory_space=pltpu.VMEM)
    smem = pl.BlockSpec(memory_space=pltpu.SMEM)
    unroll = next(u for u in (32, 16, 8, 4, 2, 1) if far_slots % u == 0)
    return pl.pallas_call(
        functools.partial(far_kernel, pieces=len(pieces), plain=plain, leaf=leaf, unroll=unroll),
        out_shape=(pltpu.VMEM((column_leaves, rhs, leaf), BF16), pltpu.VMEM((row_leaves, rhs, leaf), F32)),
        in_specs=[smem] * 4 + [vmem] * (2 + len(pieces)),
        out_specs=(vmem, vmem),
        scratch_shapes=[pltpu.VMEM((far_slots, rhs, rank), BF16)],
        compiler_params=pltpu.CompilerParams(vmem_limit_bytes=12 << 20),
        cost_estimate=pl.CostEstimate(flops=2_000_000_000, bytes_accessed=8 << 20, transcendentals=0),
        name="far",
    )(source_fill, far_source, far_target, far_rank, left, right, *pieces)


def near_field(table, target_fill, far, x, made, features, owners, plain, leaves, carried=(), out_carried=()):
    firsts, arrays = zip(*made)
    made = [value for pair in arrays for value in pair]
    _, rhs, leaf = far.shape
    width = len(leaves) * leaf
    if plain:
        out_shape = (jax.ShapeDtypeStruct((rhs, width), F32),)
    else:
        out_shape = tuple(
            jax.ShapeDtypeStruct(
                (rhs // owners, width + (carried[0].shape[1] if m in out_carried else 0)), F32 if m == 0 else BF16
            )
            for m in range(owners)
        )
    rest = table.shape[1] // 2 - sum(value.shape[0] for value in made) // 2
    complete = rest == 0
    rest = max(rest, 1)
    return pl.pallas_call(
        functools.partial(
            near_kernel, base_leaf=leaves[0], firsts=firsts, complete=complete, plain=plain,
            out_carried=tuple(out_carried),
        ),
        out_shape=out_shape,
        in_specs=[SMEM] * 2 + [VMEM] * (4 + len(made) + len(carried)),
        out_specs=(VMEM,) * len(out_shape),
        scratch_shapes=[pltpu.VMEM((rest, leaf, leaf), BF16)] * 2 + [pltpu.VMEM((len(leaves), rhs, leaf), F32)] * SUMS,
        compiler_params=pltpu.CompilerParams(vmem_limit_bytes=20 << 20),
        cost_estimate=pl.CostEstimate(flops=4_000_000_000, bytes_accessed=8 << 20, transcendentals=0),
        name="near",
    )(table, target_fill, far, x, *features, *made, *carried)


def shards(
    source_points, source_areas, source_fill, target_points, target_fill, charges, near_fill, near_source,
    near_target, far_source, far_target, far_rank, left_basis, right_basis, *, rows, columns,
):
    plain = charges.shape[0] % 8 != 0 or rows != 2 * columns
    if plain:
        pieces = [lax.all_gather(charges, "row", axis=0, tiled=True)]
    else:

        def swap(value, axis, size, mask):
            return lax.ppermute(value, axis, [(i, i ^ mask) for i in range(size)])

        pieces = [charges] + [swap(charges, "row", rows, mask) for mask in range(2, rows, 2)]
    row_leaves, column_leaves = target_fill.shape[0], source_fill.shape[0]
    first_outs = first_entries(
        near_fill, near_source, near_target, source_points, source_areas, target_points,
        (source_fill, target_fill, far_source, far_target, far_rank), (left_basis[0], right_basis[0]),
        (column_leaves, row_leaves),
    )
    *entries, table, s_features, t_features = first_outs[:5]
    features = (s_features, t_features)
    source_fill, target_fill, far_source, far_target, far_rank, left, right = first_outs[5:]
    if not plain:
        pieces, table = lax.optimization_barrier((pieces, table))
        pieces = pieces + [swap(piece, "row", rows, 1) for piece in pieces]
    slots = near_source.shape[1]
    first, second = first_count(slots), second_count(slots)
    more = list(more_entries(table, *features, first, second))
    if not plain:
        pieces, more[0] = lax.optimization_barrier((pieces, more[0]))
    made = [(0, entries), (first, more)]
    x, far = far_field(
        source_fill, row_leaves, far_source, far_target, far_rank, left, right, pieces, plain
    )
    if plain or row_leaves < 2 or columns < 3:
        outs = near_field(table, target_fill, far, x, made, features, columns, plain, range(row_leaves))
        if plain:
            return lax.psum_scatter(outs[0], "col", scatter_dimension=0, tiled=True)
        result = outs[0]
        for mask in reversed(range(1, columns)):
            result = result + swap(outs[mask], "col", columns, mask).astype(F32)
        return result

    def exchange(value, mask):
        return swap(value, "col", columns, mask)

    split = first_leaves(row_leaves)
    inputs = (table, target_fill, far, x, made, features, columns, plain)
    one = near_field(*inputs, range(split))
    early = {mask: exchange(one[mask], mask) for mask in far_masks(columns)}
    two = near_field(*inputs, range(split, row_leaves), (one[1],), (1,))
    late = {mask: exchange(two[mask], mask) for mask in far_masks(columns) + [1]}
    result = jnp.concatenate([one[0], two[0]], axis=1) + late[1].astype(F32)
    for mask in early:
        result = result + jnp.concatenate([early[mask], late[mask]], axis=1).astype(F32)
    return result


def far_masks(columns):
    return list(range(2, columns))


def solution(mesh):
    placed = (
        P(None, "col"), P("col"), P("col"), P(None, "row"), P("row"), P("row", "col"), P("row", "col"),
        P("row", "col"), P("row", "col"), P("row", "col"), P("row", "col"), P("row", "col"),
        P("row", "col", None, None), P("row", "col", None, None),
    )
    return jax.shard_map(
        functools.partial(shards, rows=mesh.shape["row"], columns=mesh.shape["col"]),
        mesh=mesh, in_specs=placed, out_specs=P("col", "row"), check_vma=False,
    )
```

```python
import functools

import jax
import jax.numpy as jnp
from jax import lax
from jax.experimental import pallas as pl
from jax.experimental.pallas import tpu as pltpu
from jax.sharding import PartitionSpec as P


INV_FOUR_PI = 0.07957747154594767
SOFTENING_SQ = 0.0025
F32 = jnp.float32
BF16 = jnp.bfloat16
ENTRY_TRIP = 16
SUMS = 1
NEAR_TRIP = 16


def split3(value):
    first = value.astype(BF16).astype(F32)
    rest = value - first
    second = rest.astype(BF16).astype(F32)
    return first, second, rest - second


def feature_rows(rows):
    count = rows[0].shape[1]
    index = lax.broadcasted_iota(jnp.int32, (8, count), 0)
    out = jnp.zeros((8, count), F32)
    for position, row in enumerate(rows):
        out = jnp.where(index == position, jnp.broadcast_to(row, (8, count)), out)
    return out


def build_list(id_row, list_ref, half_id):
    slots = id_row.shape[1]
    square = (slots, slots)

    def across(row):
        return jnp.broadcast_to(row, square).T

    id_row = id_row.astype(F32)
    id_r = jnp.broadcast_to(id_row, square)
    lane = lax.broadcasted_iota(jnp.int32, square, 1)
    sub = lax.broadcasted_iota(jnp.int32, square, 0)
    same = jnp.where(id_r == across(id_row), 1.0, 0.0)
    count_r = jnp.sum(same, axis=0, keepdims=True)
    earlier_r = jnp.sum(jnp.where(sub < lane, same, 0.0), axis=0, keepdims=True)
    first_r = (earlier_r == 0.0) & (id_row >= 0.0)
    key_c = across(jnp.where(first_r, id_row, 1e9))
    rank_r = jnp.sum(jnp.where(key_c < id_r, 1.0, 0.0), axis=0, keepdims=True)
    rank_c = across(jnp.where(first_r, rank_r, -1.0))
    count_c = across(count_r)
    hit = rank_c == lane.astype(F32)
    list_r = jnp.sum(jnp.where(hit, key_c, 0.0), axis=0, keepdims=True)
    copies_r = jnp.sum(jnp.where(hit, count_c, 0.0), axis=0, keepdims=True)
    total = jnp.sum(jnp.where(first_r, 1.0, 0.0))
    half = jnp.sum(jnp.where(first_r & (id_row < float(half_id)), 1.0, 0.0))
    index = lax.broadcasted_iota(jnp.int32, (8, slots), 0)
    table = jnp.where(index == 0, jnp.broadcast_to(list_r, (8, slots)), 0.0)
    table = jnp.where(index == 1, jnp.broadcast_to(copies_r, (8, slots)), table)
    table = jnp.where(index == 2, total, table)
    table = jnp.where(index == 3, half, table)
    list_ref[...] = table.astype(jnp.int32)


def entry_loop(table_ref, s_ref, t_ref, entries_refs, base, low, high, fresh):
    column_leaves, leaf, width = s_ref.shape
    depth = t_ref.shape[1]
    slots = table_ref.shape[1]
    start, stop = (low - base) // ENTRY_TRIP, (high - base + ENTRY_TRIP - 1) // ENTRY_TRIP

    def push(k, u):
        pair = table_ref[0, jnp.minimum(k, slots - 1)]
        rhs = jnp.concatenate([t_ref[pair // column_leaves], jnp.zeros((leaf - depth, leaf), BF16)], axis=0)
        pltpu.matmul_push_rhs(rhs, staging_register=(u // 2) % 2, mxu_index=u % 2)

    def work(*accs):
        def drain(u, turn):
            row = jnp.maximum(turn * (ENTRY_TRIP // 2) + u // 2, 0)
            entries_refs[u % 2][row] = lax.rsqrt(pltpu.matmul_pop(accs[u % 8])).astype(BF16)

        if fresh:
            for acc in accs:
                pltpu.matmul_pop(acc)

        @pl.when(stop > start)
        def _():
            for u in range(2):
                push(base + start * ENTRY_TRIP + u, u)

            @pl.loop(start, stop)
            def _(turn):
                for u in range(ENTRY_TRIP):
                    k = base + turn * ENTRY_TRIP + u
                    lhs = jnp.concatenate(
                        [s_ref[table_ref[0, k] % column_leaves], jnp.zeros((leaf, leaf - width), BF16)], axis=1
                    )
                    pltpu.matmul_acc_lhs(accs[u % 8], lhs, load_staged_rhs=(u // 2) % 2)
                    push(k + 2, u + 2)
                    if u < 4:
                        drain(ENTRY_TRIP - 4 + u, turn - 1)
                    else:
                        drain(u - 4, turn)

            for u in range(2):
                pltpu.matmul_acc_lhs(accs[u], jnp.zeros((leaf, leaf), BF16), load_staged_rhs=0)
            for u in range(ENTRY_TRIP - 4, ENTRY_TRIP):
                drain(u, stop - 1)

    pl.run_scoped(work, *[pltpu.ACC(u % 2)((leaf, leaf), F32) for u in range(8)])


def near_loop(table_ref, x_ref, entries, acc_refs, base_leaf, low, high, fresh):
    chunk_leaves, rhs, leaf = acc_refs[0].shape
    column_leaves = x_ref.shape[0]

    def work(*accs):
        def drain(u, k):
            inside = (k >= low) & (k < high)
            slot = jnp.maximum(k, 0)
            t = jnp.clip(table_ref[0, slot] // column_leaves - base_leaf, 0, chunk_leaves - 1)
            copies = jnp.where(inside, table_ref[1, slot], 0).astype(F32)
            block = pltpu.matmul_pop(accs[u])
            acc_ref = acc_refs[u % len(acc_refs)]
            acc_ref[t] = acc_ref[t] + jnp.where(inside, block * copies, 0.0)

        if fresh:
            for acc in accs:
                pltpu.matmul_pop(acc)

        @pl.when(high > low)
        def _():
            for *entries_refs, base in entries:
                end = base + 2 * entries_refs[0].shape[0]
                start = jnp.clip(low, base, end) // NEAR_TRIP
                stop = (jnp.clip(high, base, end) + NEAR_TRIP - 1) // NEAR_TRIP

                @pl.loop(start, stop)
                def _(turn):
                    for u in range(NEAR_TRIP):
                        k = turn * NEAR_TRIP + u
                        source = table_ref[0, k] % column_leaves
                        row = turn * (NEAR_TRIP // 2) - base // 2 + u // 2
                        stage = (u // 2) % 2
                        pltpu.matmul_push_rhs(entries_refs[u % 2][row], staging_register=stage, mxu_index=u % 2)
                        pltpu.matmul_acc_lhs(accs[u % 16], x_ref[source], load_staged_rhs=stage)
                        drain((u + 8) % 16, k - 8)

            end = (high + NEAR_TRIP - 1) // NEAR_TRIP * NEAR_TRIP
            for u in range(8):
                drain(u + 8, end - 8 + u)

    spare = pltpu.ACC(0)((rhs, leaf), F32), pltpu.ACC(1)((rhs, leaf), F32)
    pl.run_scoped(work, *(spare * (16 if fresh else 8)))


def first_entries_kernel(*refs, column_leaves, row_leaves, leaf, indices, bases):
    fill_ref, inputs, index_inputs = refs[0], refs[1:6], refs[6 : 6 + indices + bases]
    moved = indices + bases
    outputs, scratch = refs[6 + moved : 11 + 2 * moved], refs[11 + 2 * moved :]
    (*entries_refs, table_ref, s_ref, t_ref), index_outputs = outputs[:5], outputs[5:]
    copies, (list_ref, sem, in_sem) = scratch[:5], scratch[5:]
    moves = list(zip(inputs, copies)) + list(zip(index_inputs, index_outputs))
    loads = [pltpu.make_async_copy(src, dst, in_sem.at[i]) for i, (src, dst) in enumerate(moves)]
    for load in loads:
        load.start()
    nsrc_ref, ntgt_ref, spts_ref, area_ref, tpts_ref = copies
    for load in loads[:2]:
        load.wait()
    used = lax.broadcasted_iota(jnp.int32, nsrc_ref.shape, 1) < fill_ref[0, 0]
    ids = jnp.where(used, ntgt_ref[...] * column_leaves + nsrc_ref[...], -1)
    build_list(ids, list_ref, first_leaves(row_leaves) * column_leaves)
    copy = pltpu.make_async_copy(list_ref, table_ref, sem)
    copy.start()
    for load in loads[2:5]:
        load.wait()

    tx, ty, tz = (tpts_ref[i : i + 1, :] - 0.5 for i in range(3))
    norm = tx * tx + ty * ty + tz * tz
    h1, h2, h3 = split3(feature_rows([tx, ty, tz, jnp.ones_like(tx), norm]))
    features = jnp.concatenate([h1, h2, h1, h2, h3, h1, jnp.zeros((16,) + h1.shape[1:], F32)], axis=0).astype(BF16)
    for t in range(row_leaves):
        t_ref[t] = features[:, t * leaf : (t + 1) * leaf]

    sx, sy, sz = (spts_ref[i : i + 1, :] - 0.5 for i in range(3))
    scale = area_ref[...] * INV_FOUR_PI
    weight = 1.0 / (scale * scale)
    norm = sx * sx + sy * sy + sz * sz + SOFTENING_SQ
    g1, g2, g3 = split3(
        feature_rows([-2.0 * weight * sx, -2.0 * weight * sy, -2.0 * weight * sz, weight * norm, weight])
    )
    features = jnp.concatenate([g1, g1, g2, g2, g1, g3, jnp.zeros((16,) + g1.shape[1:], F32)], axis=0).astype(BF16)
    for s in range(column_leaves):
        column = features[:, s * leaf : (s + 1) * leaf].T
        s_ref[s] = jnp.concatenate([column, jnp.zeros((leaf, 128 - column.shape[1]), BF16)], axis=1)

    copy.wait()
    entry_loop(table_ref, s_ref, t_ref, entries_refs, 0, 0, jnp.minimum(table_ref[2, 0], 2 * entries_refs[0].shape[0]), True)
    for load in loads[5:]:
        load.wait()


def more_entries_kernel(table_ref, s_ref, t_ref, *entries_refs, first):
    last = first + 2 * entries_refs[0].shape[0]
    entry_loop(table_ref, s_ref, t_ref, entries_refs, first, first, jnp.clip(table_ref[2, 0], first, last), False)


VMEM = pl.BlockSpec(memory_space=pltpu.VMEM)
SMEM = pl.BlockSpec(memory_space=pltpu.SMEM)
HBM = pl.BlockSpec(memory_space=pltpu.HBM)


def first_leaves(row_leaves):
    return row_leaves * 9 // 16


def first_count(slots):
    return max(slots * 3 // 8 // NEAR_TRIP, 1) * NEAR_TRIP


def second_count(slots):
    return max(slots // 8 // NEAR_TRIP, 1) * NEAR_TRIP


def first_entries(near_fill, near_source, near_target, source_points, source_areas, target_points, indices, bases, leaves):
    column_leaves, row_leaves = leaves
    slots = near_source.shape[1]
    leaf = source_points.shape[1] // column_leaves
    depth = 64
    inputs = (near_source, near_target, source_points, source_areas[None, :], target_points)
    hbm_inputs = tuple(pltpu.with_memory_space_constraint(value, pltpu.HBM) for value in inputs + tuple(indices) + tuple(bases))
    return pl.pallas_call(
        functools.partial(
            first_entries_kernel, column_leaves=column_leaves, row_leaves=row_leaves, leaf=leaf,
            indices=len(indices), bases=len(bases),
        ),
        out_shape=(
            *[pltpu.VMEM((first_count(slots) // 2, leaf, leaf), BF16)] * 2,
            pltpu.SMEM((8, slots), jnp.int32),
            pltpu.VMEM((column_leaves, leaf, 128), BF16),
            pltpu.VMEM((row_leaves, depth, leaf), BF16),
        )
        + tuple(pltpu.SMEM(value.shape, jnp.int32) for value in indices)
        + tuple(pltpu.VMEM(value.shape, value.dtype) for value in bases),
        in_specs=[SMEM] + [HBM] * len(hbm_inputs),
        out_specs=(VMEM, VMEM, SMEM, VMEM, VMEM) + (SMEM,) * len(indices) + (VMEM,) * len(bases),
        scratch_shapes=[pltpu.VMEM(value.shape, value.dtype) for value in inputs]
        + [pltpu.VMEM((8, slots), jnp.int32), pltpu.SemaphoreType.DMA, pltpu.SemaphoreType.DMA((len(hbm_inputs),))],
        compiler_params=pltpu.CompilerParams(vmem_limit_bytes=10 << 20),
        cost_estimate=pl.CostEstimate(flops=8_000_000_000, bytes_accessed=1 << 20, transcendentals=0),
        name="entries",
    )(near_fill, *hbm_inputs)


def more_entries(table, s_features, t_features, first, count):
    leaf = s_features.shape[1]
    return pl.pallas_call(
        functools.partial(more_entries_kernel, first=first),
        out_shape=(pltpu.VMEM((count // 2, leaf, leaf), BF16),) * 2,
        in_specs=[SMEM, VMEM, VMEM],
        out_specs=(VMEM, VMEM),
        compiler_params=pltpu.CompilerParams(vmem_limit_bytes=4 << 20),
        cost_estimate=pl.CostEstimate(flops=8_000_000_000, bytes_accessed=1 << 20, transcendentals=0),
        name="entries_rest",
    )(table, s_features, t_features)


def far_kernel(*refs, pieces, plain, leaf, unroll):
    (sfill_ref, fsrc_ref, ftgt_ref, frank_ref, left_ref, right_ref) = refs[:6]
    piece_refs = refs[6 : 6 + pieces]
    x_ref, acc_ref, coef_ref = refs[6 + pieces :]
    column_leaves, rhs, _ = x_ref.shape
    far_slots, rank, _ = left_ref.shape

    lane = lax.broadcasted_iota(jnp.int32, (rhs, leaf), 1)
    if not plain:
        parity = lax.rem(lax.axis_index("row"), 2)
    for s in range(column_leaves):
        window = slice(s * leaf, (s + 1) * leaf)
        if plain:
            block = piece_refs[0][:, window].astype(F32)
        else:
            rows = []
            for j in range(pieces // 2):
                mine = piece_refs[j][:, window].astype(F32)
                other = piece_refs[pieces // 2 + j][:, window].astype(F32)
                rows.append(jnp.where(parity == 0, mine, other))
                rows.append(jnp.where(parity == 0, other, mine))
            block = jnp.concatenate(rows, axis=0)
        x_ref[s] = jnp.where(lane < sfill_ref[s], block, 0.0).astype(BF16)

    acc_ref[...] = jnp.zeros_like(acc_ref)

    rank_lane = lax.broadcasted_iota(jnp.int32, (rhs, rank), 1)

    @pl.loop(0, far_slots // unroll)
    def _(turn):
        for u in range(unroll):
            k = turn * unroll + u
            coef = lax.dot_general(
                x_ref[fsrc_ref[0, k]], right_ref[k], (((1,), (1,)), ((), ())), preferred_element_type=F32
            )
            coef_ref[k] = jnp.where(rank_lane < frank_ref[0, k], coef, 0.0).astype(BF16)

    @pl.loop(0, far_slots // unroll)
    def _(turn):
        blocks = []
        for u in range(unroll):
            k = turn * unroll + u
            blocks.append(jnp.dot(coef_ref[k], left_ref[k], preferred_element_type=F32))
        for u in range(unroll):
            t = ftgt_ref[0, turn * unroll + u]
            acc_ref[t] = acc_ref[t] + blocks[u]


def near_kernel(*refs, base_leaf, plain, out_carried, firsts, complete):
    carried, arrays = len(out_carried), 2 * len(firsts)
    (table_ref, tfill_ref, far_ref, x_ref, s_ref, t_ref), made_refs = refs[:6], refs[6 : 6 + arrays]
    carried_refs = refs[6 + arrays : 6 + arrays + carried]
    tail = len(refs) - SUMS
    out_refs, rest_refs, acc_refs = refs[6 + arrays + carried : tail - 2], refs[tail - 2 : tail], refs[tail:]
    chunk_leaves, rhs, leaf = acc_refs[0].shape
    total, half = table_ref[2, 0], table_ref[3, 0]
    low = half if base_leaf > 0 else 0
    high = total if base_leaf + chunk_leaves == far_ref.shape[0] else half
    made = firsts[-1] + 2 * made_refs[-1].shape[0]
    for acc_ref in acc_refs:
        acc_ref[...] = jnp.zeros_like(acc_ref)
    near_loop(
        table_ref, x_ref, [(made_refs[2 * i], made_refs[2 * i + 1], first) for i, first in enumerate(firsts)], acc_refs,
        base_leaf, jnp.minimum(low, made), jnp.minimum(high, made), base_leaf == 0,
    )
    if not complete:
        rest = (jnp.maximum(low, made), jnp.maximum(high, made))
        entry_loop(table_ref, s_ref, t_ref, rest_refs, made, *rest, False)
        near_loop(table_ref, x_ref, [(*rest_refs, made)], acc_refs, base_leaf, *rest, False)

    if plain:
        lane_t = lax.broadcasted_iota(jnp.int32, (rhs, leaf), 1)
        for t in range(chunk_leaves):
            value = sum((acc_ref[t] for acc_ref in acc_refs), far_ref[base_leaf + t])
            out_refs[0][:, t * leaf : (t + 1) * leaf] = jnp.where(lane_t < tfill_ref[base_leaf + t], value, 0.0)
    else:
        owners = len(out_refs)
        height = rhs // owners
        lane_t = lax.broadcasted_iota(jnp.int32, (height, leaf), 1)
        base = lax.axis_index("col") ^ (lax.axis_index("row") // 2)
        for m in range(owners):
            start = pl.multiple_of((base ^ m) * height, height)
            shift = out_refs[m].shape[1] - chunk_leaves * leaf
            if shift:
                out_refs[m][:, :shift] = carried_refs[out_carried.index(m)][...]
            for t in range(chunk_leaves):
                rows = pl.ds(start, height)
                value = sum((acc_ref[t, rows, :] for acc_ref in acc_refs), far_ref[base_leaf + t, rows, :])
                value = jnp.where(lane_t < tfill_ref[base_leaf + t], value, 0.0)
                window = slice(shift + t * leaf, shift + (t + 1) * leaf)
                out_refs[m][:, window] = value.astype(out_refs[m].dtype)


def far_field(source_fill, row_leaves, far_source, far_target, far_rank, left, right, pieces, plain):
    column_leaves = source_fill.shape[0]
    far_slots, rank, leaf = left.shape
    rhs = sum(p.shape[0] for p in pieces)
    vmem = pl.BlockSpec(memory_space=pltpu.VMEM)
    smem = pl.BlockSpec(memory_space=pltpu.SMEM)
    unroll = next(u for u in (32, 16, 8, 4, 2, 1) if far_slots % u == 0)
    return pl.pallas_call(
        functools.partial(far_kernel, pieces=len(pieces), plain=plain, leaf=leaf, unroll=unroll),
        out_shape=(pltpu.VMEM((column_leaves, rhs, leaf), BF16), pltpu.VMEM((row_leaves, rhs, leaf), F32)),
        in_specs=[smem] * 4 + [vmem] * (2 + len(pieces)),
        out_specs=(vmem, vmem),
        scratch_shapes=[pltpu.VMEM((far_slots, rhs, rank), BF16)],
        compiler_params=pltpu.CompilerParams(vmem_limit_bytes=12 << 20),
        cost_estimate=pl.CostEstimate(flops=2_000_000_000, bytes_accessed=8 << 20, transcendentals=0),
        name="far",
    )(source_fill, far_source, far_target, far_rank, left, right, *pieces)


def near_field(table, target_fill, far, x, made, features, owners, plain, leaves, carried=(), out_carried=()):
    firsts, arrays = zip(*made)
    made = [value for pair in arrays for value in pair]
    _, rhs, leaf = far.shape
    width = len(leaves) * leaf
    if plain:
        out_shape = (jax.ShapeDtypeStruct((rhs, width), F32),)
    else:
        out_shape = tuple(
            jax.ShapeDtypeStruct(
                (rhs // owners, width + (carried[0].shape[1] if m in out_carried else 0)), F32 if m == 0 else BF16
            )
            for m in range(owners)
        )
    rest = table.shape[1] // 2 - sum(value.shape[0] for value in made) // 2
    complete = rest == 0
    rest = max(rest, 1)
    return pl.pallas_call(
        functools.partial(
            near_kernel, base_leaf=leaves[0], firsts=firsts, complete=complete, plain=plain,
            out_carried=tuple(out_carried),
        ),
        out_shape=out_shape,
        in_specs=[SMEM] * 2 + [VMEM] * (4 + len(made) + len(carried)),
        out_specs=(VMEM,) * len(out_shape),
        scratch_shapes=[pltpu.VMEM((rest, leaf, leaf), BF16)] * 2 + [pltpu.VMEM((len(leaves), rhs, leaf), F32)] * SUMS,
        compiler_params=pltpu.CompilerParams(vmem_limit_bytes=20 << 20),
        cost_estimate=pl.CostEstimate(flops=4_000_000_000, bytes_accessed=8 << 20, transcendentals=0),
        name="near",
    )(table, target_fill, far, x, *features, *made, *carried)


def shards(
    source_points, source_areas, source_fill, target_points, target_fill, charges, near_fill, near_source,
    near_target, far_source, far_target, far_rank, left_basis, right_basis, *, rows, columns,
):
    plain = charges.shape[0] % 8 != 0 or rows != 2 * columns
    if plain:
        pieces = [lax.all_gather(charges, "row", axis=0, tiled=True)]
    else:

        def swap(value, axis, size, mask):
            return lax.ppermute(value, axis, [(i, i ^ mask) for i in range(size)])

        pieces = [charges] + [swap(charges, "row", rows, mask) for mask in range(2, rows, 2)]
    row_leaves, column_leaves = target_fill.shape[0], source_fill.shape[0]
    first_outs = first_entries(
        near_fill, near_source, near_target, source_points, source_areas, target_points,
        (source_fill, target_fill, far_source, far_target, far_rank), (left_basis[0], right_basis[0]),
        (column_leaves, row_leaves),
    )
    *entries, table, s_features, t_features = first_outs[:5]
    features = (s_features, t_features)
    source_fill, target_fill, far_source, far_target, far_rank, left, right = first_outs[5:]
    if not plain:
        pieces, table = lax.optimization_barrier((pieces, table))
        pieces = pieces + [swap(piece, "row", rows, 1) for piece in pieces]
    slots = near_source.shape[1]
    first, second = first_count(slots), second_count(slots)
    more = list(more_entries(table, *features, first, second))
    if not plain:
        pieces, more[0] = lax.optimization_barrier((pieces, more[0]))
    made = [(0, entries), (first, more)]
    x, far = far_field(
        source_fill, row_leaves, far_source, far_target, far_rank, left, right, pieces, plain
    )
    if plain or row_leaves < 2 or columns < 3:
        outs = near_field(table, target_fill, far, x, made, features, columns, plain, range(row_leaves))
        if plain:
            return lax.psum_scatter(outs[0], "col", scatter_dimension=0, tiled=True)
        result = outs[0]
        for mask in reversed(range(1, columns)):
            result = result + swap(outs[mask], "col", columns, mask).astype(F32)
        return result

    def exchange(value, mask):
        return swap(value, "col", columns, mask)

    split = first_leaves(row_leaves)
    inputs = (table, target_fill, far, x, made, features, columns, plain)
    one = near_field(*inputs, range(split))
    early = {mask: exchange(one[mask], mask) for mask in far_masks(columns)}
    two = near_field(*inputs, range(split, row_leaves), (one[1],), (1,))
    late = {mask: exchange(two[mask], mask) for mask in far_masks(columns) + [1]}
    result = jnp.concatenate([one[0], two[0]], axis=1) + late[1].astype(F32)
    for mask in early:
        result = result + jnp.concatenate([early[mask], late[mask]], axis=1).astype(F32)
    return result


def far_masks(columns):
    return list(range(2, columns))


def solution(mesh):
    placed = (
        P(None, "col"), P("col"), P("col"), P(None, "row"), P("row"), P("row", "col"), P("row", "col"),
        P("row", "col"), P("row", "col"), P("row", "col"), P("row", "col"), P("row", "col"),
        P("row", "col", None, None), P("row", "col", None, None),
    )
    return jax.shard_map(
        functools.partial(shards, rows=mesh.shape["row"], columns=mesh.shape["col"]),
        mesh=mesh, in_specs=placed, out_specs=P("col", "row"), check_vma=False,
    )
```

```python
import functools

import jax
import jax.numpy as jnp
from jax import lax
from jax.experimental import pallas as pl
from jax.experimental.pallas import tpu as pltpu
from jax.sharding import PartitionSpec as P


INV_FOUR_PI = 0.07957747154594767
SOFTENING_SQ = 0.0025
F32 = jnp.float32
BF16 = jnp.bfloat16
ENTRY_TRIP = 16
SUMS = 1
NEAR_TRIP = 16


def split3(value):
    first = value.astype(BF16).astype(F32)
    rest = value - first
    second = rest.astype(BF16).astype(F32)
    return first, second, rest - second


def feature_rows(rows):
    count = rows[0].shape[1]
    index = lax.broadcasted_iota(jnp.int32, (8, count), 0)
    out = jnp.zeros((8, count), F32)
    for position, row in enumerate(rows):
        out = jnp.where(index == position, jnp.broadcast_to(row, (8, count)), out)
    return out


def build_list(id_row, list_ref, half_id):
    slots = id_row.shape[1]
    square = (slots, slots)

    def across(row):
        return jnp.broadcast_to(row, square).T

    id_row = id_row.astype(F32)
    id_r = jnp.broadcast_to(id_row, square)
    lane = lax.broadcasted_iota(jnp.int32, square, 1)
    sub = lax.broadcasted_iota(jnp.int32, square, 0)
    same = jnp.where(id_r == across(id_row), 1.0, 0.0)
    count_r = jnp.sum(same, axis=0, keepdims=True)
    earlier_r = jnp.sum(jnp.where(sub < lane, same, 0.0), axis=0, keepdims=True)
    first_r = (earlier_r == 0.0) & (id_row >= 0.0)
    key_c = across(jnp.where(first_r, id_row, 1e9))
    rank_r = jnp.sum(jnp.where(key_c < id_r, 1.0, 0.0), axis=0, keepdims=True)
    rank_c = across(jnp.where(first_r, rank_r, -1.0))
    count_c = across(count_r)
    hit = rank_c == lane.astype(F32)
    list_r = jnp.sum(jnp.where(hit, key_c, 0.0), axis=0, keepdims=True)
    copies_r = jnp.sum(jnp.where(hit, count_c, 0.0), axis=0, keepdims=True)
    total = jnp.sum(jnp.where(first_r, 1.0, 0.0))
    half = jnp.sum(jnp.where(first_r & (id_row < float(half_id)), 1.0, 0.0))
    index = lax.broadcasted_iota(jnp.int32, (8, slots), 0)
    table = jnp.where(index == 0, jnp.broadcast_to(list_r, (8, slots)), 0.0)
    table = jnp.where(index == 1, jnp.broadcast_to(copies_r, (8, slots)), table)
    table = jnp.where(index == 2, total, table)
    table = jnp.where(index == 3, half, table)
    list_ref[...] = table.astype(jnp.int32)


def entry_loop(table_ref, s_ref, t_ref, entries_refs, base, low, high, fresh):
    column_leaves, leaf, width = s_ref.shape
    depth = t_ref.shape[1]
    slots = table_ref.shape[1]
    start, stop = (low - base) // ENTRY_TRIP, (high - base + ENTRY_TRIP - 1) // ENTRY_TRIP

    def push(k, u):
        pair = table_ref[0, jnp.minimum(k, slots - 1)]
        rhs = jnp.concatenate([t_ref[pair // column_leaves], jnp.zeros((leaf - depth, leaf), BF16)], axis=0)
        pltpu.matmul_push_rhs(rhs, staging_register=(u // 2) % 2, mxu_index=u % 2)

    def work(*accs):
        def drain(u, turn):
            row = jnp.maximum(turn * (ENTRY_TRIP // 2) + u // 2, 0)
            entries_refs[u % 2][row] = lax.rsqrt(pltpu.matmul_pop(accs[u % 8])).astype(BF16)

        if fresh:
            for acc in accs:
                pltpu.matmul_pop(acc)

        @pl.when(stop > start)
        def _():
            for u in range(2):
                push(base + start * ENTRY_TRIP + u, u)

            @pl.loop(start, stop)
            def _(turn):
                for u in range(ENTRY_TRIP):
                    k = base + turn * ENTRY_TRIP + u
                    lhs = jnp.concatenate(
                        [s_ref[table_ref[0, k] % column_leaves], jnp.zeros((leaf, leaf - width), BF16)], axis=1
                    )
                    pltpu.matmul_acc_lhs(accs[u % 8], lhs, load_staged_rhs=(u // 2) % 2)
                    push(k + 2, u + 2)
                    if u < 4:
                        drain(ENTRY_TRIP - 4 + u, turn - 1)
                    else:
                        drain(u - 4, turn)

            for u in range(2):
                pltpu.matmul_acc_lhs(accs[u], jnp.zeros((leaf, leaf), BF16), load_staged_rhs=0)
            for u in range(ENTRY_TRIP - 4, ENTRY_TRIP):
                drain(u, stop - 1)

    pl.run_scoped(work, *[pltpu.ACC(u % 2)((leaf, leaf), F32) for u in range(8)])


def near_loop(table_ref, x_ref, entries, acc_refs, base_leaf, low, high, fresh):
    chunk_leaves, rhs, leaf = acc_refs[0].shape
    column_leaves = x_ref.shape[0]

    def work(*accs):
        def drain(u, k):
            inside = (k >= low) & (k < high)
            slot = jnp.maximum(k, 0)
            t = jnp.clip(table_ref[0, slot] // column_leaves - base_leaf, 0, chunk_leaves - 1)
            copies = jnp.where(inside, table_ref[1, slot], 0).astype(F32)
            block = pltpu.matmul_pop(accs[u])
            acc_ref = acc_refs[u % len(acc_refs)]
            acc_ref[t] = acc_ref[t] + jnp.where(inside, block * copies, 0.0)

        if fresh:
            for acc in accs:
                pltpu.matmul_pop(acc)

        @pl.when(high > low)
        def _():
            for *entries_refs, base in entries:
                end = base + 2 * entries_refs[0].shape[0]
                start = jnp.clip(low, base, end) // NEAR_TRIP
                stop = (jnp.clip(high, base, end) + NEAR_TRIP - 1) // NEAR_TRIP

                @pl.loop(start, stop)
                def _(turn):
                    for u in range(NEAR_TRIP):
                        k = turn * NEAR_TRIP + u
                        source = table_ref[0, k] % column_leaves
                        row = turn * (NEAR_TRIP // 2) - base // 2 + u // 2
                        stage = (u // 2) % 2
                        pltpu.matmul_push_rhs(entries_refs[u % 2][row], staging_register=stage, mxu_index=u % 2)
                        pltpu.matmul_acc_lhs(accs[u % 16], x_ref[source], load_staged_rhs=stage)
                        drain((u + 8) % 16, k - 8)

            end = (high + NEAR_TRIP - 1) // NEAR_TRIP * NEAR_TRIP
            for u in range(8):
                drain(u + 8, end - 8 + u)

    spare = pltpu.ACC(0)((rhs, leaf), F32), pltpu.ACC(1)((rhs, leaf), F32)
    pl.run_scoped(work, *(spare * (16 if fresh else 8)))


def first_entries_kernel(*refs, column_leaves, row_leaves, leaf, indices, bases):
    fill_ref, inputs, index_inputs = refs[0], refs[1:6], refs[6 : 6 + indices + bases]
    moved = indices + bases
    outputs, scratch = refs[6 + moved : 11 + 2 * moved], refs[11 + 2 * moved :]
    (*entries_refs, table_ref, s_ref, t_ref), index_outputs = outputs[:5], outputs[5:]
    copies, (list_ref, sem, in_sem) = scratch[:5], scratch[5:]
    moves = list(zip(inputs, copies)) + list(zip(index_inputs, index_outputs))
    loads = [pltpu.make_async_copy(src, dst, in_sem.at[i]) for i, (src, dst) in enumerate(moves)]
    for load in loads:
        load.start()
    nsrc_ref, ntgt_ref, spts_ref, area_ref, tpts_ref = copies
    for load in loads[:2]:
        load.wait()
    used = lax.broadcasted_iota(jnp.int32, nsrc_ref.shape, 1) < fill_ref[0, 0]
    ids = jnp.where(used, ntgt_ref[...] * column_leaves + nsrc_ref[...], -1)
    build_list(ids, list_ref, first_leaves(row_leaves) * column_leaves)
    copy = pltpu.make_async_copy(list_ref, table_ref, sem)
    copy.start()
    for load in loads[2:5]:
        load.wait()

    tx, ty, tz = (tpts_ref[i : i + 1, :] - 0.5 for i in range(3))
    norm = tx * tx + ty * ty + tz * tz
    h1, h2, h3 = split3(feature_rows([tx, ty, tz, jnp.ones_like(tx), norm]))
    features = jnp.concatenate([h1, h2, h1, h2, h3, h1, jnp.zeros((16,) + h1.shape[1:], F32)], axis=0).astype(BF16)
    for t in range(row_leaves):
        t_ref[t] = features[:, t * leaf : (t + 1) * leaf]

    sx, sy, sz = (spts_ref[i : i + 1, :] - 0.5 for i in range(3))
    scale = area_ref[...] * INV_FOUR_PI
    weight = 1.0 / (scale * scale)
    norm = sx * sx + sy * sy + sz * sz + SOFTENING_SQ
    g1, g2, g3 = split3(
        feature_rows([-2.0 * weight * sx, -2.0 * weight * sy, -2.0 * weight * sz, weight * norm, weight])
    )
    features = jnp.concatenate([g1, g1, g2, g2, g1, g3, jnp.zeros((16,) + g1.shape[1:], F32)], axis=0).astype(BF16)
    for s in range(column_leaves):
        column = features[:, s * leaf : (s + 1) * leaf].T
        s_ref[s] = jnp.concatenate([column, jnp.zeros((leaf, 128 - column.shape[1]), BF16)], axis=1)

    copy.wait()
    entry_loop(table_ref, s_ref, t_ref, entries_refs, 0, 0, jnp.minimum(table_ref[2, 0], 2 * entries_refs[0].shape[0]), True)
    for load in loads[5:]:
        load.wait()


def more_entries_kernel(table_ref, s_ref, t_ref, *entries_refs, first):
    last = first + 2 * entries_refs[0].shape[0]
    entry_loop(table_ref, s_ref, t_ref, entries_refs, first, first, jnp.clip(table_ref[2, 0], first, last), False)


VMEM = pl.BlockSpec(memory_space=pltpu.VMEM)
SMEM = pl.BlockSpec(memory_space=pltpu.SMEM)
HBM = pl.BlockSpec(memory_space=pltpu.HBM)


def first_leaves(row_leaves):
    return row_leaves * 11 // 16


def first_count(slots):
    return max(slots * 3 // 8 // NEAR_TRIP, 1) * NEAR_TRIP


def second_count(slots):
    return max(slots // 4 // NEAR_TRIP, 1) * NEAR_TRIP


def first_entries(near_fill, near_source, near_target, source_points, source_areas, target_points, indices, bases, leaves):
    column_leaves, row_leaves = leaves
    slots = near_source.shape[1]
    leaf = source_points.shape[1] // column_leaves
    depth = 64
    inputs = (near_source, near_target, source_points, source_areas[None, :], target_points)
    hbm_inputs = tuple(pltpu.with_memory_space_constraint(value, pltpu.HBM) for value in inputs + tuple(indices) + tuple(bases))
    return pl.pallas_call(
        functools.partial(
            first_entries_kernel, column_leaves=column_leaves, row_leaves=row_leaves, leaf=leaf,
            indices=len(indices), bases=len(bases),
        ),
        out_shape=(
            *[pltpu.VMEM((first_count(slots) // 2, leaf, leaf), BF16)] * 2,
            pltpu.SMEM((8, slots), jnp.int32),
            pltpu.VMEM((column_leaves, leaf, 128), BF16),
            pltpu.VMEM((row_leaves, depth, leaf), BF16),
        )
        + tuple(pltpu.SMEM(value.shape, jnp.int32) for value in indices)
        + tuple(pltpu.VMEM(value.shape, value.dtype) for value in bases),
        in_specs=[SMEM] + [HBM] * len(hbm_inputs),
        out_specs=(VMEM, VMEM, SMEM, VMEM, VMEM) + (SMEM,) * len(indices) + (VMEM,) * len(bases),
        scratch_shapes=[pltpu.VMEM(value.shape, value.dtype) for value in inputs]
        + [pltpu.VMEM((8, slots), jnp.int32), pltpu.SemaphoreType.DMA, pltpu.SemaphoreType.DMA((len(hbm_inputs),))],
        compiler_params=pltpu.CompilerParams(vmem_limit_bytes=10 << 20),
        cost_estimate=pl.CostEstimate(flops=8_000_000_000, bytes_accessed=1 << 20, transcendentals=0),
        name="entries",
    )(near_fill, *hbm_inputs)


def more_entries(table, s_features, t_features, first, count):
    leaf = s_features.shape[1]
    return pl.pallas_call(
        functools.partial(more_entries_kernel, first=first),
        out_shape=(pltpu.VMEM((count // 2, leaf, leaf), BF16),) * 2,
        in_specs=[SMEM, VMEM, VMEM],
        out_specs=(VMEM, VMEM),
        compiler_params=pltpu.CompilerParams(vmem_limit_bytes=4 << 20),
        cost_estimate=pl.CostEstimate(flops=8_000_000_000, bytes_accessed=1 << 20, transcendentals=0),
        name="entries_rest",
    )(table, s_features, t_features)


def far_kernel(*refs, pieces, plain, leaf, unroll):
    (sfill_ref, fsrc_ref, ftgt_ref, frank_ref, left_ref, right_ref) = refs[:6]
    piece_refs = refs[6 : 6 + pieces]
    x_ref, acc_ref, coef_ref = refs[6 + pieces :]
    column_leaves, rhs, _ = x_ref.shape
    far_slots, rank, _ = left_ref.shape

    lane = lax.broadcasted_iota(jnp.int32, (rhs, leaf), 1)
    if not plain:
        parity = lax.rem(lax.axis_index("row"), 2)
    for s in range(column_leaves):
        window = slice(s * leaf, (s + 1) * leaf)
        if plain:
            block = piece_refs[0][:, window].astype(F32)
        else:
            rows = []
            for j in range(pieces // 2):
                mine = piece_refs[j][:, window].astype(F32)
                other = piece_refs[pieces // 2 + j][:, window].astype(F32)
                rows.append(jnp.where(parity == 0, mine, other))
                rows.append(jnp.where(parity == 0, other, mine))
            block = jnp.concatenate(rows, axis=0)
        x_ref[s] = jnp.where(lane < sfill_ref[s], block, 0.0).astype(BF16)

    acc_ref[...] = jnp.zeros_like(acc_ref)

    rank_lane = lax.broadcasted_iota(jnp.int32, (rhs, rank), 1)

    @pl.loop(0, far_slots // unroll)
    def _(turn):
        for u in range(unroll):
            k = turn * unroll + u
            coef = lax.dot_general(
                x_ref[fsrc_ref[0, k]], right_ref[k], (((1,), (1,)), ((), ())), preferred_element_type=F32
            )
            coef_ref[k] = jnp.where(rank_lane < frank_ref[0, k], coef, 0.0).astype(BF16)

    @pl.loop(0, far_slots // unroll)
    def _(turn):
        blocks = []
        for u in range(unroll):
            k = turn * unroll + u
            blocks.append(jnp.dot(coef_ref[k], left_ref[k], preferred_element_type=F32))
        for u in range(unroll):
            t = ftgt_ref[0, turn * unroll + u]
            acc_ref[t] = acc_ref[t] + blocks[u]


def near_kernel(*refs, base_leaf, plain, out_carried, firsts, complete):
    carried, arrays = len(out_carried), 2 * len(firsts)
    (table_ref, tfill_ref, far_ref, x_ref, s_ref, t_ref), made_refs = refs[:6], refs[6 : 6 + arrays]
    carried_refs = refs[6 + arrays : 6 + arrays + carried]
    tail = len(refs) - SUMS
    out_refs, rest_refs, acc_refs = refs[6 + arrays + carried : tail - 2], refs[tail - 2 : tail], refs[tail:]
    chunk_leaves, rhs, leaf = acc_refs[0].shape
    total, half = table_ref[2, 0], table_ref[3, 0]
    low = half if base_leaf > 0 else 0
    high = total if base_leaf + chunk_leaves == far_ref.shape[0] else half
    made = firsts[-1] + 2 * made_refs[-1].shape[0]
    for acc_ref in acc_refs:
        acc_ref[...] = jnp.zeros_like(acc_ref)
    near_loop(
        table_ref, x_ref, [(made_refs[2 * i], made_refs[2 * i + 1], first) for i, first in enumerate(firsts)], acc_refs,
        base_leaf, jnp.minimum(low, made), jnp.minimum(high, made), base_leaf == 0,
    )
    if not complete:
        rest = (jnp.maximum(low, made), jnp.maximum(high, made))
        entry_loop(table_ref, s_ref, t_ref, rest_refs, made, *rest, False)
        near_loop(table_ref, x_ref, [(*rest_refs, made)], acc_refs, base_leaf, *rest, False)

    if plain:
        lane_t = lax.broadcasted_iota(jnp.int32, (rhs, leaf), 1)
        for t in range(chunk_leaves):
            value = sum((acc_ref[t] for acc_ref in acc_refs), far_ref[base_leaf + t])
            out_refs[0][:, t * leaf : (t + 1) * leaf] = jnp.where(lane_t < tfill_ref[base_leaf + t], value, 0.0)
    else:
        owners = len(out_refs)
        height = rhs // owners
        lane_t = lax.broadcasted_iota(jnp.int32, (height, leaf), 1)
        base = lax.axis_index("col") ^ (lax.axis_index("row") // 2)
        for m in range(owners):
            start = pl.multiple_of((base ^ m) * height, height)
            shift = out_refs[m].shape[1] - chunk_leaves * leaf
            if shift:
                out_refs[m][:, :shift] = carried_refs[out_carried.index(m)][...]
            for t in range(chunk_leaves):
                rows = pl.ds(start, height)
                value = sum((acc_ref[t, rows, :] for acc_ref in acc_refs), far_ref[base_leaf + t, rows, :])
                value = jnp.where(lane_t < tfill_ref[base_leaf + t], value, 0.0)
                window = slice(shift + t * leaf, shift + (t + 1) * leaf)
                out_refs[m][:, window] = value.astype(out_refs[m].dtype)


def far_field(source_fill, row_leaves, far_source, far_target, far_rank, left, right, pieces, plain):
    column_leaves = source_fill.shape[0]
    far_slots, rank, leaf = left.shape
    rhs = sum(p.shape[0] for p in pieces)
    vmem = pl.BlockSpec(memory_space=pltpu.VMEM)
    smem = pl.BlockSpec(memory_space=pltpu.SMEM)
    unroll = next(u for u in (32, 16, 8, 4, 2, 1) if far_slots % u == 0)
    return pl.pallas_call(
        functools.partial(far_kernel, pieces=len(pieces), plain=plain, leaf=leaf, unroll=unroll),
        out_shape=(pltpu.VMEM((column_leaves, rhs, leaf), BF16), pltpu.VMEM((row_leaves, rhs, leaf), F32)),
        in_specs=[smem] * 4 + [vmem] * (2 + len(pieces)),
        out_specs=(vmem, vmem),
        scratch_shapes=[pltpu.VMEM((far_slots, rhs, rank), BF16)],
        compiler_params=pltpu.CompilerParams(vmem_limit_bytes=12 << 20),
        cost_estimate=pl.CostEstimate(flops=2_000_000_000, bytes_accessed=8 << 20, transcendentals=0),
        name="far",
    )(source_fill, far_source, far_target, far_rank, left, right, *pieces)


def near_field(table, target_fill, far, x, made, features, owners, plain, leaves, carried=(), out_carried=()):
    firsts, arrays = zip(*made)
    made = [value for pair in arrays for value in pair]
    _, rhs, leaf = far.shape
    width = len(leaves) * leaf
    if plain:
        out_shape = (jax.ShapeDtypeStruct((rhs, width), F32),)
    else:
        out_shape = tuple(
            jax.ShapeDtypeStruct(
                (rhs // owners, width + (carried[0].shape[1] if m in out_carried else 0)), F32 if m == 0 else BF16
            )
            for m in range(owners)
        )
    rest = table.shape[1] // 2 - sum(value.shape[0] for value in made) // 2
    complete = rest == 0
    rest = max(rest, 1)
    return pl.pallas_call(
        functools.partial(
            near_kernel, base_leaf=leaves[0], firsts=firsts, complete=complete, plain=plain,
            out_carried=tuple(out_carried),
        ),
        out_shape=out_shape,
        in_specs=[SMEM] * 2 + [VMEM] * (4 + len(made) + len(carried)),
        out_specs=(VMEM,) * len(out_shape),
        scratch_shapes=[pltpu.VMEM((rest, leaf, leaf), BF16)] * 2 + [pltpu.VMEM((len(leaves), rhs, leaf), F32)] * SUMS,
        compiler_params=pltpu.CompilerParams(vmem_limit_bytes=20 << 20),
        cost_estimate=pl.CostEstimate(flops=4_000_000_000, bytes_accessed=8 << 20, transcendentals=0),
        name="near",
    )(table, target_fill, far, x, *features, *made, *carried)


def shards(
    source_points, source_areas, source_fill, target_points, target_fill, charges, near_fill, near_source,
    near_target, far_source, far_target, far_rank, left_basis, right_basis, *, rows, columns,
):
    plain = charges.shape[0] % 8 != 0 or rows != 2 * columns
    if plain:
        pieces = [lax.all_gather(charges, "row", axis=0, tiled=True)]
    else:

        def swap(value, axis, size, mask):
            return lax.ppermute(value, axis, [(i, i ^ mask) for i in range(size)])

        pieces = [charges] + [swap(charges, "row", rows, mask) for mask in range(2, rows, 2)]
    row_leaves, column_leaves = target_fill.shape[0], source_fill.shape[0]
    first_outs = first_entries(
        near_fill, near_source, near_target, source_points, source_areas, target_points,
        (source_fill, target_fill, far_source, far_target, far_rank), (left_basis[0], right_basis[0]),
        (column_leaves, row_leaves),
    )
    *entries, table, s_features, t_features = first_outs[:5]
    features = (s_features, t_features)
    source_fill, target_fill, far_source, far_target, far_rank, left, right = first_outs[5:]
    if not plain:
        pieces, table = lax.optimization_barrier((pieces, table))
        pieces = pieces + [swap(piece, "row", rows, 1) for piece in pieces]
    slots = near_source.shape[1]
    first, second = first_count(slots), second_count(slots)
    more = list(more_entries(table, *features, first, second))
    if not plain:
        pieces, more[0] = lax.optimization_barrier((pieces, more[0]))
    made = [(0, entries), (first, more)]
    x, far = far_field(
        source_fill, row_leaves, far_source, far_target, far_rank, left, right, pieces, plain
    )
    if plain or row_leaves < 2 or columns < 3:
        outs = near_field(table, target_fill, far, x, made, features, columns, plain, range(row_leaves))
        if plain:
            return lax.psum_scatter(outs[0], "col", scatter_dimension=0, tiled=True)
        result = outs[0]
        for mask in reversed(range(1, columns)):
            result = result + swap(outs[mask], "col", columns, mask).astype(F32)
        return result

    def exchange(value, mask):
        return swap(value, "col", columns, mask)

    split = first_leaves(row_leaves)
    inputs = (table, target_fill, far, x, made, features, columns, plain)
    one = near_field(*inputs, range(split))
    early = {mask: exchange(one[mask], mask) for mask in far_masks(columns)}
    two = near_field(*inputs, range(split, row_leaves), (one[1],), (1,))
    late = {mask: exchange(two[mask], mask) for mask in late_masks(columns)}
    result = jnp.concatenate([one[0], two[0]], axis=1) + late[1].astype(F32)
    for mask in early:
        result = result + jnp.concatenate([early[mask], late[mask]], axis=1).astype(F32)
    return result


def far_masks(columns):
    return list(range(2, columns))


def late_masks(columns):
    return [1] + far_masks(columns)[::-1]


def solution(mesh):
    placed = (
        P(None, "col"), P("col"), P("col"), P(None, "row"), P("row"), P("row", "col"), P("row", "col"),
        P("row", "col"), P("row", "col"), P("row", "col"), P("row", "col"), P("row", "col"),
        P("row", "col", None, None), P("row", "col", None, None),
    )
    return jax.shard_map(
        functools.partial(shards, rows=mesh.shape["row"], columns=mesh.shape["col"]),
        mesh=mesh, in_specs=placed, out_specs=P("col", "row"), check_vma=False,
    )
```
